128 devices in a mesh: tm: 8 (over x, core), lat: 4 (over y), lon: 4 (over z).
Axes of the slice: x: 4, y: 4, z: 4, core: 2. Of those that a mesh axis runs over, the one named last changes fastest.
Arguments:
- forcing: float32 [32, 512, 2048], P('tm', 'lat', 'lon'), may hold values from -17 to 17
- depth: float32 [512, 2048], P('lat', 'lon'), may hold values from 0.2 to 2
- mask: int32 [512, 2048], P('lat', 'lon'), may hold values 0 or 1
- guess: float32 [8, 512, 2048], P('tm', 'lat', 'lon'), may hold values from -6 to 6
Outputs:
- adjoint: float32 [32, 512, 2048], P('tm', 'lat', 'lon')
The draws below stay inside these ranges and needn't reach their ends.
All inputs are finite; a program needn't handle non-finite values. No bound on the sum of `mask` on one device may be relied on, other than what follows from the above.
Results may differ from the reference program's by a relative error of at most 0.0001.
Values sent between devices are 32-bit elements; how exact they have to be, the bound alone decides.
A program may use at most 64 MiB of HBM per device.

```python
import math
import jax
import jax.numpy as jnp
from jax import lax

FS = 4
FINE_ITERS = 2
NLAT = 512
NLON = 2048
NSTEPS = 32
N_TM = 8


def draw_forcing(key, part):
    lat_pos = jnp.arange(NLAT, dtype=jnp.float32) / (NLAT - 1)
    lon_pos = jnp.arange(NLON, dtype=jnp.float32) / (NLON - 1)
    scale = (0.5 * 3.0 ** lat_pos)[:, None] * (1.0 + 2.0 * lon_pos)[None, :]
    noise = jax.random.truncated_normal(key, -3.0, 3.0, (NSTEPS, NLAT, NLON), jnp.float32)
    return noise * scale[None]


def with_ends(values, stream_key, least, high):
    place = [jax.random.randint(jax.random.fold_in(stream_key, axis), (), 0, length) for axis, length in enumerate(values.shape)]
    main_axis = values.shape.index(max(values.shape))
    beside = place[:main_axis] + [(place[main_axis] + 1) % values.shape[main_axis]] + place[main_axis + 1:]
    return values.at[tuple(place)].set(least).at[tuple(beside)].set(high)


def shard_levels(key, shape, shards, least, largest):
    def one(dim, shards_of):
        draws = jax.random.uniform(jax.random.fold_in(jax.random.fold_in(key, 6), dim), (shards_of,), jnp.float32, least / len(shards), largest / len(shards))
        return jnp.repeat(jnp.exp(draws), shape[dim] // shards_of).reshape((-1,) + (1,) * (len(shape) - dim - 1))

    factor_of = one(*shards[0])
    for cut in shards[1:]:
        factor_of = factor_of * one(*cut)
    return factor_of


def normal_values(own_key, extent, deviation, most, shards=(), kind=jnp.bfloat16):
    loudness = shard_levels(own_key, extent, shards, -0.22, 0.18) if shards else 1.0
    drawn = jax.random.normal(own_key, extent, jnp.float32) * deviation * loudness
    return jnp.minimum(jnp.maximum(drawn, -most), most).astype(kind)


def setup_inputs(seed: int = 0) -> dict:
    streams_of = jax.random.split(jax.random.key(seed), 5)
    return {
        "forcing": draw_forcing(jax.random.fold_in(streams_of[4], 71), 0),
        "depth": jnp.clip(jnp.exp(math.log(2.0) - 2.3025851 * jax.random.uniform(streams_of[1], (NLAT, NLON), jnp.float32) ** shard_levels(streams_of[1], (NLAT, NLON), ((0, 4), (1, 4)), -0.2, 0.2)), 0.2, 2.0),
        "mask": with_ends((jax.random.randint(streams_of[2], (NLAT, NLON), 0, 10) < 7).astype(jnp.int32), jax.random.fold_in(streams_of[2], 1), 0, 1),
        "guess": normal_values(streams_of[3], (N_TM, NLAT, NLON), 1.0, 6.0, ((0, 8), (1, 4), (2, 4)), jnp.float32),
    }


COUPLING = 3.0
EPSILON = 1e-6


def face_terms(depth, mask):
    wet = mask.astype(jnp.float32)
    east = COUPLING * wet * jnp.roll(wet, -1, 1) * 0.5 * (depth + jnp.roll(depth, -1, 1))
    north = COUPLING * wet[:-1] * wet[1:] * 0.5 * (depth[:-1] + depth[1:])
    return east, north


def apply_op(field, east, north, factor):
    flux_east = east * (field - jnp.roll(field, -1, 1))
    spread = flux_east - jnp.roll(flux_east, 1, 1)
    flux_north = north * (field[:-1] - field[1:])
    zero_row = jnp.zeros((1, field.shape[1]), jnp.float32)
    spread = spread + jnp.concatenate([flux_north, zero_row], 0) - jnp.concatenate([zero_row, flux_north], 0)
    return field + factor * spread


def solve(source, east, north, factor, count):
    solution = jnp.zeros_like(source)
    residual = source
    direction = source
    norm_now = jnp.sum(residual * residual)
    for level in range(count):
        image = apply_op(direction, east, north, factor)
        alpha = norm_now / (jnp.sum(direction * image) + EPSILON)
        solution = solution + alpha * direction
        residual = residual - alpha * image
        if level + 1 < count:
            norm_next = jnp.sum(residual * residual)
            direction = residual + (norm_next / (norm_now + EPSILON)) * direction
            norm_now = norm_next
    return solution


def reference(forcing, depth, mask, guess):
    east, north = face_terms(depth, mask)

    def fine(value):
        return solve(value, east, north, 1.0, FINE_ITERS)

    def coarse(value):
        return solve(value, east, north, float(FS), 1)

    slabs = forcing.reshape(N_TM, FS, NLAT, NLON)
    empty = jnp.zeros((), jnp.float32)

    def relax(carry, inputs):
        start, terms = inputs
        value = start
        for level in range(FS - 1, 0, -1):
            value = fine(value) + terms[level]
        finished = fine(value) + terms[0]
        return carry, finished - coarse(start)

    _, offsets = lax.scan(relax, empty, (guess, slabs))

    def chain(upper, offset):
        here = coarse(upper) + offset
        return here, (upper, here)

    _, (uppers, heres) = lax.scan(chain, guess[N_TM - 1], offsets, reverse=True)

    def correct(carry, inputs):
        upper, here, terms = inputs
        value = upper
        later = []
        for level in range(FS - 1, 0, -1):
            value = fine(value) + terms[level]
            later.append(value)
        return carry, jnp.stack([here] + later[::-1])

    _, result = lax.scan(correct, empty, (uppers, heres, slabs))
    return result.reshape(NSTEPS, NLAT, NLON)
```

```python
import functools

import jax
import jax.numpy as jnp
from jax import lax
from jax.experimental import pallas as pl
from jax.experimental.pallas import tpu as pltpu
from jax.sharding import PartitionSpec as P

FS = 4
EPS = 1e-6
MESH = pl.DeviceIdType.MESH

TILES, ROWS, LANES = 5, 160, 128
TOP, LOW, END = 8, 16, 144
FULL = ((8, 48), (56, 48), (104, 48))
OWN = ((16, 64), (80, 64))
DM, CG, G3, G2, G1, G0 = range(6)


def lane_iota(shape):
    return lax.broadcasted_iota(jnp.int32, shape, len(shape) - 1)


def sides(ref, row, count):
    v = ref[:, row : row + count, :]
    down = ref[:, row + 1 : row + 1 + count, :]
    up = ref[:, row - 1 : row - 1 + count, :]
    lane = lane_iota(v.shape)
    ahead = pltpu.roll(v, LANES - 1, 2)
    right = jnp.where(lane == LANES - 1, jnp.concatenate([ahead[1:], ahead[:1]], 0), ahead)
    behind = pltpu.roll(v, 1, 2)
    left = jnp.where(lane == 0, jnp.concatenate([behind[-1:], behind[:-1]], 0), behind)
    return v, right, left, down, up


def spread(ref, coef, row, count):
    v, right, left, down, up = sides(ref, row, count)
    part = slice(row, row + count)
    out = coef[0, :, part, :] * (v - right) + coef[1, :, part, :] * (v - left)
    out = out + coef[2, :, part, :] * (v - down) + coef[3, :, part, :] * (v - up)
    return v, out


def own_part(x, row, count):
    first, last = max(row, LOW) - row, min(row + count, END) - row
    return x[:4, first:last, :]


def fold(x):
    return jnp.sum(x.reshape(-1, 8, LANES), axis=0)


class Sums:
    def __init__(self):
        self.terms = {}

    def add(self, key, a, b):
        value = fold(a * b)
        self.terms[key] = value if key not in self.terms else self.terms[key] + value


def fine_coefs(m):
    den = m[0] + m[1] + EPS
    alpha = m[0] / den
    gamma = (m[1] + EPS) / den
    s1 = jnp.maximum(
        gamma * gamma * m[0] - 2.0 * gamma * alpha * m[1] + alpha * alpha * m[2], 0.0
    )
    beta = s1 / (m[0] + EPS)
    f = gamma + beta
    pp = s1 + beta * (2.0 * EPS * alpha + beta * m[0])
    plp = jnp.maximum(f * f * m[1] - 2.0 * f * alpha * m[2] + alpha * alpha * m[3], 0.0)
    later = jnp.minimum(s1 / (pp + plp + EPS), 1.0)
    return alpha + later * f, -alpha * later


def kernel(
    forcing, depth, mask, guess, out,
    F, K, V, X, U, W, LG, TG, UG, WG, DEP, MSK, OUT, KAP, ROW,
    PKS, PKR, CKS, CKR, PT, MSG, AR,
    in_sem, hs, hr, ar_s, ar_r, ts, tr, tps, tpr, fs, fps, out_sem,
):
    tm = lax.axis_index("tm")
    lat = lax.axis_index("lat")
    lon = lax.axis_index("lon")
    me = lat * 4 + lon
    chip, core = tm // 2, tm % 2
    sib = 2 * chip + 1 - core

    def cols(c):
        return pl.ds(LANES * c, LANES)

    loads = []
    own_rows = pl.ds(LOW, END - LOW)

    def load(src, dst, field, c):
        copy = pltpu.make_async_copy(src, dst, in_sem.at[field, c])
        copy.start()
        loads.append(copy)

    for c in range(4):
        load(depth.at[:, cols(c)], DEP.at[c], 0, c)
        load(mask.at[:, cols(c)], MSK.at[c], 1, c)
    for c in range(4):
        load(guess.at[0, :, cols(c)], F.at[CG, c, own_rows, :], 2, c)
    for field, level in ((G3, 3), (G2, 2), (G1, 1), (G0, 0)):
        for c in range(4):
            load(forcing.at[level, :, cols(c)], F.at[field, c, own_rows, :], 3 + level, c)

    barrier = pltpu.get_barrier_semaphore()

    def greet(step, _):
        there = lax.rem(me + step, 16)
        pl.semaphore_signal(
            barrier, inc=1, device_id={"lat": there // 4, "lon": there % 4}, device_id_type=MESH
        )
        return 0

    lax.fori_loop(1, 16, greet, 0)
    for step in (2, 4, 6):
        pl.semaphore_signal(
            barrier, inc=1, device_id={"tm": lax.rem(tm + step, 8)}, device_id_type=MESH
        )
    pl.semaphore_signal(barrier, inc=1, device_id={"tm": sib}, device_id_type=MESH)

    def clear(ref):
        zero = jnp.zeros((TILES, 8, LANES), jnp.float32)
        ref[:, 0:8, :] = zero
        ref[:, 152:160, :] = zero

    def clear_fields(i, _):
        clear(F.at[i])
        return 0

    lax.fori_loop(0, 6, clear_fields, 0)
    for ref in (V, X, U):
        clear(ref)

    def clear_slab(i, _):
        clear(TG.at[i])

        @pl.when(i <= tm)
        def _():
            TG[i, :, TOP:152, :] = jnp.zeros((TILES, 144, LANES), jnp.float32)

        ROW[:, i] = jnp.zeros((4, 8, LANES), jnp.float32)
        return 0

    lax.fori_loop(0, 8, clear_slab, 0)

    for copy in loads:
        copy.wait()
    for c in range(4):
        F[DM, c, LOW:END, :] = jnp.where(MSK[c] > 0, DEP[c], 0.0)

    lane6 = lane_iota((6, 8, LANES))
    right_edge = jnp.zeros((6, 8, LANES), jnp.float32)
    left_edge = jnp.zeros((6, 8, LANES), jnp.float32)
    for t in range(16):
        here = (lane6 >= 8 * t) & (lane6 < 8 * t + 8)
        rows = slice(LOW + 8 * t, LOW + 8 * t + 8)
        right_edge = jnp.where(here, pltpu.roll(F[:, 3, rows, :], (8 * t + 8) % LANES, 2), right_edge)
        left_edge = jnp.where(here, pltpu.roll(F[:, 0, rows, :], 8 * t, 2), left_edge)
    PKS[0] = right_edge
    PKS[1] = left_edge
    lane1 = lane_iota((8, LANES))
    corners = ((136, 3, 8), (136, 0, 0), (16, 3, 8), (16, 0, 0))
    for i, (row, tile, shift) in enumerate(corners):
        packed = jnp.zeros((8, LANES), jnp.float32)
        for f in range(6):
            here = (lane1 >= 8 * f) & (lane1 < 8 * f + 8)
            edge = pltpu.roll(F[f, tile, row : row + 8, :], (8 * f + shift) % LANES, 1)
            packed = jnp.where(here, edge, packed)
        CKS[i] = packed

    pl.semaphore_wait(barrier, 19)

    north, south = lax.rem(lat + 3, 4), lax.rem(lat + 1, 4)
    west, east = lax.rem(lon + 3, 4), lax.rem(lon + 1, 4)
    halos = []

    def push(src, dst, i, target):
        copy = pltpu.make_async_remote_copy(
            src, dst, hs.at[i], hr.at[i], device_id=target, device_id_type=MESH
        )
        copy.start()
        halos.append(copy)

    targets = ((south, east), (south, west), (north, east), (north, west))
    for i, (a, b) in enumerate(targets):
        push(CKS.at[i], CKR.at[i], i, {"lat": a, "lon": b})
    push(PKS.at[0], PKR.at[0], 4, {"lon": east})
    push(PKS.at[1], PKR.at[1], 5, {"lon": west})
    for i, first in ((6, 0), (8, 3)):
        group = pl.ds(first, 3)
        push(
            F.at[group, pl.ds(0, 4), pl.ds(136, 8), :],
            F.at[group, pl.ds(0, 4), pl.ds(8, 8), :],
            i, {"lat": south},
        )
        push(
            F.at[group, pl.ds(0, 4), pl.ds(16, 8), :],
            F.at[group, pl.ds(0, 4), pl.ds(144, 8), :],
            i + 1, {"lat": north},
        )
    for copy in halos:
        copy.wait_recv()

    from_left, from_right = PKR[0], PKR[1]
    for t in range(16):
        rows = slice(LOW + 8 * t, LOW + 8 * t + 8)
        a = pltpu.roll(from_left, (120 - 8 * t) % LANES, 2)
        b = pltpu.roll(from_right, (LANES - 8 * t) % LANES, 2)
        F[:, 4, rows, :] = jnp.where(lane6 >= 120, a, jnp.where(lane6 < 8, b, 0.0))
    for row, left, right in ((8, 0, 1), (144, 2, 3)):
        a0, b0 = CKR[left], CKR[right]
        for f in range(6):
            a = pltpu.roll(a0, (120 - 8 * f) % LANES, 1)
            b = pltpu.roll(b0, (LANES - 8 * f) % LANES, 1)
            F[f, 4, row : row + 8, :] = jnp.where(lane1 >= 120, a, jnp.where(lane1 < 8, b, 0.0))

    inside_top = jnp.where(lat > 0, 1.0, 0.0).astype(jnp.float32)
    inside_end = jnp.where(lat < 3, 1.0, 0.0).astype(jnp.float32)
    F[DM, :, 8:16, :] = F[DM, :, 8:16, :] * inside_top
    F[DM, :, 144:152, :] = F[DM, :, 144:152, :] * inside_end

    for row, count in FULL:
        d, *around = sides(F.at[DM], row, count)
        for i, other in enumerate(around):
            K[i, :, row : row + count, :] = jnp.where(
                (d > 0.0) & (other > 0.0), 1.5 * (d + other), 0.0
            )

    def send_sums(r, message):
        MSG[r] = message
        AR[r, me] = message

        def one(step, _):
            there = lax.rem(me + step, 16)
            pltpu.make_async_remote_copy(
                MSG.at[r], AR.at[r, me], ar_s.at[r], ar_r.at[r],
                device_id={"lat": there // 4, "lon": there % 4}, device_id_type=MESH,
            ).start()
            return 0

        lax.fori_loop(1, 16, one, 0)

    def recv_sums(r):
        box = AR.at[r, pl.ds(0, 15)]
        pltpu.make_async_copy(box, box, ar_r.at[r]).wait()
        return jnp.sum(AR[r], axis=0)

    def rows_of(accs):
        row = lax.broadcasted_iota(jnp.int32, (16, LANES), 0)
        stacked = jnp.zeros((16, LANES), jnp.float32)
        for i, acc in enumerate(accs):
            stacked = jnp.where(row == i, jnp.sum(acc, axis=0, keepdims=True), stacked)
        return jnp.broadcast_to(jnp.sum(stacked, axis=1, keepdims=True), (16, LANES))

    def prepare(field, slot):
        sums = Sums()
        for row, count in FULL:
            g, lg = spread(F.at[field], K, row, count)
            LG[slot, :, row : row + count, :] = lg
            g, lg = own_part(g, row, count), own_part(lg, row, count)
            sums.add(0, g, g)
            sums.add(1, g, lg)
            sums.add(2, lg, lg)
        for row, count in OWN:
            lg, llg = spread(LG.at[slot], K, row, count)
            sums.add(3, lg[:4], llg[:4])
        for i in range(4):
            KAP[slot, i] = sums.terms[i]

    def two_steps(r, v_ref, field, slot, between):
        sums = Sums()
        for row, count in FULL:
            v, u = spread(v_ref, K, row, count)
            U[:, row : row + count, :] = u
            g = own_part(F[field, :, row : row + count, :], row, count)
            v, u = own_part(v, row, count), own_part(u, row, count)
            sums.add("m0", v, v)
            sums.add("m1", v, u)
            sums.add("m2", u, u)
            sums.add("n0", v, g)
            sums.add("n1", u, g)
        for row, count in FULL:
            u, w = spread(U, K, row, count)
            W[:, row : row + count, :] = w
            lg = own_part(LG[slot, :, row : row + count, :], row, count)
            u, w = own_part(u, row, count), own_part(w, row, count)
            sums.add("m3", u, w)
            sums.add("m4", w, w)
            sums.add("n2", u, lg)
            sums.add("n3", w, lg)
        for row, count in OWN:
            w, lw = spread(W, K, row, count)
            lg = LG[slot, :4, row : row + count, :]
            sums.add("m5", w[:4], lw[:4])
            sums.add("n4", lw[:4], lg)
        names = ["m0", "m1", "m2", "m3", "m4", "m5", "n0", "n1", "n2", "n3", "n4"]
        accs = [sums.terms[n] for n in names] + [KAP[slot, i] for i in range(4)]
        send_sums(r, rows_of(accs))
        between()
        total = recv_sums(r)
        at = [total[i : i + 1, :] for i in range(15)]
        m, n, k = at[:6], at[6:11], at[11:]
        a, b = fine_coefs(m)
        later = [
            jnp.maximum(
                a * a * m[i] + 2.0 * a * b * m[i + 1] + b * b * m[i + 2]
                + 2.0 * (a * n[i] + b * n[i + 1]) + k[i],
                0.0,
            )
            for i in range(4)
        ]
        a2, b2 = fine_coefs(later)
        return m, (a, b), (a2 * a, a2 * b + b2 * a, b2 * b, a2, b2)

    def scaled(s, x):
        return jnp.broadcast_to(s.reshape(1, 1, LANES), x.shape) * x

    prepare(G3, 0)
    m_start, _, c = two_steps(0, F.at[CG], G3, 0, lambda: prepare(G1, 1))
    for row, count in FULL:
        part = slice(row, row + count)
        X[:, part, :] = (
            scaled(c[0], F[CG, :, part, :]) + scaled(c[1], U[:, part, :]) + scaled(c[2], W[:, part, :])
            + scaled(c[3], F[G3, :, part, :]) + scaled(c[4], LG[0, :, part, :]) + F[G2, :, part, :]
        )
    last = jnp.where(tm == 7, 1.0, 0.0).astype(jnp.float32)
    psi = m_start[0] / (m_start[0] + 4.0 * m_start[1] + EPS)
    drop = psi * (last - 1.0)

    _, _, c = two_steps(1, X, G1, 1, lambda: prepare(G2, 2))
    for row, count in FULL:
        part = slice(row, row + count)
        TG[tm, :, part, :] = (
            scaled(c[0], X[:, part, :]) + scaled(c[1], U[:, part, :]) + scaled(c[2], W[:, part, :])
            + scaled(c[3], F[G1, :, part, :]) + scaled(c[4], LG[1, :, part, :]) + F[G0, :, part, :]
            + scaled(drop, F[CG, :, part, :])
        )

    lane2 = lane_iota((8, LANES))
    for half in range(2):
        packed = jnp.zeros((8, LANES), jnp.float32)
        for t in range(9):
            row = TOP + 8 * (9 * half + t)
            here = (lane2 >= 8 * t) & (lane2 < 8 * t + 8)
            packed = jnp.where(here, pltpu.roll(TG[tm, 4, row : row + 8, :], 8 * t + 4, 1), packed)
        PT[tm, 8 * half : 8 * half + 8, :] = packed

    def slab_copies(k, s_main, s_pack, target):
        main = TG.at[k, pl.ds(0, 4), pl.ds(TOP, 144), :]
        return (
            pltpu.make_async_remote_copy(
                main, main, s_main, tr.at[k], device_id={"tm": target}, device_id_type=MESH
            ),
            pltpu.make_async_remote_copy(
                PT.at[k], PT.at[k], s_pack, tpr.at[k], device_id={"tm": target}, device_id_type=MESH
            ),
        )

    def each_send(act):
        @pl.when(core == 1)
        def _():
            for copy in slab_copies(tm, ts.at[0], tps.at[0], sib):
                act(copy)

        for dx in (1, 3, 2):
            @pl.when(chip >= dx)
            def _():
                for copy in slab_copies(tm, ts.at[dx], tps.at[dx], jnp.maximum(tm - 2 * dx, 0)):
                    act(copy)

    each_send(lambda copy: copy.start())

    def slab_at(e):
        h = (e + 1) // 2
        dx = jnp.where(h == 1, 1, jnp.where(h == 2, 3, 2))
        same = e % 2
        k = jnp.where(e == 0, tm + 1, jnp.where(same == 1, tm, sib) + 2 * dx)
        valid = jnp.where(e == 0, core == 0, chip + dx <= 3)
        return jnp.minimum(k, 7), dx, valid

    def arrive(e, _):
        k, dx, valid = slab_at(e)

        @pl.when(valid)
        def _():
            for copy in slab_copies(k, ts.at[0], tps.at[0], sib):
                copy.wait_recv()

            @pl.when(e % 2 == 1)
            def _():
                for copy in slab_copies(k, fs.at[dx], fps.at[dx], sib):
                    copy.start()

            for half in range(2):
                packed = PT[k, 8 * half : 8 * half + 8, :]
                for t in range(9):
                    row = TOP + 8 * (9 * half + t)
                    back = pltpu.roll(packed, (LANES - 8 * t - 4) % LANES, 1)
                    TG[k, 4, row : row + 8, :] = jnp.where((lane2 < 4) | (lane2 >= 124), back, 0.0)
            for row, count in FULL:
                _, u = spread(TG.at[k], K, row, count)
                UG[k, :, row : row + count, :] = u
            for row, count in OWN:
                _, w = spread(UG.at[k], K, row, count)
                WG[:, row - LOW : row - LOW + count, :] = w[:4]

            def pair(q, _):
                j, _, held = slab_at(q)

                @pl.when(held)
                def _():
                    sums = Sums()
                    for t in range(4):
                        tk, uk, wk = TG[k, t, LOW:END, :], UG[k, t, LOW:END, :], WG[t]
                        tj, uj = TG[j, t, LOW:END, :], UG[j, t, LOW:END, :]
                        sums.add(0, tj, tk)
                        sums.add(1, tj, uk)
                        sums.add(2, uj, uk)
                        sums.add(3, uj, wk)
                    for i in range(4):
                        value = jnp.sum(sums.terms[i], axis=0, keepdims=True)
                        ROW[i, k, pl.ds(j, 1), :] = value
                        ROW[i, j, pl.ds(k, 1), :] = value

                return 0

            lax.fori_loop(0, e + 1, pair, 0)

        return 0

    lax.fori_loop(0, 7, arrive, 0)

    lane3 = lane_iota((8, 8, LANES))
    sub3 = lax.broadcasted_iota(jnp.int32, (8, 8, LANES), 1)
    gram = jnp.zeros((8, 8, LANES), jnp.float32)
    for i in range(4):
        gram = jnp.where(lane3 == 8 * i + sub3, jnp.sum(ROW[i], axis=2, keepdims=True), gram)
    gram = jnp.sum(gram, axis=1)
    send_sums(2, jnp.concatenate([gram, jnp.zeros((8, LANES), jnp.float32)], 0))
    total = recv_sums(2)[:8]

    lane = lane_iota((8, LANES))
    table = [
        [
            None if j == 0 else jnp.broadcast_to(
                jnp.sum(jnp.where(lane == 8 * i + j, total, 0.0), axis=1, keepdims=True), (8, LANES)
            )
            for j in range(8)
        ]
        for i in range(4)
    ]

    def entry(i, k, j):
        return table[i][j][k : k + 1, :]

    one = jnp.ones((1, LANES), jnp.float32)
    zero = jnp.zeros((1, LANES), jnp.float32)
    coefs = {7: one}
    quad = [entry(i, 7, 7) for i in range(4)]
    cross = [{j: entry(i, 7, j) for j in range(1, 7)} for i in range(4)]
    is_last = jnp.full((1, LANES), tm == 7)
    held_c = {k: zero for k in range(1, 8)}
    held_q = [m_start[i] for i in range(4)]
    for t in range(7, 0, -1):
        if t < 7:
            psi_t = quad[0] / (quad[0] + 4.0 * quad[1] + EPS)
            quad = [
                psi_t * psi_t * quad[i] + 2.0 * psi_t * cross[i][t] + entry(i, t, t)
                for i in range(4)
            ]
            cross = [{j: psi_t * cross[i][j] + entry(i, t, j) for j in range(1, t)} for i in range(4)]
            coefs = {k: psi_t * x for k, x in coefs.items()}
            coefs[t] = one
        now = jnp.full((1, LANES), tm + 1 == t)
        for k in coefs:
            held_c[k] = jnp.where(now, coefs[k], held_c[k])
        held_q = [jnp.where(now, quad[i], held_q[i]) for i in range(4)]
    psi = held_q[0] / (held_q[0] + 4.0 * held_q[1] + EPS)
    psi = jnp.where(is_last, 0.0, psi)
    for row, count in FULL:
        part = slice(row, row + count)
        value = F[CG, :, part, :] * last
        for k in range(1, 8):
            value = value + scaled(held_c[k], TG[k, :, part, :])
        V[:, part, :] = value

    outs = []

    def put(level):
        for c in range(4):
            copy = pltpu.make_async_copy(
                OUT.at[level, c], out.at[level, :, cols(c)], out_sem.at[level, c]
            )
            copy.start()
            outs.append(copy)

    a, b = fine_coefs(held_q)
    for row, count in FULL:
        part = slice(row, row + count)
        v, u = spread(V, K, row, count)
        value = scaled(a, v) + scaled(b, u) + F[G3, :, part, :]
        X[:, part, :] = value
        first, end = max(row, LOW) - LOW, min(row + count, END) - LOW
        OUT[3, :, first:end, :] = own_part(value, row, count)
    put(3)

    def write_first():
        for row, count in OWN:
            part = slice(row, row + count)
            value = scaled(psi, V[:4, part, :]) + TG[tm, :4, part, :]
            OUT[0, :, row - LOW : row - LOW + count, :] = value
        put(0)

    _, (a, b), c = two_steps(3, X, G2, 2, write_first)
    for row, count in OWN:
        part = slice(row, row + count)
        inner = slice(row - LOW, row - LOW + count)
        v, u, w = X[:4, part, :], U[:4, part, :], W[:4, part, :]
        g = F[G2, :4, part, :]
        OUT[2, :, inner, :] = scaled(a, v) + scaled(b, u) + g
        OUT[1, :, inner, :] = (
            scaled(c[0], v) + scaled(c[1], u) + scaled(c[2], w) + scaled(c[3], g)
            + scaled(c[4], LG[2, :4, part, :]) + F[G1, :4, part, :]
        )
    put(2)
    put(1)

    for copy in halos:
        copy.wait_send()
    for r in range(4):
        box = AR.at[r, pl.ds(0, 15)]
        pltpu.make_async_copy(box, box, ar_s.at[r]).wait()
    each_send(lambda copy: copy.wait_send())
    for dx in (1, 3, 2):
        @pl.when(chip + dx <= 3)
        def _():
            for copy in slab_copies(jnp.minimum(tm + 2 * dx, 7), fs.at[dx], fps.at[dx], sib):
                copy.wait_send()
    for copy in outs:
        copy.wait()


def local(forcing, depth, mask, guess):
    f32 = jnp.float32
    field = (TILES, ROWS, LANES)
    dma = pltpu.SemaphoreType.DMA
    return pl.pallas_call(
        kernel,
        out_shape=jax.ShapeDtypeStruct(forcing.shape, f32),
        in_specs=[pl.BlockSpec(memory_space=pl.ANY)] * 4,
        out_specs=pl.BlockSpec(memory_space=pl.ANY),
        scratch_shapes=[
            pltpu.VMEM((6, *field), f32),
            pltpu.VMEM((4, *field), f32),
            pltpu.VMEM(field, f32),
            pltpu.VMEM(field, f32),
            pltpu.VMEM(field, f32),
            pltpu.VMEM(field, f32),
            pltpu.VMEM((3, *field), f32),
            pltpu.VMEM((8, *field), f32),
            pltpu.VMEM((8, *field), f32),
            pltpu.VMEM((4, 128, LANES), f32),
            pltpu.VMEM((4, 128, LANES), f32),
            pltpu.VMEM((4, 128, LANES), jnp.int32),
            pltpu.VMEM((4, 4, 128, LANES), f32),
            pltpu.VMEM((3, 4, 8, LANES), f32),
            pltpu.VMEM((4, 8, 8, LANES), f32),
            pltpu.VMEM((2, 6, 8, LANES), f32),
            pltpu.VMEM((2, 6, 8, LANES), f32),
            pltpu.VMEM((4, 8, LANES), f32),
            pltpu.VMEM((4, 8, LANES), f32),
            pltpu.VMEM((8, 16, LANES), f32),
            pltpu.VMEM((4, 16, LANES), f32),
            pltpu.VMEM((4, 16, 16, LANES), f32),
            dma((7, 4)),
            dma((10,)),
            dma((10,)),
            dma((4,)),
            dma((4,)),
            dma((4,)),
            dma((8,)),
            dma((4,)),
            dma((8,)),
            dma((4,)),
            dma((4,)),
            dma((4, 4)),
        ],
        compiler_params=pltpu.CompilerParams(
            collective_id=0, has_side_effects=True, vmem_limit_bytes=48 * 1024 * 1024
        ),
        name="cycle",
    )(forcing, depth, mask, guess)


def solution(mesh):
    return jax.shard_map(
        local,
        mesh=mesh,
        in_specs=(P("tm", "lat", "lon"), P("lat", "lon"), P("lat", "lon"), P("tm", "lat", "lon")),
        out_specs=P("tm", "lat", "lon"),
        check_vma=False,
    )
```

```python
import functools

import jax
import jax.numpy as jnp
from jax import lax
from jax.experimental import pallas as pl
from jax.experimental.pallas import tpu as pltpu
from jax.sharding import PartitionSpec as P

FS = 4
EPS = 1e-6
VMEM_LIMIT = 40 * 1024 * 1024
MESH = pl.DeviceIdType.MESH

TILES, ROWS, LANES = 5, 160, 128
TOP, LOW, END = 8, 16, 144
FULL = ((8, 48), (56, 48), (104, 48))
OWN = ((16, 64), (80, 64))
DM, CG, G3, G2, G1, G0 = range(6)


def lane_iota(shape):
    return lax.broadcasted_iota(jnp.int32, shape, len(shape) - 1)


def sides(ref, row, count):
    v = ref[:, row : row + count, :]
    down = ref[:, row + 1 : row + 1 + count, :]
    up = ref[:, row - 1 : row - 1 + count, :]
    lane = lane_iota(v.shape)
    ahead = pltpu.roll(v, LANES - 1, 2)
    right = jnp.where(lane == LANES - 1, jnp.concatenate([ahead[1:], ahead[:1]], 0), ahead)
    behind = pltpu.roll(v, 1, 2)
    left = jnp.where(lane == 0, jnp.concatenate([behind[-1:], behind[:-1]], 0), behind)
    return v, right, left, down, up


def spread(ref, coef, row, count):
    v, right, left, down, up = sides(ref, row, count)
    part = slice(row, row + count)
    out = coef[0, :, part, :] * (v - right) + coef[1, :, part, :] * (v - left)
    out = out + coef[2, :, part, :] * (v - down) + coef[3, :, part, :] * (v - up)
    return v, out


def own_part(x, row, count):
    first, last = max(row, LOW) - row, min(row + count, END) - row
    return x[:4, first:last, :]


def fold(x):
    return jnp.sum(x.reshape(-1, 8, LANES), axis=0)


class Phase:
    def __init__(self):
        self.open = None

    def __call__(self, name):
        if self.open is not None:
            self.open.__exit__(None, None, None)
        self.open = jax.named_scope(name) if name else None
        if self.open is not None:
            self.open.__enter__()


class Sums:
    def __init__(self):
        self.terms = {}

    def add(self, key, a, b):
        value = fold(a * b)
        self.terms[key] = value if key not in self.terms else self.terms[key] + value


def fine_coefs(m):
    den = m[0] + m[1] + EPS
    alpha = m[0] / den
    gamma = (m[1] + EPS) / den
    s1 = jnp.maximum(
        gamma * gamma * m[0] - 2.0 * gamma * alpha * m[1] + alpha * alpha * m[2], 0.0
    )
    beta = s1 / (m[0] + EPS)
    f = gamma + beta
    pp = s1 + beta * (2.0 * EPS * alpha + beta * m[0])
    plp = jnp.maximum(f * f * m[1] - 2.0 * f * alpha * m[2] + alpha * alpha * m[3], 0.0)
    later = jnp.minimum(s1 / (pp + plp + EPS), 1.0)
    return alpha + later * f, -alpha * later


def kernel(
    forcing, depth, mask, guess, out,
    F, K, V, X, U, W, LG, TG, UG, WG, DEP, MSK, KAP, ROW,
    PKS, PKR, CKS, CKR, PT, MSG, AR,
    in_sem, hs, hr, ar_s, ar_r, ts, tr, tps, tpr, fs, fps,
):
    phase = Phase()
    phase("a0_load")
    tm = lax.axis_index("tm")
    lat = lax.axis_index("lat")
    lon = lax.axis_index("lon")
    me = lat * 4 + lon
    chip, core = tm // 2, tm % 2
    sib = 2 * chip + 1 - core

    def cols(c):
        return pl.ds(LANES * c, LANES)

    barrier = pltpu.get_barrier_semaphore()
    north, south = lax.rem(lat + 3, 4), lax.rem(lat + 1, 4)
    west, east = lax.rem(lon + 3, 4), lax.rem(lon + 1, 4)

    def greet(target):
        pl.semaphore_signal(barrier, inc=1, device_id=target, device_id_type=MESH)

    for a in (north, south):
        for b in (west, east):
            greet({"lat": a, "lon": b})
    for step in (4, 2, 6):
        greet({"tm": lax.rem(tm + step, 8)})
    for a in (north, south):
        greet({"lat": a})
    for b in (west, east):
        greet({"lon": b})
    greet({"tm": sib})

    loads = []
    own_rows = pl.ds(LOW, END - LOW)

    def load(src, dst, field, c):
        copy = pltpu.make_async_copy(src, dst, in_sem.at[field, c])
        copy.start()
        loads.append(copy)

    for c in range(4):
        load(depth.at[:, cols(c)], DEP.at[c], 0, c)
        load(mask.at[:, cols(c)], MSK.at[c], 1, c)
    for c in range(4):
        load(guess.at[0, :, cols(c)], F.at[CG, c, own_rows, :], 2, c)
    for field, level in ((G3, 3), (G2, 2), (G1, 1), (G0, 0)):
        for c in range(4):
            load(forcing.at[level, :, cols(c)], F.at[field, c, own_rows, :], 3 + level, c)

    phase("a1_clear")
    def clear(ref):
        zero = jnp.zeros((TILES, 8, LANES), jnp.float32)
        ref[:, 0:8, :] = zero
        ref[:, 152:160, :] = zero

    def clear_fields(i, _):
        clear(F.at[i])
        return 0

    lax.fori_loop(0, 6, clear_fields, 0)
    for ref in (V, X, U):
        clear(ref)

    def clear_slab(i, _):
        clear(TG.at[i])

        @pl.when(i <= tm)
        def _():
            TG[i, :, TOP:152, :] = jnp.zeros((TILES, 144, LANES), jnp.float32)

        ROW[:, i] = jnp.zeros((4, 8, LANES), jnp.float32)
        return 0

    lax.fori_loop(0, 8, clear_slab, 0)

    phase("a2_loadwait")
    for copy in loads:
        copy.wait()
    for c in range(4):
        F[DM, c, LOW:END, :] = jnp.where(MSK[c] > 0, DEP[c], 0.0)

    phase("a3_pack")
    lane6 = lane_iota((6, 8, LANES))
    right_edge = jnp.zeros((6, 8, LANES), jnp.float32)
    left_edge = jnp.zeros((6, 8, LANES), jnp.float32)
    for t in range(16):
        here = (lane6 >= 8 * t) & (lane6 < 8 * t + 8)
        rows = slice(LOW + 8 * t, LOW + 8 * t + 8)
        right_edge = jnp.where(here, pltpu.roll(F[:, 3, rows, :], (8 * t + 8) % LANES, 2), right_edge)
        left_edge = jnp.where(here, pltpu.roll(F[:, 0, rows, :], 8 * t, 2), left_edge)
    PKS[0] = right_edge
    PKS[1] = left_edge
    lane1 = lane_iota((8, LANES))
    corners = ((136, 3, 8), (136, 0, 0), (16, 3, 8), (16, 0, 0))
    for i, (row, tile, shift) in enumerate(corners):
        packed = jnp.zeros((8, LANES), jnp.float32)
        for f in range(6):
            here = (lane1 >= 8 * f) & (lane1 < 8 * f + 8)
            edge = pltpu.roll(F[f, tile, row : row + 8, :], (8 * f + shift) % LANES, 1)
            packed = jnp.where(here, edge, packed)
        CKS[i] = packed

    phase("a4_barrier")
    pl.semaphore_wait(barrier, 12)

    halos = []

    def push(src, dst, i, target):
        copy = pltpu.make_async_remote_copy(
            src, dst, hs.at[i], hr.at[i], device_id=target, device_id_type=MESH
        )
        copy.start()
        halos.append(copy)

    targets = ((south, east), (south, west), (north, east), (north, west))
    for i, (a, b) in enumerate(targets):
        push(CKS.at[i], CKR.at[i], i, {"lat": a, "lon": b})
    push(PKS.at[0], PKR.at[0], 4, {"lon": east})
    push(PKS.at[1], PKR.at[1], 5, {"lon": west})
    for i, first in ((6, 0), (8, 3)):
        group = pl.ds(first, 3)
        push(
            F.at[group, pl.ds(0, 4), pl.ds(136, 8), :],
            F.at[group, pl.ds(0, 4), pl.ds(8, 8), :],
            i, {"lat": south},
        )
        push(
            F.at[group, pl.ds(0, 4), pl.ds(16, 8), :],
            F.at[group, pl.ds(0, 4), pl.ds(144, 8), :],
            i + 1, {"lat": north},
        )
    phase("a5_halowait")
    for copy in halos[:8]:
        copy.wait_recv()

    phase("a6_unpack")
    from_left, from_right = PKR[0], PKR[1]
    for t in range(16):
        rows = slice(LOW + 8 * t, LOW + 8 * t + 8)
        a = pltpu.roll(from_left, (120 - 8 * t) % LANES, 2)
        b = pltpu.roll(from_right, (LANES - 8 * t) % LANES, 2)
        F[:, 4, rows, :] = jnp.where(lane6 >= 120, a, jnp.where(lane6 < 8, b, 0.0))
    for row, left, right in ((8, 0, 1), (144, 2, 3)):
        a0, b0 = CKR[left], CKR[right]
        for f in range(6):
            a = pltpu.roll(a0, (120 - 8 * f) % LANES, 1)
            b = pltpu.roll(b0, (LANES - 8 * f) % LANES, 1)
            F[f, 4, row : row + 8, :] = jnp.where(lane1 >= 120, a, jnp.where(lane1 < 8, b, 0.0))

    inside_top = jnp.where(lat > 0, 1.0, 0.0).astype(jnp.float32)
    inside_end = jnp.where(lat < 3, 1.0, 0.0).astype(jnp.float32)
    F[DM, :, 8:16, :] = F[DM, :, 8:16, :] * inside_top
    F[DM, :, 144:152, :] = F[DM, :, 144:152, :] * inside_end

    for row, count in FULL:
        d, *around = sides(F.at[DM], row, count)
        for i, other in enumerate(around):
            K[i, :, row : row + count, :] = jnp.where(
                (d > 0.0) & (other > 0.0), 1.5 * (d + other), 0.0
            )

    def send_sums(r, message):
        MSG[r] = message
        AR[r, me] = message

        def one(step, _):
            there = lax.rem(me + step, 16)
            pltpu.make_async_remote_copy(
                MSG.at[r], AR.at[r, me], ar_s.at[r], ar_r.at[r],
                device_id={"lat": there // 4, "lon": there % 4}, device_id_type=MESH,
            ).start()
            return 0

        lax.fori_loop(1, 16, one, 0)

    def recv_sums(r):
        box = AR.at[r, pl.ds(0, 15)]
        pltpu.make_async_copy(box, box, ar_r.at[r]).wait()
        return jnp.sum(AR[r], axis=0)

    def rows_of(accs):
        row = lax.broadcasted_iota(jnp.int32, (16, LANES), 0)
        stacked = jnp.zeros((16, LANES), jnp.float32)
        for i, acc in enumerate(accs):
            stacked = jnp.where(row == i, jnp.sum(acc, axis=0, keepdims=True), stacked)
        return jnp.broadcast_to(jnp.sum(stacked, axis=1, keepdims=True), (16, LANES))

    def prepare(field, slot):
        sums = Sums()
        for row, count in FULL:
            g, lg = spread(F.at[field], K, row, count)
            LG[slot, :, row : row + count, :] = lg
            g, lg = own_part(g, row, count), own_part(lg, row, count)
            sums.add(0, g, g)
            sums.add(1, g, lg)
            sums.add(2, lg, lg)
        for row, count in OWN:
            lg, llg = spread(LG.at[slot], K, row, count)
            sums.add(3, lg[:4], llg[:4])
        for i in range(4):
            KAP[slot, i] = sums.terms[i]

    def two_steps(r, v_ref, field, slot, between):
        phase(f"r{r}_moments")
        sums = Sums()
        for row, count in FULL:
            v, u = spread(v_ref, K, row, count)
            U[:, row : row + count, :] = u
            g = own_part(F[field, :, row : row + count, :], row, count)
            v, u = own_part(v, row, count), own_part(u, row, count)
            sums.add("m0", v, v)
            sums.add("m1", v, u)
            sums.add("m2", u, u)
            sums.add("n0", v, g)
            sums.add("n1", u, g)
        for row, count in FULL:
            u, w = spread(U, K, row, count)
            W[:, row : row + count, :] = w
            lg = own_part(LG[slot, :, row : row + count, :], row, count)
            u, w = own_part(u, row, count), own_part(w, row, count)
            sums.add("m3", u, w)
            sums.add("m4", w, w)
            sums.add("n2", u, lg)
            sums.add("n3", w, lg)
        for row, count in OWN:
            w, lw = spread(W, K, row, count)
            lg = LG[slot, :4, row : row + count, :]
            sums.add("m5", w[:4], lw[:4])
            sums.add("n4", lw[:4], lg)
        names = ["m0", "m1", "m2", "m3", "m4", "m5", "n0", "n1", "n2", "n3", "n4"]
        accs = [sums.terms[n] for n in names] + [KAP[slot, i] for i in range(4)]
        send_sums(r, rows_of(accs))
        phase(f"r{r}_between")
        between()
        phase(f"r{r}_wait")
        total = recv_sums(r)
        phase(f"r{r}_scalars")
        at = [total[i : i + 1, :] for i in range(15)]
        m, n, k = at[:6], at[6:11], at[11:]
        a, b = fine_coefs(m)
        later = [
            jnp.maximum(
                a * a * m[i] + 2.0 * a * b * m[i + 1] + b * b * m[i + 2]
                + 2.0 * (a * n[i] + b * n[i + 1]) + k[i],
                0.0,
            )
            for i in range(4)
        ]
        a2, b2 = fine_coefs(later)
        return m, (a, b), (a2 * a, a2 * b + b2 * a, b2 * b, a2, b2)

    def scaled(s, x):
        return jnp.broadcast_to(s.reshape(1, 1, LANES), x.shape) * x

    phase("a7_prepare")
    prepare(G3, 0)

    def rest_of_halo():
        for copy in halos[8:]:
            copy.wait_recv()
        prepare(G1, 1)

    m_start, _, c = two_steps(0, F.at[CG], G3, 0, rest_of_halo)
    for row, count in FULL:
        part = slice(row, row + count)
        X[:, part, :] = (
            scaled(c[0], F[CG, :, part, :]) + scaled(c[1], U[:, part, :]) + scaled(c[2], W[:, part, :])
            + scaled(c[3], F[G3, :, part, :]) + scaled(c[4], LG[0, :, part, :]) + F[G2, :, part, :]
        )
    last = jnp.where(tm == 7, 1.0, 0.0).astype(jnp.float32)
    psi = m_start[0] / (m_start[0] + 4.0 * m_start[1] + EPS)
    drop = psi * (last - 1.0)

    _, _, c = two_steps(1, X, G1, 1, lambda: prepare(G2, 2))
    for row, count in FULL:
        part = slice(row, row + count)
        TG[tm, :, part, :] = (
            scaled(c[0], X[:, part, :]) + scaled(c[1], U[:, part, :]) + scaled(c[2], W[:, part, :])
            + scaled(c[3], F[G1, :, part, :]) + scaled(c[4], LG[1, :, part, :]) + F[G0, :, part, :]
            + scaled(drop, F[CG, :, part, :])
        )

    phase("b0_gather")
    lane2 = lane_iota((8, LANES))
    for half in range(2):
        packed = jnp.zeros((8, LANES), jnp.float32)
        for t in range(9):
            row = TOP + 8 * (9 * half + t)
            here = (lane2 >= 8 * t) & (lane2 < 8 * t + 8)
            packed = jnp.where(here, pltpu.roll(TG[tm, 4, row : row + 8, :], 8 * t + 4, 1), packed)
        PT[tm, 8 * half : 8 * half + 8, :] = packed

    def slab_copies(k, s_main, s_pack, target):
        main = TG.at[k, pl.ds(0, 4), pl.ds(TOP, 144), :]
        return (
            pltpu.make_async_remote_copy(
                main, main, s_main, tr.at[k], device_id={"tm": target}, device_id_type=MESH
            ),
            pltpu.make_async_remote_copy(
                PT.at[k], PT.at[k], s_pack, tpr.at[k], device_id={"tm": target}, device_id_type=MESH
            ),
        )

    def each_send(act):
        @pl.when(core == 1)
        def _():
            for copy in slab_copies(tm, ts.at[0], tps.at[0], sib):
                act(copy)

        for dx in (1, 3, 2):
            @pl.when(chip >= dx)
            def _():
                for copy in slab_copies(tm, ts.at[dx], tps.at[dx], jnp.maximum(tm - 2 * dx, 0)):
                    act(copy)

    each_send(lambda copy: copy.start())

    def slab_at(e):
        h = (e + 1) // 2
        dx = jnp.where(h == 1, 1, jnp.where(h == 2, 3, 2))
        same = e % 2
        k = jnp.where(e == 0, tm + 1, jnp.where(same == 1, tm, sib) + 2 * dx)
        valid = jnp.where(e == 0, core == 0, chip + dx <= 3)
        return jnp.minimum(k, 7), dx, valid

    def arrive(e, _):
        k, dx, valid = slab_at(e)

        @pl.when(valid)
        def _():
            with jax.named_scope("b1_slabwait"):
                for copy in slab_copies(k, ts.at[0], tps.at[0], sib):
                    copy.wait_recv()

            @pl.when(e % 2 == 1)
            def _():
                for copy in slab_copies(k, fs.at[dx], fps.at[dx], sib):
                    copy.start()

            for half in range(2):
                packed = PT[k, 8 * half : 8 * half + 8, :]
                for t in range(9):
                    row = TOP + 8 * (9 * half + t)
                    back = pltpu.roll(packed, (LANES - 8 * t - 4) % LANES, 1)
                    TG[k, 4, row : row + 8, :] = jnp.where((lane2 < 4) | (lane2 >= 124), back, 0.0)
            for row, count in FULL:
                _, u = spread(TG.at[k], K, row, count)
                UG[k, :, row : row + count, :] = u
            for row, count in OWN:
                _, w = spread(UG.at[k], K, row, count)
                WG[:, row - LOW : row - LOW + count, :] = w[:4]

            def pair(q, _):
                j, _, held = slab_at(q)

                @pl.when(held)
                def _():
                    sums = Sums()
                    for t in range(4):
                        tk, uk, wk = TG[k, t, LOW:END, :], UG[k, t, LOW:END, :], WG[t]
                        tj, uj = TG[j, t, LOW:END, :], UG[j, t, LOW:END, :]
                        sums.add(0, tj, tk)
                        sums.add(1, tj, uk)
                        sums.add(2, uj, uk)
                        sums.add(3, uj, wk)
                    for i in range(4):
                        value = jnp.sum(sums.terms[i], axis=0, keepdims=True)
                        ROW[i, k, pl.ds(j, 1), :] = value
                        ROW[i, j, pl.ds(k, 1), :] = value

                return 0

            lax.fori_loop(0, e + 1, pair, 0)

        return 0

    phase("b1_arrive")
    lax.fori_loop(0, 7, arrive, 0)

    phase("b2_gram")
    lane3 = lane_iota((8, 8, LANES))
    sub3 = lax.broadcasted_iota(jnp.int32, (8, 8, LANES), 1)
    gram = jnp.zeros((8, 8, LANES), jnp.float32)
    for i in range(4):
        gram = jnp.where(lane3 == 8 * i + sub3, jnp.sum(ROW[i], axis=2, keepdims=True), gram)
    gram = jnp.sum(gram, axis=1)
    send_sums(2, jnp.concatenate([gram, jnp.zeros((8, LANES), jnp.float32)], 0))
    phase("b3_wait")
    total = recv_sums(2)[:8]
    phase("b4_chain")

    lane = lane_iota((8, LANES))
    table = [
        [
            None if j == 0 else jnp.broadcast_to(
                jnp.sum(jnp.where(lane == 8 * i + j, total, 0.0), axis=1, keepdims=True), (8, LANES)
            )
            for j in range(8)
        ]
        for i in range(4)
    ]

    def entry(i, k, j):
        return table[i][j][k : k + 1, :]

    one = jnp.ones((1, LANES), jnp.float32)
    zero = jnp.zeros((1, LANES), jnp.float32)
    coefs = {7: one}
    quad = [entry(i, 7, 7) for i in range(4)]
    cross = [{j: entry(i, 7, j) for j in range(1, 7)} for i in range(4)]
    is_last = jnp.full((1, LANES), tm == 7)
    held_c = {k: zero for k in range(1, 8)}
    held_q = [m_start[i] for i in range(4)]
    for t in range(7, 0, -1):
        if t < 7:
            psi_t = quad[0] / (quad[0] + 4.0 * quad[1] + EPS)
            quad = [
                psi_t * psi_t * quad[i] + 2.0 * psi_t * cross[i][t] + entry(i, t, t)
                for i in range(4)
            ]
            cross = [{j: psi_t * cross[i][j] + entry(i, t, j) for j in range(1, t)} for i in range(4)]
            coefs = {k: psi_t * x for k, x in coefs.items()}
            coefs[t] = one
        now = jnp.full((1, LANES), tm + 1 == t)
        for k in coefs:
            held_c[k] = jnp.where(now, coefs[k], held_c[k])
        held_q = [jnp.where(now, quad[i], held_q[i]) for i in range(4)]
    psi = held_q[0] / (held_q[0] + 4.0 * held_q[1] + EPS)
    psi = jnp.where(is_last, 0.0, psi)
    for row, count in FULL:
        part = slice(row, row + count)
        value = F[CG, :, part, :] * last
        for k in range(1, 8):
            value = value + scaled(held_c[k], TG[k, :, part, :])
        V[:, part, :] = value

    def put(level, row, value):
        for t in range(4):
            out[level, row - LOW : row - LOW + value.shape[1], cols(t)] = value[t]

    phase("c0_correct")
    a, b = fine_coefs(held_q)
    for row, count in FULL:
        part = slice(row, row + count)
        v, u = spread(V, K, row, count)
        value = scaled(a, v) + scaled(b, u) + F[G3, :, part, :]
        X[:, part, :] = value
        put(3, max(row, LOW), own_part(value, row, count))

    def write_first():
        for row, count in OWN:
            part = slice(row, row + count)
            put(0, row, scaled(psi, V[:4, part, :]) + TG[tm, :4, part, :])

    _, (a, b), c = two_steps(3, X, G2, 2, write_first)
    for row, count in OWN:
        part = slice(row, row + count)
        v, u, w = X[:4, part, :], U[:4, part, :], W[:4, part, :]
        g = F[G2, :4, part, :]
        put(2, row, scaled(a, v) + scaled(b, u) + g)
        last_value = (
            scaled(c[0], v) + scaled(c[1], u) + scaled(c[2], w) + scaled(c[3], g)
            + scaled(c[4], LG[2, :4, part, :]) + F[G1, :4, part, :]
        )
        put(1, row, last_value)

    phase("c9_end")
    for copy in halos:
        copy.wait_send()
    for r in range(4):
        box = AR.at[r, pl.ds(0, 15)]
        pltpu.make_async_copy(box, box, ar_s.at[r]).wait()
    each_send(lambda copy: copy.wait_send())
    for dx in (1, 3, 2):
        @pl.when(chip + dx <= 3)
        def _():
            for copy in slab_copies(jnp.minimum(tm + 2 * dx, 7), fs.at[dx], fps.at[dx], sib):
                copy.wait_send()
    phase(None)


def local(forcing, depth, mask, guess):
    f32 = jnp.float32
    field = (TILES, ROWS, LANES)
    dma = pltpu.SemaphoreType.DMA
    return pl.pallas_call(
        kernel,
        out_shape=jax.ShapeDtypeStruct(forcing.shape, f32),
        in_specs=[pl.BlockSpec(memory_space=pltpu.HBM)] * 4,
        out_specs=pl.BlockSpec(memory_space=pltpu.VMEM),
        scratch_shapes=[
            pltpu.VMEM((6, *field), f32),
            pltpu.VMEM((4, *field), f32),
            pltpu.VMEM(field, f32),
            pltpu.VMEM(field, f32),
            pltpu.VMEM(field, f32),
            pltpu.VMEM(field, f32),
            pltpu.VMEM((3, *field), f32),
            pltpu.VMEM((8, *field), f32),
            pltpu.VMEM((8, *field), f32),
            pltpu.VMEM((4, 128, LANES), f32),
            pltpu.VMEM((4, 128, LANES), f32),
            pltpu.VMEM((4, 128, LANES), jnp.int32),
            pltpu.VMEM((3, 4, 8, LANES), f32),
            pltpu.VMEM((4, 8, 8, LANES), f32),
            pltpu.VMEM((2, 6, 8, LANES), f32),
            pltpu.VMEM((2, 6, 8, LANES), f32),
            pltpu.VMEM((4, 8, LANES), f32),
            pltpu.VMEM((4, 8, LANES), f32),
            pltpu.VMEM((8, 16, LANES), f32),
            pltpu.VMEM((4, 16, LANES), f32),
            pltpu.VMEM((4, 16, 16, LANES), f32),
            dma((7, 4)),
            dma((10,)),
            dma((10,)),
            dma((4,)),
            dma((4,)),
            dma((4,)),
            dma((8,)),
            dma((4,)),
            dma((8,)),
            dma((4,)),
            dma((4,)),
        ],
        compiler_params=pltpu.CompilerParams(
            collective_id=0, has_side_effects=True, vmem_limit_bytes=VMEM_LIMIT
        ),
        name="cycle",
    )(*(pltpu.with_memory_space_constraint(x, pltpu.HBM) for x in (forcing, depth, mask, guess)))


def solution(mesh):
    return jax.shard_map(
        local,
        mesh=mesh,
        in_specs=(P("tm", "lat", "lon"), P("lat", "lon"), P("lat", "lon"), P("tm", "lat", "lon")),
        out_specs=P("tm", "lat", "lon"),
        check_vma=False,
    )
```

```python
import functools

import jax
import jax.numpy as jnp
from jax import lax
from jax.experimental import pallas as pl
from jax.experimental.pallas import tpu as pltpu
from jax.sharding import PartitionSpec as P

FS = 4
EPS = 1e-6
VMEM_LIMIT = 40 * 1024 * 1024
MESH = pl.DeviceIdType.MESH

TILES, ROWS, LANES = 5, 160, 128
TOP, LOW, END = 8, 16, 144
FULL = ((8, 48), (56, 48), (104, 48))
OWN = ((16, 64), (80, 64))
HALVES = ((12, 68), (80, 68))
GRAM_U = (((8, 32), (40, 36)), ((64, 48), (112, 40)))
GRAM_OWN = (((16, 56),), ((72, 40), (112, 32)))
DM, CG, G3, G2, G1, G0 = range(6)


def lane_iota(shape):
    return lax.broadcasted_iota(jnp.int32, shape, len(shape) - 1)


def sides(ref, row, count):
    v = ref[:, row : row + count, :]
    down = ref[:, row + 1 : row + 1 + count, :]
    up = ref[:, row - 1 : row - 1 + count, :]
    lane = lane_iota(v.shape)
    ahead = pltpu.roll(v, LANES - 1, 2)
    right = jnp.where(lane == LANES - 1, jnp.concatenate([ahead[1:], ahead[:1]], 0), ahead)
    behind = pltpu.roll(v, 1, 2)
    left = jnp.where(lane == 0, jnp.concatenate([behind[-1:], behind[:-1]], 0), behind)
    return v, right, left, down, up


def spread(ref, coef, row, count):
    v, right, left, down, up = sides(ref, row, count)
    part = slice(row, row + count)
    out = coef[0, :, part, :] * (v - right) + coef[1, :, part, :] * (v - left)
    out = out + coef[2, :, part, :] * (v - down) + coef[3, :, part, :] * (v - up)
    return v, out


def own_part(x, row, count):
    first, last = max(row, LOW) - row, min(row + count, END) - row
    return x[:4, first:last, :]


def fold(x):
    return jnp.sum(x.reshape(-1, 8, LANES), axis=0)


class Phase:
    def __init__(self):
        self.open = None

    def __call__(self, name):
        if self.open is not None:
            self.open.__exit__(None, None, None)
        self.open = jax.named_scope(name) if name else None
        if self.open is not None:
            self.open.__enter__()


class Sums:
    def __init__(self):
        self.terms = {}

    def add(self, key, a, b):
        value = fold(a * b)
        self.terms[key] = value if key not in self.terms else self.terms[key] + value


def fine_coefs(m):
    den = m[0] + m[1] + EPS
    alpha = m[0] / den
    gamma = (m[1] + EPS) / den
    s1 = jnp.maximum(
        gamma * gamma * m[0] - 2.0 * gamma * alpha * m[1] + alpha * alpha * m[2], 0.0
    )
    beta = s1 / (m[0] + EPS)
    f = gamma + beta
    pp = s1 + beta * (2.0 * EPS * alpha + beta * m[0])
    plp = jnp.maximum(f * f * m[1] - 2.0 * f * alpha * m[2] + alpha * alpha * m[3], 0.0)
    later = jnp.minimum(s1 / (pp + plp + EPS), 1.0)
    return alpha + later * f, -alpha * later


def kernel(
    forcing, depth, mask, guess, out,
    F, K, V, X, U, W, LG, TG, UG, WG, DEP, MSK, KAP, ROW,
    PKS, PKR, CKS, CKR, PT, MSG, AR,
    GM, GR, in_sem, hs, hr, ar_s, ar_r, ts, tr, tpr, fs, rs, gs, gr, plane_sem,
):
    phase = Phase()
    phase("a0_load")
    tm = lax.axis_index("tm")
    lat = lax.axis_index("lat")
    lon = lax.axis_index("lon")
    me = lat * 4 + lon
    chip, core = tm // 2, tm % 2
    sib = 2 * chip + 1 - core

    def cols(c):
        return pl.ds(LANES * c, LANES)

    barrier = pltpu.get_barrier_semaphore()
    north, south = lax.rem(lat + 3, 4), lax.rem(lat + 1, 4)
    west, east = lax.rem(lon + 3, 4), lax.rem(lon + 1, 4)

    def greet(target):
        pl.semaphore_signal(barrier, inc=1, device_id=target, device_id_type=MESH)

    for a in (north, south):
        for b in (west, east):
            greet({"lat": a, "lon": b})
    for step in (4, 2, 6):
        greet({"tm": lax.rem(tm + step, 8)})
    for a in (north, south):
        greet({"lat": a})
    for b in (west, east):
        greet({"lon": b})
    greet({"tm": sib})

    loads = []
    own_rows = pl.ds(LOW, END - LOW)

    def load(src, dst, field, c):
        copy = pltpu.make_async_copy(src, dst, in_sem.at[field, c])
        copy.start()
        loads.append(copy)

    for c in range(4):
        load(depth.at[:, cols(c)], DEP.at[c], 0, c)
        load(mask.at[:, cols(c)], MSK.at[c], 1, c)
    for c in range(4):
        load(guess.at[0, :, cols(c)], F.at[CG, c, own_rows, :], 2, c)
    for field, level in ((G3, 3), (G2, 2), (G1, 1), (G0, 0)):
        for c in range(4):
            load(forcing.at[level, :, cols(c)], F.at[field, c, own_rows, :], 3 + level, c)

    phase("a1_clear")
    def clear(ref):
        zero = jnp.zeros((TILES, 8, LANES), jnp.float32)
        ref[:, 0:8, :] = zero
        ref[:, 152:160, :] = zero

    def clear_fields(i, _):
        clear(F.at[i])
        return 0

    lax.fori_loop(0, 6, clear_fields, 0)
    for ref in (V, X, U):
        clear(ref)

    def clear_slab(i, _):
        clear(TG.at[i])
        ROW[:, i] = jnp.zeros((4, 8, LANES), jnp.float32)
        return 0

    lax.fori_loop(0, 8, clear_slab, 0)

    phase("a2_loadwait")
    for copy in loads:
        copy.wait()
    for c in range(4):
        F[DM, c, LOW:END, :] = jnp.where(MSK[c] > 0, DEP[c], 0.0)

    phase("a3_pack")
    lane6 = lane_iota((6, 8, LANES))
    right_edge = jnp.zeros((6, 8, LANES), jnp.float32)
    left_edge = jnp.zeros((6, 8, LANES), jnp.float32)
    for t in range(16):
        here = (lane6 >= 8 * t) & (lane6 < 8 * t + 8)
        rows = slice(LOW + 8 * t, LOW + 8 * t + 8)
        right_edge = jnp.where(here, pltpu.roll(F[:, 3, rows, :], (8 * t + 8) % LANES, 2), right_edge)
        left_edge = jnp.where(here, pltpu.roll(F[:, 0, rows, :], 8 * t, 2), left_edge)
    PKS[0] = right_edge
    PKS[1] = left_edge
    lane1 = lane_iota((8, LANES))
    corners = ((136, 3, 8), (136, 0, 0), (16, 3, 8), (16, 0, 0))
    for i, (row, tile, shift) in enumerate(corners):
        packed = jnp.zeros((8, LANES), jnp.float32)
        for f in range(6):
            here = (lane1 >= 8 * f) & (lane1 < 8 * f + 8)
            edge = pltpu.roll(F[f, tile, row : row + 8, :], (8 * f + shift) % LANES, 1)
            packed = jnp.where(here, edge, packed)
        CKS[i] = packed

    phase("a4_barrier")
    pl.semaphore_wait(barrier, 12)

    halos = []

    def push(src, dst, i, target):
        copy = pltpu.make_async_remote_copy(
            src, dst, hs.at[i], hr.at[i], device_id=target, device_id_type=MESH
        )
        copy.start()
        halos.append(copy)

    targets = ((south, east), (south, west), (north, east), (north, west))
    for i, (a, b) in enumerate(targets):
        push(CKS.at[i], CKR.at[i], i, {"lat": a, "lon": b})
    push(PKS.at[0], PKR.at[0], 4, {"lon": east})
    push(PKS.at[1], PKR.at[1], 5, {"lon": west})
    for i, first in ((6, 0), (8, 3)):
        group = pl.ds(first, 3)
        push(
            F.at[group, pl.ds(0, 4), pl.ds(136, 8), :],
            F.at[group, pl.ds(0, 4), pl.ds(8, 8), :],
            i, {"lat": south},
        )
        push(
            F.at[group, pl.ds(0, 4), pl.ds(16, 8), :],
            F.at[group, pl.ds(0, 4), pl.ds(144, 8), :],
            i + 1, {"lat": north},
        )
    phase("a5_halowait")
    for copy in halos[:8]:
        copy.wait_recv()

    pl.semaphore_signal(plane_sem, inc=1, device_id={"tm": sib}, device_id_type=MESH)
    phase("a6_unpack")
    from_left, from_right = PKR[0], PKR[1]
    for t in range(16):
        rows = slice(LOW + 8 * t, LOW + 8 * t + 8)
        a = pltpu.roll(from_left, (120 - 8 * t) % LANES, 2)
        b = pltpu.roll(from_right, (LANES - 8 * t) % LANES, 2)
        F[:, 4, rows, :] = jnp.where(lane6 >= 120, a, jnp.where(lane6 < 8, b, 0.0))
    for row, left, right in ((8, 0, 1), (144, 2, 3)):
        a0, b0 = CKR[left], CKR[right]
        for f in range(6):
            a = pltpu.roll(a0, (120 - 8 * f) % LANES, 1)
            b = pltpu.roll(b0, (LANES - 8 * f) % LANES, 1)
            F[f, 4, row : row + 8, :] = jnp.where(lane1 >= 120, a, jnp.where(lane1 < 8, b, 0.0))

    inside_top = jnp.where(lat > 0, 1.0, 0.0).astype(jnp.float32)
    inside_end = jnp.where(lat < 3, 1.0, 0.0).astype(jnp.float32)
    F[DM, :, 8:16, :] = F[DM, :, 8:16, :] * inside_top
    F[DM, :, 144:152, :] = F[DM, :, 144:152, :] * inside_end

    for row, count in FULL:
        d, *around = sides(F.at[DM], row, count)
        for i, other in enumerate(around):
            K[i, :, row : row + count, :] = jnp.where(
                (d > 0.0) & (other > 0.0), 1.5 * (d + other), 0.0
            )

    def send_sums(r, message):
        MSG[r] = message
        AR[r, me] = message

        def one(step, _):
            there = lax.rem(me + step, 16)
            pltpu.make_async_remote_copy(
                MSG.at[r], AR.at[r, me], ar_s.at[r], ar_r.at[r],
                device_id={"lat": there // 4, "lon": there % 4}, device_id_type=MESH,
            ).start()
            return 0

        lax.fori_loop(1, 16, one, 0)

    def recv_sums(r):
        box = AR.at[r, pl.ds(0, 15)]
        pltpu.make_async_copy(box, box, ar_r.at[r]).wait()
        return jnp.sum(AR[r], axis=0)

    def rows_of(accs):
        row = lax.broadcasted_iota(jnp.int32, (16, LANES), 0)
        stacked = jnp.zeros((16, LANES), jnp.float32)
        for i, acc in enumerate(accs):
            stacked = jnp.where(row == i, jnp.sum(acc, axis=0, keepdims=True), stacked)
        return jnp.broadcast_to(jnp.sum(stacked, axis=1, keepdims=True), (16, LANES))

    def prepare(field, slot):
        sums = Sums()
        for row, count in FULL:
            g, lg = spread(F.at[field], K, row, count)
            LG[slot, :, row : row + count, :] = lg
            g, lg = own_part(g, row, count), own_part(lg, row, count)
            sums.add(0, g, g)
            sums.add(1, g, lg)
            sums.add(2, lg, lg)
        for row, count in OWN:
            lg, llg = spread(LG.at[slot], K, row, count)
            sums.add(3, lg[:4], llg[:4])
        for i in range(4):
            KAP[slot, i] = sums.terms[i]

    def two_steps(r, v_ref, field, slot, between):
        phase(f"r{r}_moments")
        sums = Sums()
        for row, count in FULL:
            v, u = spread(v_ref, K, row, count)
            U[:, row : row + count, :] = u
            g = own_part(F[field, :, row : row + count, :], row, count)
            v, u = own_part(v, row, count), own_part(u, row, count)
            sums.add("m0", v, v)
            sums.add("m1", v, u)
            sums.add("m2", u, u)
            sums.add("n0", v, g)
            sums.add("n1", u, g)
        for row, count in FULL:
            u, w = spread(U, K, row, count)
            W[:, row : row + count, :] = w
            lg = own_part(LG[slot, :, row : row + count, :], row, count)
            u, w = own_part(u, row, count), own_part(w, row, count)
            sums.add("m3", u, w)
            sums.add("m4", w, w)
            sums.add("n2", u, lg)
            sums.add("n3", w, lg)
        for row, count in OWN:
            w, lw = spread(W, K, row, count)
            lg = LG[slot, :4, row : row + count, :]
            sums.add("m5", w[:4], lw[:4])
            sums.add("n4", lw[:4], lg)
        names = ["m0", "m1", "m2", "m3", "m4", "m5", "n0", "n1", "n2", "n3", "n4"]
        accs = [sums.terms[n] for n in names] + [KAP[slot, i] for i in range(4)]
        send_sums(r, rows_of(accs))
        phase(f"r{r}_between")
        between()
        phase(f"r{r}_wait")
        total = recv_sums(r)
        phase(f"r{r}_scalars")
        at = [total[i : i + 1, :] for i in range(15)]
        m, n, k = at[:6], at[6:11], at[11:]
        a, b = fine_coefs(m)
        later = [
            jnp.maximum(
                a * a * m[i] + 2.0 * a * b * m[i + 1] + b * b * m[i + 2]
                + 2.0 * (a * n[i] + b * n[i + 1]) + k[i],
                0.0,
            )
            for i in range(4)
        ]
        a2, b2 = fine_coefs(later)
        return m, (a, b), (a2 * a, a2 * b + b2 * a, b2 * b, a2, b2)

    def scaled(s, x):
        return jnp.broadcast_to(s.reshape(1, 1, LANES), x.shape) * x

    phase("a7_prepare")
    prepare(G3, 0)

    def rest_of_halo():
        for copy in halos[8:]:
            copy.wait_recv()
        prepare(G1, 1)

    m_start, _, c = two_steps(0, F.at[CG], G3, 0, rest_of_halo)
    for row, count in FULL:
        part = slice(row, row + count)
        X[:, part, :] = (
            scaled(c[0], F[CG, :, part, :]) + scaled(c[1], U[:, part, :]) + scaled(c[2], W[:, part, :])
            + scaled(c[3], F[G3, :, part, :]) + scaled(c[4], LG[0, :, part, :]) + F[G2, :, part, :]
        )
    last = jnp.where(tm == 7, 1.0, 0.0).astype(jnp.float32)
    psi = m_start[0] / (m_start[0] + 4.0 * m_start[1] + EPS)
    drop = psi * (last - 1.0)

    _, _, c = two_steps(1, X, G1, 1, lambda: prepare(G2, 2))
    for row, count in FULL:
        part = slice(row, row + count)
        TG[tm, :, part, :] = (
            scaled(c[0], X[:, part, :]) + scaled(c[1], U[:, part, :]) + scaled(c[2], W[:, part, :])
            + scaled(c[3], F[G1, :, part, :]) + scaled(c[4], LG[1, :, part, :]) + F[G0, :, part, :]
            + scaled(drop, F[CG, :, part, :])
        )

    phase("b0_gather")
    lane2 = lane_iota((8, LANES))
    for half in range(2):
        packed = jnp.zeros((8, LANES), jnp.float32)
        for t in range(9):
            row = TOP + 8 * (9 * half + t)
            here = (lane2 >= 8 * t) & (lane2 < 8 * t + 8)
            packed = jnp.where(here, pltpu.roll(TG[tm, 4, row : row + 8, :], 8 * t + 4, 1), packed)
        PT[tm, 8 * half : 8 * half + 8, :] = packed

    def half_copies(k, h, sems, target):
        row, count = HALVES[h]
        main = TG.at[k, pl.ds(0, 4), pl.ds(row, count), :]
        pack = PT.at[k, pl.ds(8 * h, 8), :]
        return [
            pltpu.make_async_remote_copy(
                ref, ref, sems.at[i], recv.at[k, h], device_id={"tm": target}, device_id_type=MESH
            )
            for i, (ref, recv) in enumerate(((main, tr), (pack, tpr)))
        ]

    below, above = jnp.maximum(tm - 2, 0), jnp.minimum(tm + 2, 7)
    wrapped = lax.rem(tm + 2, 8)

    def own_sends(act):
        for h in range(2):
            @pl.when(core == 1)
            def _():
                act(half_copies(tm, h, ts.at[0, h], sib))

            @pl.when(chip == 3)
            def _():
                act(half_copies(tm, h, ts.at[1, h], wrapped))

            @pl.when(chip >= 1)
            def _():
                act(half_copies(tm, h, ts.at[2, h], below))

            if h == 1:
                @pl.when(chip == 2)
                def _():
                    act(half_copies(tm, h, ts.at[1, h], above))

    def start(copies):
        for copy in copies:
            copy.start()

    def sent(copies):
        for copy in copies:
            copy.wait_send()

    def landed(copies):
        for copy in copies:
            copy.wait_recv()

    own_sends(start)

    def slab_at(e):
        dx = jnp.where(e >= 5, 2, jnp.where(e % 2 == 1, 1, 3))
        same = (e == 1) | (e == 2) | (e == 5)
        k = jnp.where(e == 0, 2 * chip + 1, jnp.where(same, tm, sib) + 2 * dx)
        valid = (e == 0) | (chip + dx <= 3)
        return jnp.minimum(k, 7), dx, same, valid

    def relay_from(e, h):
        if h == 0:
            return (e == 1) & ((chip == 1) | (chip == 2)), below
        return (e == 2) & (chip == 0), above

    def unpack(k, h):
        packed = PT[k, 8 * h : 8 * h + 8, :]
        for t in range(9):
            row = TOP + 8 * (9 * h + t)
            back = pltpu.roll(packed, (LANES - 8 * t - 4) % LANES, 1)
            TG[k, 4, row : row + 8, :] = jnp.where((lane2 < 4) | (lane2 >= 124), back, 0.0)

    def gram_sums(e, k, half):
        for row, count in GRAM_U[half]:
            _, u = spread(TG.at[k], K, row, count)
            UG[k, :, row : row + count, :] = u
        for row, count in GRAM_OWN[half]:
            _, w = spread(UG.at[k], K, row, count)
            WG[k, :, row - LOW : row - LOW + count, :] = w[:4]
        first = GRAM_OWN[half][0][0]
        end = sum(GRAM_OWN[half][-1])

        def pair(q, _):
            j, _, _, held = slab_at(q)

            @pl.when(held)
            def _():
                sums = Sums()
                low, high = jnp.minimum(j, k), jnp.maximum(j, k)
                for t in range(4):
                    tk, uk = TG[high, t, first:end, :], UG[high, t, first:end, :]
                    wk = WG[high, t, first - LOW : end - LOW, :]
                    tj, uj = TG[low, t, first:end, :], UG[low, t, first:end, :]
                    sums.add(0, tj, tk)
                    sums.add(1, tj, uk)
                    sums.add(2, uj, uk)
                    sums.add(3, uj, wk)
                for i in range(4):
                    value = jnp.sum(sums.terms[i], axis=0, keepdims=True)
                    ROW[i, k, pl.ds(j, 1), :] = value
                    ROW[i, j, pl.ds(k, 1), :] = value

            return 0

        lax.fori_loop(0, e + 1, pair, 0)

    def arrive(i, _):
        late = i >= 10
        half = jnp.where(i < 2, i, jnp.where(late, (i - 10) // 2, (i - 2) // 4))
        e = jnp.where(i < 2, 0, jnp.where(late, 5 + i % 2, 1 + (i - 2) % 4))
        k, dx, same, valid = slab_at(e)
        for h in range(2):
            @pl.when(valid & (half == h))
            def _():
                @pl.when((e > 0) | (core == 0))
                def _():
                    with jax.named_scope("b1_slabwait"):
                        landed(half_copies(k, h, ts.at[0, h], sib))

                    @pl.when(same)
                    def _():
                        start(half_copies(k, h, fs.at[dx, h], sib))

                    do_relay, target = relay_from(e, h)

                    @pl.when(do_relay)
                    def _():
                        start(half_copies(k, h, rs.at[0, h], target))

                    unpack(k, h)

                @pl.when(core == h)
                def _():
                    gram_sums(e, k, h)

        return 0

    phase("b1_arrive")
    lax.fori_loop(0, 14, arrive, 0)

    @pl.when(chip == 3)
    def _():
        landed(half_copies(below, 1, ts.at[0, 1], sib))
        start(half_copies(below, 1, rs.at[0, 1], wrapped))

    phase("b2_gram")
    lane3 = lane_iota((8, 8, LANES))
    sub3 = lax.broadcasted_iota(jnp.int32, (8, 8, LANES), 1)
    gram = jnp.zeros((8, 8, LANES), jnp.float32)
    for i in range(4):
        gram = jnp.where(lane3 == 8 * i + sub3, jnp.sum(ROW[i], axis=2, keepdims=True), gram)
    gram = jnp.sum(gram, axis=1)
    GM[...] = gram
    GR[core * 16 + me] = gram
    pl.semaphore_wait(plane_sem, 1)

    def send_gram(step, _):
        there = lax.rem(me + step, 16)
        place = {"lat": there // 4, "lon": there % 4}

        @pl.when(step < 16)
        def _():
            pltpu.make_async_remote_copy(
                GM, GR.at[core * 16 + me], gs, gr, device_id=place, device_id_type=MESH
            ).start()

        pltpu.make_async_remote_copy(
            GM, GR.at[core * 16 + me], gs, gr, device_id={"tm": sib, **place}, device_id_type=MESH
        ).start()
        return 0

    lax.fori_loop(1, 17, send_gram, 0)
    phase("b3_wait")
    box = GR.at[pl.ds(0, 31)]
    pltpu.make_async_copy(box, box, gr).wait()
    total = jnp.sum(GR[...], axis=0)
    phase("b4_chain")

    lane = lane_iota((8, LANES))
    table = [
        [
            None if j == 0 else jnp.broadcast_to(
                jnp.sum(jnp.where(lane == 8 * i + j, total, 0.0), axis=1, keepdims=True), (8, LANES)
            )
            for j in range(8)
        ]
        for i in range(4)
    ]

    def entry(i, k, j):
        return table[i][j][k : k + 1, :]

    one = jnp.ones((1, LANES), jnp.float32)
    zero = jnp.zeros((1, LANES), jnp.float32)
    coefs = {7: one}
    quad = [entry(i, 7, 7) for i in range(4)]
    cross = [{j: entry(i, 7, j) for j in range(1, 7)} for i in range(4)]
    is_last = jnp.full((1, LANES), tm == 7)
    held_c = {k: zero for k in range(1, 8)}
    held_q = [m_start[i] for i in range(4)]
    for t in range(7, 0, -1):
        if t < 7:
            psi_t = quad[0] / (quad[0] + 4.0 * quad[1] + EPS)
            quad = [
                psi_t * psi_t * quad[i] + 2.0 * psi_t * cross[i][t] + entry(i, t, t)
                for i in range(4)
            ]
            cross = [{j: psi_t * cross[i][j] + entry(i, t, j) for j in range(1, t)} for i in range(4)]
            coefs = {k: psi_t * x for k, x in coefs.items()}
            coefs[t] = one
        now = jnp.full((1, LANES), tm + 1 == t)
        for k in coefs:
            held_c[k] = jnp.where(now, coefs[k], held_c[k])
        held_q = [jnp.where(now, quad[i], held_q[i]) for i in range(4)]
    psi = held_q[0] / (held_q[0] + 4.0 * held_q[1] + EPS)
    psi = jnp.where(is_last, 0.0, psi)
    for row, count in FULL:
        part = slice(row, row + count)
        value = F[CG, :, part, :] * last
        for k in range(1, 8):
            value = value + scaled(held_c[k], jnp.where(tm < k, TG[k, :, part, :], 0.0))
        V[:, part, :] = value

    def put(level, row, value):
        for t in range(4):
            out[level, row - LOW : row - LOW + value.shape[1], cols(t)] = value[t]

    phase("c0_correct")
    a, b = fine_coefs(held_q)
    for row, count in FULL:
        part = slice(row, row + count)
        v, u = spread(V, K, row, count)
        value = scaled(a, v) + scaled(b, u) + F[G3, :, part, :]
        X[:, part, :] = value
        put(3, max(row, LOW), own_part(value, row, count))

    def write_first():
        for row, count in OWN:
            part = slice(row, row + count)
            put(0, row, scaled(psi, V[:4, part, :]) + TG[tm, :4, part, :])

    _, (a, b), c = two_steps(2, X, G2, 2, write_first)
    for row, count in OWN:
        part = slice(row, row + count)
        v, u, w = X[:4, part, :], U[:4, part, :], W[:4, part, :]
        g = F[G2, :4, part, :]
        put(2, row, scaled(a, v) + scaled(b, u) + g)
        last_value = (
            scaled(c[0], v) + scaled(c[1], u) + scaled(c[2], w) + scaled(c[3], g)
            + scaled(c[4], LG[2, :4, part, :]) + F[G1, :4, part, :]
        )
        put(1, row, last_value)

    phase("c9_end")
    for copy in halos:
        copy.wait_send()
    for r in range(3):
        box = AR.at[r, pl.ds(0, 15)]
        pltpu.make_async_copy(box, box, ar_s.at[r]).wait()
    box = GR.at[pl.ds(0, 31)]
    pltpu.make_async_copy(box, box, gs).wait()
    own_sends(sent)
    for dx in (1, 3, 2):
        @pl.when(chip + dx <= 3)
        def _():
            for h in range(2):
                sent(half_copies(jnp.minimum(tm + 2 * dx, 7), h, fs.at[dx, h], sib))

    @pl.when((chip == 1) | (chip == 2))
    def _():
        sent(half_copies(above, 0, rs.at[0, 0], below))

    @pl.when(chip == 0)
    def _():
        sent(half_copies(jnp.minimum(tm + 6, 7), 1, rs.at[0, 1], above))

    @pl.when(chip == 3)
    def _():
        sent(half_copies(below, 1, rs.at[0, 1], wrapped))

    phase(None)


def local(forcing, depth, mask, guess):
    f32 = jnp.float32
    field = (TILES, ROWS, LANES)
    dma = pltpu.SemaphoreType.DMA
    return pl.pallas_call(
        kernel,
        out_shape=jax.ShapeDtypeStruct(forcing.shape, f32),
        in_specs=[pl.BlockSpec(memory_space=pltpu.HBM)] * 4,
        out_specs=pl.BlockSpec(memory_space=pltpu.VMEM),
        scratch_shapes=[
            pltpu.VMEM((6, *field), f32),
            pltpu.VMEM((4, *field), f32),
            pltpu.VMEM(field, f32),
            pltpu.VMEM(field, f32),
            pltpu.VMEM(field, f32),
            pltpu.VMEM(field, f32),
            pltpu.VMEM((3, *field), f32),
            pltpu.VMEM((8, *field), f32),
            pltpu.VMEM((8, *field), f32),
            pltpu.VMEM((8, 4, 128, LANES), f32),
            pltpu.VMEM((4, 128, LANES), f32),
            pltpu.VMEM((4, 128, LANES), jnp.int32),
            pltpu.VMEM((3, 4, 8, LANES), f32),
            pltpu.VMEM((4, 8, 8, LANES), f32),
            pltpu.VMEM((2, 6, 8, LANES), f32),
            pltpu.VMEM((2, 6, 8, LANES), f32),
            pltpu.VMEM((4, 8, LANES), f32),
            pltpu.VMEM((4, 8, LANES), f32),
            pltpu.VMEM((8, 16, LANES), f32),
            pltpu.VMEM((3, 16, LANES), f32),
            pltpu.VMEM((3, 16, 16, LANES), f32),
            pltpu.VMEM((8, LANES), f32),
            pltpu.VMEM((32, 8, LANES), f32),
            dma((7, 4)),
            dma((10,)),
            dma((10,)),
            dma((3,)),
            dma((3,)),
            dma((3, 2, 2)),
            dma((8, 2)),
            dma((8, 2)),
            dma((4, 2, 2)),
            dma((1, 2, 2)),
            dma,
            dma,
            pltpu.SemaphoreType.REGULAR,
        ],
        compiler_params=pltpu.CompilerParams(
            collective_id=0, has_side_effects=True, vmem_limit_bytes=VMEM_LIMIT
        ),
        name="cycle",
    )(*(pltpu.with_memory_space_constraint(x, pltpu.HBM) for x in (forcing, depth, mask, guess)))


def solution(mesh):
    return jax.shard_map(
        local,
        mesh=mesh,
        in_specs=(P("tm", "lat", "lon"), P("lat", "lon"), P("lat", "lon"), P("tm", "lat", "lon")),
        out_specs=P("tm", "lat", "lon"),
        check_vma=False,
    )
```

```python
import functools

import jax
import jax.numpy as jnp
from jax import lax
from jax.experimental import pallas as pl
from jax.experimental.pallas import tpu as pltpu
from jax.sharding import PartitionSpec as P

FS = 4
EPS = 1e-6
VMEM_LIMIT = 40 * 1024 * 1024
MESH = pl.DeviceIdType.MESH

TILES, ROWS, LANES = 5, 160, 128
TOP, LOW, END = 8, 16, 144
FULL = tuple((row, 24) for row in range(8, 152, 24))
OWN = tuple((row, 32) for row in range(16, 144, 32))
HALF_ROWS = 96
HALF = ((8, 24), (32, 24), (56, 32))
HALF_OWN = ((16, 32), (48, 32))
HALF_LOW, HALF_END = 16, 80
DM, CG, G3, G2, G1, G0 = range(6)


def lane_iota(shape):
    return lax.broadcasted_iota(jnp.int32, shape, len(shape) - 1)


def sides(ref, row, count):
    v = ref[:, row : row + count, :]
    down = ref[:, row + 1 : row + 1 + count, :]
    up = ref[:, row - 1 : row - 1 + count, :]
    lane = lane_iota(v.shape)
    ahead = pltpu.roll(v, LANES - 1, 2)
    right = jnp.where(lane == LANES - 1, jnp.concatenate([ahead[1:], ahead[:1]], 0), ahead)
    behind = pltpu.roll(v, 1, 2)
    left = jnp.where(lane == 0, jnp.concatenate([behind[-1:], behind[:-1]], 0), behind)
    return v, right, left, down, up


def spread(ref, coef, row, count):
    v, right, left, down, up = sides(ref, row, count)
    part = slice(row, row + count)
    out = coef[0, :, part, :] * (v - right) + coef[1, :, part, :] * (v - left)
    out = out + coef[2, :, part, :] * (v - down) + coef[3, :, part, :] * (v - up)
    return v, out


def own_part(x, row, count):
    first, last = max(row, LOW) - row, min(row + count, END) - row
    return x[:4, first:last, :]


def fold(x):
    return jnp.sum(x.reshape(-1, 8, LANES), axis=0)


class Phase:
    def __init__(self):
        self.open = None

    def __call__(self, name):
        if self.open is not None:
            self.open.__exit__(None, None, None)
        self.open = jax.named_scope(name) if name else None
        if self.open is not None:
            self.open.__enter__()


class Sums:
    def __init__(self):
        self.terms = {}

    def add(self, key, a, b):
        value = fold(a * b)
        self.terms[key] = value if key not in self.terms else self.terms[key] + value


def fine_coefs(m):
    den = m[0] + m[1] + EPS
    alpha = m[0] / den
    gamma = (m[1] + EPS) / den
    s1 = jnp.maximum(
        gamma * gamma * m[0] - 2.0 * gamma * alpha * m[1] + alpha * alpha * m[2], 0.0
    )
    beta = s1 / (m[0] + EPS)
    f = gamma + beta
    pp = s1 + beta * (2.0 * EPS * alpha + beta * m[0])
    plp = jnp.maximum(f * f * m[1] - 2.0 * f * alpha * m[2] + alpha * alpha * m[3], 0.0)
    later = jnp.minimum(s1 / (pp + plp + EPS), 1.0)
    return alpha + later * f, -alpha * later


def kernel(
    forcing, depth, mask, guess, out,
    F, K, V, X, U, W, LG, GP, KH, TH, UG, TG2, TG3, TG4, DEP, MSK, KAP, ROW, CR, KQ,
    PKS, PKR, CKS, CKR, PT, MSG, AR,
    GM, GR, in_sem, hs, hr, ar_s, ar_r, ts, tr, tpr, fs, rs, gs, gr, plane_sem,
):
    phase = Phase()
    phase("a0_load")
    tm = lax.axis_index("tm")
    lat = lax.axis_index("lat")
    lon = lax.axis_index("lon")
    me = lat * 4 + lon
    chip, core = tm // 2, tm % 2
    sib = 2 * chip + 1 - core

    def cols(c):
        return pl.ds(LANES * c, LANES)

    barrier = pltpu.get_barrier_semaphore()
    north, south = lax.rem(lat + 3, 4), lax.rem(lat + 1, 4)
    west, east = lax.rem(lon + 3, 4), lax.rem(lon + 1, 4)

    def greet(target):
        pl.semaphore_signal(barrier, inc=1, device_id=target, device_id_type=MESH)

    for a in (north, south):
        for b in (west, east):
            greet({"lat": a, "lon": b})
    for step in (4, 3, 5, 2, 6, 1, 7):
        greet({"tm": lax.rem(tm + step, 8)})
    for a in (north, south):
        greet({"lat": a})
    for b in (west, east):
        greet({"lon": b})

    loads = []
    own_rows = pl.ds(LOW, END - LOW)

    def load(src, dst, field, c):
        copy = pltpu.make_async_copy(src, dst, in_sem.at[field, c])
        copy.start()
        loads.append(copy)

    for c in range(4):
        load(depth.at[:, cols(c)], DEP.at[c], 0, c)
        load(mask.at[:, cols(c)], MSK.at[c], 1, c)
    for c in range(4):
        load(guess.at[0, :, cols(c)], F.at[CG, c, own_rows, :], 2, c)
    for field, level in ((G3, 3), (G2, 2), (G1, 1), (G0, 0)):
        for c in range(4):
            load(forcing.at[level, :, cols(c)], F.at[field, c, own_rows, :], 3 + level, c)

    phase("a1_clear")
    def clear(ref):
        zero = jnp.zeros((TILES, 8, LANES), jnp.float32)
        ref[:, 0:8, :] = zero
        ref[:, 152:160, :] = zero

    def clear_fields(i, _):
        clear(F.at[i])
        return 0

    lax.fori_loop(0, 6, clear_fields, 0)
    for ref in (V, X, U):
        clear(ref)

    def clear_slab(i, _):
        ROW[:, i] = jnp.zeros((8, 8, LANES), jnp.float32)
        CR[i] = jnp.zeros((16, LANES), jnp.float32)
        return 0

    lax.fori_loop(0, 8, clear_slab, 0)
    KQ[...] = jnp.zeros((24, LANES), jnp.float32)
    for i in range(9):
        clear(GP.at[i])
    for i in range(3):
        clear(LG.at[i])

    phase("a2_loadwait")
    for copy in loads:
        copy.wait()
    for c in range(4):
        F[DM, c, LOW:END, :] = jnp.where(MSK[c] > 0, DEP[c], 0.0)

    phase("a3_pack")
    lane6 = lane_iota((6, 8, LANES))
    right_edge = jnp.zeros((6, 8, LANES), jnp.float32)
    left_edge = jnp.zeros((6, 8, LANES), jnp.float32)
    for t in range(16):
        here = (lane6 >= 8 * t) & (lane6 < 8 * t + 8)
        rows = slice(LOW + 8 * t, LOW + 8 * t + 8)
        right_edge = jnp.where(here, pltpu.roll(F[:, 3, rows, :], (8 * t + 8) % LANES, 2), right_edge)
        left_edge = jnp.where(here, pltpu.roll(F[:, 0, rows, :], 8 * t, 2), left_edge)
    PKS[0] = right_edge
    PKS[1] = left_edge
    lane1 = lane_iota((8, LANES))
    corners = ((136, 3, 8), (136, 0, 0), (16, 3, 8), (16, 0, 0))
    for i, (row, tile, shift) in enumerate(corners):
        packed = jnp.zeros((8, LANES), jnp.float32)
        for f in range(6):
            here = (lane1 >= 8 * f) & (lane1 < 8 * f + 8)
            edge = pltpu.roll(F[f, tile, row : row + 8, :], (8 * f + shift) % LANES, 1)
            packed = jnp.where(here, edge, packed)
        CKS[i] = packed

    phase("a4_barrier")
    pl.semaphore_wait(barrier, 15)

    halos = []

    def push(src, dst, i, target):
        copy = pltpu.make_async_remote_copy(
            src, dst, hs.at[i], hr.at[i], device_id=target, device_id_type=MESH
        )
        copy.start()
        halos.append(copy)

    targets = ((south, east), (south, west), (north, east), (north, west))
    for i, (a, b) in enumerate(targets):
        push(CKS.at[i], CKR.at[i], i, {"lat": a, "lon": b})
    push(PKS.at[0], PKR.at[0], 4, {"lon": east})
    push(PKS.at[1], PKR.at[1], 5, {"lon": west})
    for i, first in ((6, 0), (8, 3)):
        group = pl.ds(first, 3)
        push(
            F.at[group, pl.ds(0, 4), pl.ds(136, 8), :],
            F.at[group, pl.ds(0, 4), pl.ds(8, 8), :],
            i, {"lat": south},
        )
        push(
            F.at[group, pl.ds(0, 4), pl.ds(16, 8), :],
            F.at[group, pl.ds(0, 4), pl.ds(144, 8), :],
            i + 1, {"lat": north},
        )
    phase("a5_halowait")
    for copy in halos[:8]:
        copy.wait_recv()

    pl.semaphore_signal(plane_sem, inc=1, device_id={"tm": sib}, device_id_type=MESH)
    phase("a6_unpack")
    from_left, from_right = PKR[0], PKR[1]
    for t in range(16):
        rows = slice(LOW + 8 * t, LOW + 8 * t + 8)
        a = pltpu.roll(from_left, (120 - 8 * t) % LANES, 2)
        b = pltpu.roll(from_right, (LANES - 8 * t) % LANES, 2)
        F[:, 4, rows, :] = jnp.where(lane6 >= 120, a, jnp.where(lane6 < 8, b, 0.0))
    for row, left, right in ((8, 0, 1), (144, 2, 3)):
        a0, b0 = CKR[left], CKR[right]
        for f in range(6):
            a = pltpu.roll(a0, (120 - 8 * f) % LANES, 1)
            b = pltpu.roll(b0, (LANES - 8 * f) % LANES, 1)
            F[f, 4, row : row + 8, :] = jnp.where(lane1 >= 120, a, jnp.where(lane1 < 8, b, 0.0))

    inside_top = jnp.where(lat > 0, 1.0, 0.0).astype(jnp.float32)
    inside_end = jnp.where(lat < 3, 1.0, 0.0).astype(jnp.float32)
    F[DM, :, 8:16, :] = F[DM, :, 8:16, :] * inside_top
    F[DM, :, 144:152, :] = F[DM, :, 144:152, :] * inside_end

    for row, count in FULL:
        d, *around = sides(F.at[DM], row, count)
        for i, other in enumerate(around):
            K[i, :, row : row + count, :] = jnp.where(
                (d > 0.0) & (other > 0.0), 1.5 * (d + other), 0.0
            )

    def send_sums(r, message):
        MSG[r] = message
        AR[r, me] = message

        def one(step, _):
            there = lax.rem(me + step, 16)
            pltpu.make_async_remote_copy(
                MSG.at[r], AR.at[r, me], ar_s.at[r], ar_r.at[r],
                device_id={"lat": there // 4, "lon": there % 4}, device_id_type=MESH,
            ).start()
            return 0

        lax.fori_loop(1, 16, one, 0)

    def recv_sums(r):
        box = AR.at[r, pl.ds(0, 15)]
        pltpu.make_async_copy(box, box, ar_r.at[r]).wait()
        return jnp.sum(AR[r], axis=0)

    def rows_of(accs):
        row = lax.broadcasted_iota(jnp.int32, (16, LANES), 0)
        stacked = jnp.zeros((16, LANES), jnp.float32)
        for i, acc in enumerate(accs):
            stacked = jnp.where(row == i, jnp.sum(acc, axis=0, keepdims=True), stacked)
        return jnp.broadcast_to(jnp.sum(stacked, axis=1, keepdims=True), (16, LANES))

    def prepare(field, slot):
        sums = Sums()
        for row, count in FULL:
            g, lg = spread(F.at[field], K, row, count)
            LG[slot, :, row : row + count, :] = lg
            g, lg = own_part(g, row, count), own_part(lg, row, count)
            sums.add(0, g, g)
            sums.add(1, g, lg)
            sums.add(2, lg, lg)
        for row, count in OWN:
            lg, llg = spread(LG.at[slot], K, row, count)
            sums.add(3, lg[:4], llg[:4])
        for i in range(4):
            KAP[slot, i] = sums.terms[i]

    def power(src, dst):
        for row, count in FULL:
            dst[:, row : row + count, :] = spread(src, K, row, count)[1]

    def line(acc):
        return jnp.sum(acc, axis=0, keepdims=True)

    def own_sum(a, b):
        return line(fold(a[:4, LOW:END, :] * b[:4, LOW:END, :]))

    g3_powers = [F.at[G3], LG.at[0]] + [GP.at[i] for i in range(5)]
    g2_powers = [F.at[G2], LG.at[2]] + [GP.at[i] for i in range(5, 9)]

    def powers_of_g3():
        for src, dst in zip(g3_powers[1:], g3_powers[2:]):
            power(src, dst)

    def powers_of_g2():
        prepare(G2, 2)
        for src, dst in zip(g2_powers[1:], g2_powers[2:]):
            power(src, dst)
        for i in range(4):
            KQ[i : i + 1, :] = line(KAP[0, i])
            KQ[11 + i : 12 + i, :] = line(KAP[2, i])
        KQ[4:5, :] = own_sum(g3_powers[2], g3_powers[2])
        KQ[5:6, :] = own_sum(g3_powers[2], g3_powers[3])
        for i in range(5):
            KQ[6 + i : 7 + i, :] = own_sum(g2_powers[0], g3_powers[i])

    def two_steps(r, v_ref, field, slot, between):
        phase(f"r{r}_moments")
        sums = Sums()
        for row, count in FULL:
            v, u = spread(v_ref, K, row, count)
            U[:, row : row + count, :] = u
            g = own_part(F[field, :, row : row + count, :], row, count)
            v, u = own_part(v, row, count), own_part(u, row, count)
            sums.add("m0", v, v)
            sums.add("m1", v, u)
            sums.add("m2", u, u)
            sums.add("n0", v, g)
            sums.add("n1", u, g)
        for row, count in FULL:
            u, w = spread(U, K, row, count)
            W[:, row : row + count, :] = w
            lg = own_part(LG[slot, :, row : row + count, :], row, count)
            u, w = own_part(u, row, count), own_part(w, row, count)
            sums.add("m3", u, w)
            sums.add("m4", w, w)
            sums.add("n2", u, lg)
            sums.add("n3", w, lg)
        for row, count in OWN:
            w, lw = spread(W, K, row, count)
            lg = LG[slot, :4, row : row + count, :]
            sums.add("m5", w[:4], lw[:4])
            sums.add("n4", lw[:4], lg)
        names = ["m0", "m1", "m2", "m3", "m4", "m5", "n0", "n1", "n2", "n3", "n4"]
        accs = [sums.terms[n] for n in names] + [KAP[slot, i] for i in range(4)]
        send_sums(r, rows_of(accs))
        phase(f"r{r}_between")
        between()
        phase(f"r{r}_wait")
        total = recv_sums(r)
        phase(f"r{r}_scalars")
        at = [total[i : i + 1, :] for i in range(15)]
        m, n, k = at[:6], at[6:11], at[11:]
        a, b = fine_coefs(m)
        later = [
            jnp.maximum(
                a * a * m[i] + 2.0 * a * b * m[i + 1] + b * b * m[i + 2]
                + 2.0 * (a * n[i] + b * n[i + 1]) + k[i],
                0.0,
            )
            for i in range(4)
        ]
        a2, b2 = fine_coefs(later)
        return m, (a, b), (a2 * a, a2 * b + b2 * a, b2 * b, a2, b2)

    def scaled(s, x):
        return jnp.broadcast_to(s.reshape(1, 1, LANES), x.shape) * x

    phase("a7_prepare")
    prepare(G3, 0)

    def rest_of_halo():
        for copy in halos[8:]:
            copy.wait_recv()
        prepare(G1, 1)
        powers_of_g3()
        rows = pl.ds(pl.multiple_of(8 + 64 * core, 8), 80)
        for i in range(4):
            KH[i, :, 8:88, :] = K[i, :, rows, :]

    m_start, _, c = two_steps(0, F.at[CG], G3, 0, rest_of_halo)
    for row, count in FULL:
        part = slice(row, row + count)
        X[:, part, :] = (
            scaled(c[0], F[CG, :, part, :]) + scaled(c[1], U[:, part, :]) + scaled(c[2], W[:, part, :])
            + scaled(c[3], F[G3, :, part, :]) + scaled(c[4], LG[0, :, part, :]) + F[G2, :, part, :]
        )
    last = jnp.where(tm == 7, 1.0, 0.0).astype(jnp.float32)
    psi = m_start[0] / (m_start[0] + 4.0 * m_start[1] + EPS)
    drop = psi * (last - 1.0)

    _, _, c = two_steps(1, X, G1, 1, powers_of_g2)
    for h in range(2):
        for row, count in HALF:
            part = slice(64 * h + row, 64 * h + row + count)
            TH[h, tm, :, row : row + count, :] = (
                scaled(c[0], X[:, part, :]) + scaled(c[1], U[:, part, :])
                + scaled(c[2], W[:, part, :]) + scaled(c[3], F[G1, :, part, :])
                + scaled(c[4], LG[1, :, part, :]) + F[G0, :, part, :]
                + scaled(drop, F[CG, :, part, :])
            )

    phase("b0_gather")
    lane2 = lane_iota((8, LANES))
    for h in range(2):
        packed = jnp.zeros((8, LANES), jnp.float32)
        for t in range(10):
            row = 8 + 8 * t
            here = (lane2 >= 8 * t) & (lane2 < 8 * t + 8)
            edge = pltpu.roll(TH[h, tm, 4, row : row + 8, :], 8 * t + 4, 1)
            packed = jnp.where(here, edge, packed)
        PT[tm, h] = packed

    def half_copies(k, h, sems, target):
        main = TH.at[h, k, pl.ds(0, 4), pl.ds(12, 72), :]
        pack = PT.at[k, h]
        return [
            pltpu.make_async_remote_copy(
                ref, ref, sems.at[i], recv.at[k, h], device_id={"tm": target}, device_id_type=MESH
            )
            for i, (ref, recv) in enumerate(((main, tr), (pack, tpr)))
        ]

    def own_sends(act):
        for h in range(2):
            @pl.when(core == 1)
            def _():
                act(half_copies(tm, h, ts.at[0, h], sib))

            @pl.when(chip == 3)
            def _():
                act(half_copies(tm, h, ts.at[1, h], h))

            @pl.when(chip >= 1)
            def _():
                act(half_copies(tm, h, ts.at[2, h], jnp.maximum(2 * chip - 2 + h, 0)))

            if h == 1:
                @pl.when(chip == 2)
                def _():
                    act(half_copies(tm, h, ts.at[1, h], 7))

    def start(copies):
        for copy in copies:
            copy.start()

    def sent(copies):
        for copy in copies:
            copy.wait_send()

    def landed(copies):
        for copy in copies:
            copy.wait_recv()

    own_sends(start)

    def slab_at(e):
        dx = jnp.where(e >= 5, 2, jnp.where(e % 2 == 1, 1, 3))
        odd = jnp.where((e == 1) | (e == 2) | (e == 5), 1, 0)
        k = jnp.where(e == 0, 2 * chip + 1, 2 * (chip + dx) + odd)
        valid = (e == 0) | (chip + dx <= 3)
        return jnp.minimum(k, 7), dx, odd, valid

    def unpack(k, h):
        packed = PT[k, h]
        for t in range(10):
            back = pltpu.roll(packed, (LANES - 8 * t - 4) % LANES, 1)
            back = jnp.where((lane2 < 4) | (lane2 >= 124), back, 0.0)
            TH[h, k, 4, 8 + 8 * t : 16 + 8 * t, :] = back

    def gram_sums(e, k):
        refs = [TH.at[core, k], UG.at[k], TG2.at[k], TG3.at[k]]
        for src, dst in zip(refs, refs[1:]):
            for row, count in HALF:
                dst[:, row : row + count, :] = spread(src, KH, row, count)[1]
        for row, count in HALF_OWN:
            last_power = spread(refs[3], KH, row, count)[1]
            TG4[k, :, row - HALF_LOW : row - HALF_LOW + count, :] = last_power[:4]

        def pair(q, _):
            j, _, _, held = slab_at(q)

            @pl.when(held)
            def _():
                sums = Sums()
                low, high = jnp.minimum(j, k), jnp.maximum(j, k)
                for t in range(4):
                    a, b = (
                        [TH[core, s, t, HALF_LOW:HALF_END, :]]
                        + [ref[s, t, HALF_LOW:HALF_END, :] for ref in (UG, TG2, TG3)]
                        for s in (low, high)
                    )
                    b.append(TG4[high, t])
                    for i in range(8):
                        sums.add(i, a[i // 2], b[(i + 1) // 2])
                for i in range(8):
                    value = line(sums.terms[i])
                    ROW[i, k, pl.ds(j, 1), :] = value
                    ROW[i, j, pl.ds(k, 1), :] = value

            return 0

        lax.fori_loop(0, e + 1, pair, 0)

    def cross_sums(k, h):
        sums = Sums()
        rows = pl.ds(pl.multiple_of(HALF_LOW + 64 * h, 8), HALF_END - HALF_LOW)
        for t in range(4):
            value = TH[h, k, t, HALF_LOW:HALF_END, :]
            for i, ref in enumerate(g3_powers + g2_powers):
                sums.add(i, value, ref[t, rows, :])
        for i in range(13):
            CR[k, i : i + 1, :] = CR[k, i : i + 1, :] + line(sums.terms[i])

    def first_hand(e):
        k, dx, odd, valid = slab_at(e)

        @pl.when(valid)
        def _():
            @pl.when((e > 0) | (core == 0))
            def _():
                with jax.named_scope("b1_slabwait"):
                    landed(half_copies(k, core, ts.at[0, 0], sib))

            @pl.when((dx == 1) & (core == 0) & ((chip == 1) | (chip == 2)) & (e > 0))
            def _():
                start(half_copies(k, 0, rs.at[odd], jnp.maximum(tm - 2, 0)))

            @pl.when((dx == 3) & (core == 1) & (chip == 0) & (e > 0))
            def _():
                start(half_copies(k, 1, rs.at[odd], 3))

            @pl.when(e > 0)
            def _():
                start(half_copies(k, core, fs.at[e], sib))

            @pl.when(k > tm)
            def _():
                unpack(k, core)

            gram_sums(e, k)

            @pl.when(k > tm)
            def _():
                cross_sums(k, core)

    def second_hand(e):
        k, _, _, valid = slab_at(e)

        @pl.when(valid & (k > tm))
        def _():
            with jax.named_scope("b1_sibwait"):
                landed(half_copies(k, 1 - core, ts.at[0, 0], sib))
            unpack(k, 1 - core)
            cross_sums(k, 1 - core)

    def arrive(i, _):
        @pl.when(i < 7)
        def _():
            first_hand(jnp.minimum(i, 6))

        @pl.when(i >= 3)
        def _():
            second_hand(jnp.maximum(i - 3, 0))

        return 0

    @pl.when(tm == 7)
    def _():
        refs = [F.at[CG], U, W, V, X]
        for src, dst in zip(refs, refs[1:]):
            power(src, dst)
        for i in range(8):
            KQ[16 + i : 17 + i, :] = own_sum(refs[i // 2], refs[(i + 1) // 2])
        for i, ref in enumerate(g3_powers + g2_powers):
            CR[0, i : i + 1, :] = own_sum(refs[0], ref)

    @pl.when(tm == 7)
    def _():
        for odd in (1, 0):
            landed(half_copies(4 + odd, 1, ts.at[0, 0], sib))
            start(half_copies(4 + odd, 1, rs.at[odd], 1))

    phase("b1_arrive")
    lax.fori_loop(0, 10, arrive, 0)

    phase("b2_gram")
    lane3 = lane_iota((8, 8, LANES))
    sub3 = lax.broadcasted_iota(jnp.int32, (8, 8, LANES), 1)
    gram = jnp.zeros((8, 8, LANES), jnp.float32)
    for i in range(8):
        gram = jnp.where(lane3 == 8 * i + sub3, jnp.sum(ROW[i], axis=2, keepdims=True), gram)
    gram = jnp.sum(gram, axis=1)
    lane4 = lane_iota((8, 16, LANES))
    sub4 = lax.broadcasted_iota(jnp.int32, (8, 16, LANES), 1)
    cross = jnp.where(lane4 == 64 + sub4, jnp.sum(CR[...], axis=2, keepdims=True), 0.0)
    gram = gram + jnp.sum(cross, axis=1)
    lane5 = lane_iota((24, LANES))
    sub5 = lax.broadcasted_iota(jnp.int32, (24, LANES), 0)
    own = jnp.where(lane5 == 80 + sub5, jnp.sum(KQ[...], axis=1, keepdims=True), 0.0)
    own = jnp.sum(own, axis=0, keepdims=True)
    gram = gram + jnp.where(lax.broadcasted_iota(jnp.int32, (8, LANES), 0) == 0, own, 0.0)
    GM[...] = gram
    GR[core * 16 + me] = gram
    pl.semaphore_wait(plane_sem, 1)

    def send_gram(step, _):
        there = lax.rem(me + step, 16)
        place = {"lat": there // 4, "lon": there % 4}

        @pl.when(step < 16)
        def _():
            pltpu.make_async_remote_copy(
                GM, GR.at[core * 16 + me], gs, gr, device_id=place, device_id_type=MESH
            ).start()

        pltpu.make_async_remote_copy(
            GM, GR.at[core * 16 + me], gs, gr, device_id={"tm": sib, **place}, device_id_type=MESH
        ).start()
        return 0

    lax.fori_loop(1, 17, send_gram, 0)
    phase("b3_wait")
    box = GR.at[pl.ds(0, 31)]
    pltpu.make_async_copy(box, box, gr).wait()
    total = jnp.sum(GR[...], axis=0)
    plane = jnp.sum(GR[pl.ds(core * 16, 16)], axis=0)
    phase("b4_chain")

    lane = lane_iota((8, LANES))

    def column(source, i):
        picked = jnp.sum(jnp.where(lane == i, source, 0.0), axis=1, keepdims=True)
        return jnp.broadcast_to(picked, (8, LANES))

    table = [[None if j == 0 else column(total, 8 * i + j) for j in range(8)] for i in range(8)]
    with_g = [column(plane, 64 + i) for i in range(13)]
    first_row = [column(plane, 80 + i)[0:1, :] for i in range(24)]
    k33, k32, k22 = first_row[:6], first_row[6:11], first_row[11:15]

    def entry(i, k, j):
        return table[i][j][k : k + 1, :]

    one = jnp.ones((1, LANES), jnp.float32)
    zero = jnp.zeros((1, LANES), jnp.float32)
    coefs = {7: one}
    quad = [entry(i, 7, 7) for i in range(8)]
    cross = [{j: entry(i, 7, j) for j in range(1, 7)} for i in range(8)]
    mixed = [x[7:8, :] for x in with_g]
    is_last = jnp.full((1, LANES), tm == 7)
    held_c = {k: zero for k in range(1, 8)}
    held_q = first_row[16:24]
    held_m = [x[0:1, :] for x in with_g]
    for t in range(7, 0, -1):
        if t < 7:
            psi_t = quad[0] / (quad[0] + 4.0 * quad[1] + EPS)
            quad = [
                psi_t * psi_t * quad[i] + 2.0 * psi_t * cross[i][t] + entry(i, t, t)
                for i in range(8)
            ]
            cross = [{j: psi_t * cross[i][j] + entry(i, t, j) for j in range(1, t)} for i in range(8)]
            mixed = [psi_t * x + y[t : t + 1, :] for x, y in zip(mixed, with_g)]
            coefs = {k: psi_t * x for k, x in coefs.items()}
            coefs[t] = one
        now = jnp.full((1, LANES), tm + 1 == t)
        for k in coefs:
            held_c[k] = jnp.where(now, coefs[k], held_c[k])
        held_q = [jnp.where(now, quad[i], held_q[i]) for i in range(8)]
        held_m = [jnp.where(now, mixed[i], held_m[i]) for i in range(13)]
    psi = held_q[0] / (held_q[0] + 4.0 * held_q[1] + EPS)
    psi = jnp.where(is_last, 0.0, psi)
    for row, count in FULL:
        part = slice(row, row + count)
        value = F[CG, :, part, :] * last
        for k in range(1, 8):
            slab = TH[row // 80, k, :, row - 64 * (row // 80) : row - 64 * (row // 80) + count, :]
            value = value + scaled(held_c[k], jnp.where(tm < k, slab, 0.0))
        V[:, part, :] = value

    def put(level, row, value):
        for t in range(4):
            out[level, row - LOW : row - LOW + value.shape[1], cols(t)] = value[t]

    def next_moments(a, b, m, n, k, count):
        return [
            jnp.maximum(
                a * a * m[i] + 2.0 * a * b * m[i + 1] + b * b * m[i + 2]
                + 2.0 * (a * n[i] + b * n[i + 1]) + k[i],
                0.0,
            )
            for i in range(count)
        ]

    a1, b1 = fine_coefs(held_q)
    m1 = next_moments(a1, b1, held_q, held_m[:7], k33, 6)
    n1 = [a1 * held_m[7 + i] + b1 * held_m[8 + i] + k32[i] for i in range(5)]
    a2, b2 = fine_coefs(m1)
    m2 = next_moments(a2, b2, m1, n1, k22, 4)
    a3, b3 = fine_coefs(m2)
    phase("c0_correct")
    for row, count in FULL:
        part = slice(row, row + count)
        v, u = spread(V, K, row, count)
        value = scaled(a1, v) + scaled(b1, u) + F[G3, :, part, :]
        X[:, part, :] = value
        put(3, max(row, LOW), own_part(value, row, count))
    for row, count in FULL:
        part = slice(row, row + count)
        v, u = spread(X, K, row, count)
        value = scaled(a2, v) + scaled(b2, u) + F[G2, :, part, :]
        W[:, part, :] = value
        put(2, max(row, LOW), own_part(value, row, count))
    for row, count in OWN:
        part = slice(row, row + count)
        v, u = spread(W, K, row, count)
        put(1, row, scaled(a3, v[:4]) + scaled(b3, u[:4]) + F[G1, :4, part, :])
        first = row - 64 * (row // 80)
        put(0, row, scaled(psi, V[:4, part, :]) + TH[row // 80, tm, :4, first : first + count, :])

    phase("c9_end")
    for copy in halos:
        copy.wait_send()
    for r in range(2):
        box = AR.at[r, pl.ds(0, 15)]
        pltpu.make_async_copy(box, box, ar_s.at[r]).wait()
    box = GR.at[pl.ds(0, 31)]
    pltpu.make_async_copy(box, box, gs).wait()
    own_sends(sent)
    for e in range(1, 7):
        k, _, _, valid = slab_at(e)

        @pl.when(valid)
        def _():
            sent(half_copies(k, core, fs.at[e], sib))

    relays = ((core == 0) & ((chip == 1) | (chip == 2))) | ((core == 1) & ((chip == 0) | (chip == 3)))

    @pl.when(relays)
    def _():
        for odd in range(2):
            sent(half_copies(0, core, rs.at[odd], sib))

    phase(None)


def local(forcing, depth, mask, guess):
    f32 = jnp.float32
    field = (TILES, ROWS, LANES)
    half = (TILES, HALF_ROWS, LANES)
    dma = pltpu.SemaphoreType.DMA
    return pl.pallas_call(
        kernel,
        out_shape=jax.ShapeDtypeStruct(forcing.shape, f32),
        in_specs=[pl.BlockSpec(memory_space=pltpu.HBM)] * 4,
        out_specs=pl.BlockSpec(memory_space=pltpu.VMEM),
        scratch_shapes=[
            pltpu.VMEM((6, *field), f32),
            pltpu.VMEM((4, *field), f32),
            pltpu.VMEM(field, f32),
            pltpu.VMEM(field, f32),
            pltpu.VMEM(field, f32),
            pltpu.VMEM(field, f32),
            pltpu.VMEM((3, *field), f32),
            pltpu.VMEM((9, *field), f32),
            pltpu.VMEM((4, *half), f32),
            pltpu.VMEM((2, 8, *half), f32),
            pltpu.VMEM((8, *half), f32),
            pltpu.VMEM((8, *half), f32),
            pltpu.VMEM((8, *half), f32),
            pltpu.VMEM((8, 4, 64, LANES), f32),
            pltpu.VMEM((4, 128, LANES), f32),
            pltpu.VMEM((4, 128, LANES), jnp.int32),
            pltpu.VMEM((3, 4, 8, LANES), f32),
            pltpu.VMEM((8, 8, 8, LANES), f32),
            pltpu.VMEM((8, 16, LANES), f32),
            pltpu.VMEM((24, LANES), f32),
            pltpu.VMEM((2, 6, 8, LANES), f32),
            pltpu.VMEM((2, 6, 8, LANES), f32),
            pltpu.VMEM((4, 8, LANES), f32),
            pltpu.VMEM((4, 8, LANES), f32),
            pltpu.VMEM((8, 2, 8, LANES), f32),
            pltpu.VMEM((2, 16, LANES), f32),
            pltpu.VMEM((2, 16, 16, LANES), f32),
            pltpu.VMEM((8, LANES), f32),
            pltpu.VMEM((32, 8, LANES), f32),
            dma((7, 4)),
            dma((10,)),
            dma((10,)),
            dma((2,)),
            dma((2,)),
            dma((3, 2, 2)),
            dma((8, 2)),
            dma((8, 2)),
            dma((7, 2)),
            dma((2, 2)),
            dma,
            dma,
            pltpu.SemaphoreType.REGULAR,
        ],
        compiler_params=pltpu.CompilerParams(
            collective_id=0, has_side_effects=True, vmem_limit_bytes=VMEM_LIMIT
        ),
        name="cycle",
    )(*(pltpu.with_memory_space_constraint(x, pltpu.HBM) for x in (forcing, depth, mask, guess)))


def solution(mesh):
    return jax.shard_map(
        local,
        mesh=mesh,
        in_specs=(P("tm", "lat", "lon"), P("lat", "lon"), P("lat", "lon"), P("tm", "lat", "lon")),
        out_specs=P("tm", "lat", "lon"),
        check_vma=False,
    )
```

```python
import functools

import jax
import jax.numpy as jnp
from jax import lax
from jax.experimental import pallas as pl
from jax.experimental.pallas import tpu as pltpu
from jax.sharding import PartitionSpec as P

FS = 4
EPS = 1e-6
VMEM_LIMIT = 40 * 1024 * 1024
MESH = pl.DeviceIdType.MESH

TILES, ROWS, LANES = 5, 160, 128
TOP, LOW, END = 8, 16, 144
FULL = tuple((row, 24) for row in range(8, 152, 24))
OWN = tuple((row, 32) for row in range(16, 144, 32))
HALF_ROWS = 96
HALF = ((8, 24), (32, 24), (56, 32))
HALF_OWN = ((16, 32), (48, 32))
HALF_LOW, HALF_END = 16, 80
DM, CG, G3, G2, G1, G0 = range(6)


def lane_iota(shape):
    return lax.broadcasted_iota(jnp.int32, shape, len(shape) - 1)


def sides(ref, row, count):
    v = ref[:, row : row + count, :]
    down = ref[:, row + 1 : row + 1 + count, :]
    up = ref[:, row - 1 : row - 1 + count, :]
    lane = lane_iota(v.shape)
    ahead = pltpu.roll(v, LANES - 1, 2)
    right = jnp.where(lane == LANES - 1, jnp.concatenate([ahead[1:], ahead[:1]], 0), ahead)
    behind = pltpu.roll(v, 1, 2)
    left = jnp.where(lane == 0, jnp.concatenate([behind[-1:], behind[:-1]], 0), behind)
    return v, right, left, down, up


def spread(ref, coef, row, count):
    v, right, left, down, up = sides(ref, row, count)
    part = slice(row, row + count)
    out = coef[0, :, part, :] * (v - right) + coef[1, :, part, :] * (v - left)
    out = out + coef[2, :, part, :] * (v - down) + coef[3, :, part, :] * (v - up)
    return v, out


def own_part(x, row, count):
    first, last = max(row, LOW) - row, min(row + count, END) - row
    return x[:4, first:last, :]


def fold(x):
    return jnp.sum(x.reshape(-1, 8, LANES), axis=0)


class Phase:
    def __init__(self):
        self.open = None

    def __call__(self, name):
        if self.open is not None:
            self.open.__exit__(None, None, None)
        self.open = jax.named_scope(name) if name else None
        if self.open is not None:
            self.open.__enter__()


class Sums:
    def __init__(self):
        self.terms = {}

    def add(self, key, a, b):
        value = fold(a * b)
        self.terms[key] = value if key not in self.terms else self.terms[key] + value


def fine_coefs(m):
    den = m[0] + m[1] + EPS
    alpha = m[0] / den
    gamma = (m[1] + EPS) / den
    s1 = jnp.maximum(
        gamma * gamma * m[0] - 2.0 * gamma * alpha * m[1] + alpha * alpha * m[2], 0.0
    )
    beta = s1 / (m[0] + EPS)
    f = gamma + beta
    pp = s1 + beta * (2.0 * EPS * alpha + beta * m[0])
    plp = jnp.maximum(f * f * m[1] - 2.0 * f * alpha * m[2] + alpha * alpha * m[3], 0.0)
    later = jnp.minimum(s1 / (pp + plp + EPS), 1.0)
    return alpha + later * f, -alpha * later


def kernel(
    forcing, depth, mask, guess, out,
    F, K, V, X, U, W, LG, GP, KH, TH, UG, TG2, TG3, TG4, DEP, MSK, KAP, ROW, CR, KQ,
    PKS, PKR, CKS, CKR, PT, MSG, AR,
    GM, GR, BOX, in_sem, hs, hr, ar_s, ar_r, ts, tr, fs, rs, gs, gr, plane_sem,
):
    phase = Phase()
    phase("a0_load")
    tm = lax.axis_index("tm")
    lat = lax.axis_index("lat")
    lon = lax.axis_index("lon")
    me = lat * 4 + lon
    chip, core = tm // 2, tm % 2
    sib = 2 * chip + 1 - core

    def cols(c):
        return pl.ds(LANES * c, LANES)

    barrier = pltpu.get_barrier_semaphore()
    north, south = lax.rem(lat + 3, 4), lax.rem(lat + 1, 4)
    west, east = lax.rem(lon + 3, 4), lax.rem(lon + 1, 4)

    def greet(target):
        pl.semaphore_signal(barrier, inc=1, device_id=target, device_id_type=MESH)

    for a in (north, south):
        for b in (west, east):
            greet({"lat": a, "lon": b})
    for step in (4, 3, 5, 2, 6, 1, 7):
        greet({"tm": lax.rem(tm + step, 8)})
    for a in (north, south):
        greet({"lat": a})
    for b in (west, east):
        greet({"lon": b})

    own_rows = pl.ds(LOW, END - LOW)

    for c in range(4):
        pltpu.make_async_copy(depth.at[:, cols(c)], DEP.at[c], in_sem.at[0]).start()
        pltpu.make_async_copy(mask.at[:, cols(c)], MSK.at[c], in_sem.at[1]).start()
        pltpu.make_async_copy(
            guess.at[0, :, cols(c)], F.at[CG, c, own_rows, :], in_sem.at[2]
        ).start()
    for field, level in ((G3, 3), (G2, 2), (G1, 1), (G0, 0)):
        for c in range(4):
            pltpu.make_async_copy(
                forcing.at[level, :, cols(c)], F.at[field, c, own_rows, :], in_sem.at[2]
            ).start()

    phase("a1_clear")
    def clear(ref):
        zero = jnp.zeros((TILES, 8, LANES), jnp.float32)
        ref[:, 0:8, :] = zero
        ref[:, 152:160, :] = zero

    def clear_fields(i, _):
        clear(F.at[i])
        return 0

    lax.fori_loop(0, 6, clear_fields, 0)
    for ref in (V, X, U):
        clear(ref)

    def clear_slab(i, _):
        ROW[:, i] = jnp.zeros((8, 8, LANES), jnp.float32)
        CR[i] = jnp.zeros((16, LANES), jnp.float32)
        return 0

    lax.fori_loop(0, 8, clear_slab, 0)
    KQ[...] = jnp.zeros((24, LANES), jnp.float32)
    for i in range(9):
        clear(GP.at[i])
    for i in range(3):
        clear(LG.at[i])

    phase("a2_loadwait")
    fields = F.at[pl.ds(1, 5), pl.ds(0, 4), own_rows, :]
    for i, ref in enumerate((DEP, MSK, fields)):
        pltpu.make_async_copy(ref, ref, in_sem.at[i]).wait()
    for c in range(4):
        F[DM, c, LOW:END, :] = jnp.where(MSK[c] > 0, DEP[c], 0.0)

    phase("a3_pack")
    lane6 = lane_iota((6, 8, LANES))
    right_edge = jnp.zeros((6, 8, LANES), jnp.float32)
    left_edge = jnp.zeros((6, 8, LANES), jnp.float32)
    for t in range(16):
        here = (lane6 >= 8 * t) & (lane6 < 8 * t + 8)
        rows = slice(LOW + 8 * t, LOW + 8 * t + 8)
        right_edge = jnp.where(here, pltpu.roll(F[:, 3, rows, :], (8 * t + 8) % LANES, 2), right_edge)
        left_edge = jnp.where(here, pltpu.roll(F[:, 0, rows, :], 8 * t, 2), left_edge)
    PKS[0] = right_edge
    PKS[1] = left_edge
    lane1 = lane_iota((8, LANES))
    corners = ((136, 3, 8), (136, 0, 0), (16, 3, 8), (16, 0, 0))
    for i, (row, tile, shift) in enumerate(corners):
        packed = jnp.zeros((8, LANES), jnp.float32)
        for f in range(6):
            here = (lane1 >= 8 * f) & (lane1 < 8 * f + 8)
            edge = pltpu.roll(F[f, tile, row : row + 8, :], (8 * f + shift) % LANES, 1)
            packed = jnp.where(here, edge, packed)
        CKS[i] = packed

    phase("a4_barrier")
    pl.semaphore_wait(barrier, 15)


    def push(src, dst, i, target):
        pltpu.make_async_remote_copy(
            src, dst, hs, hr.at[i], device_id=target, device_id_type=MESH
        ).start()

    def wait_rows(sem, count):
        box = BOX.at[pl.ds(0, count)]
        pltpu.make_async_copy(box, box, sem).wait()

    targets = ((south, east), (south, west), (north, east), (north, west))
    for i, (a, b) in enumerate(targets):
        push(CKS.at[i], CKR.at[i], 0, {"lat": a, "lon": b})
    push(PKS.at[0], PKR.at[0], 0, {"lon": east})
    push(PKS.at[1], PKR.at[1], 0, {"lon": west})
    for i, first in ((0, 0), (1, 3)):
        group = pl.ds(first, 3)
        push(
            F.at[group, pl.ds(0, 4), pl.ds(136, 8), :],
            F.at[group, pl.ds(0, 4), pl.ds(8, 8), :],
            i, {"lat": south},
        )
        push(
            F.at[group, pl.ds(0, 4), pl.ds(16, 8), :],
            F.at[group, pl.ds(0, 4), pl.ds(144, 8), :],
            i, {"lat": north},
        )
    phase("a5_halowait")
    wait_rows(hr.at[0], 4 * 8 + 2 * 48 + 2 * 96)

    pl.semaphore_signal(plane_sem, inc=1, device_id={"tm": sib}, device_id_type=MESH)
    phase("a6_unpack")
    from_left, from_right = PKR[0], PKR[1]
    for t in range(16):
        rows = slice(LOW + 8 * t, LOW + 8 * t + 8)
        a = pltpu.roll(from_left, (120 - 8 * t) % LANES, 2)
        b = pltpu.roll(from_right, (LANES - 8 * t) % LANES, 2)
        F[:, 4, rows, :] = jnp.where(lane6 >= 120, a, jnp.where(lane6 < 8, b, 0.0))
    for row, left, right in ((8, 0, 1), (144, 2, 3)):
        a0, b0 = CKR[left], CKR[right]
        for f in range(6):
            a = pltpu.roll(a0, (120 - 8 * f) % LANES, 1)
            b = pltpu.roll(b0, (LANES - 8 * f) % LANES, 1)
            F[f, 4, row : row + 8, :] = jnp.where(lane1 >= 120, a, jnp.where(lane1 < 8, b, 0.0))

    inside_top = jnp.where(lat > 0, 1.0, 0.0).astype(jnp.float32)
    inside_end = jnp.where(lat < 3, 1.0, 0.0).astype(jnp.float32)
    F[DM, :, 8:16, :] = F[DM, :, 8:16, :] * inside_top
    F[DM, :, 144:152, :] = F[DM, :, 144:152, :] * inside_end

    for row, count in FULL:
        d, *around = sides(F.at[DM], row, count)
        for i, other in enumerate(around):
            K[i, :, row : row + count, :] = jnp.where(
                (d > 0.0) & (other > 0.0), 1.5 * (d + other), 0.0
            )

    far_first = sorted(
        ((a, b) for a in range(4) for b in range(4) if (a, b) != (0, 0)),
        key=lambda ab: -(min(ab[0], 4 - ab[0]) + min(ab[1], 4 - ab[1])),
    )

    def plane_peer(a, b):
        return {"lat": lax.rem(lat + a, 4), "lon": lax.rem(lon + b, 4)}

    def diagonal(x, count):
        shape = (count, LANES)
        here = lane_iota(shape) == lax.broadcasted_iota(jnp.int32, shape, 0)
        picked = jnp.where(here, jnp.broadcast_to(x, shape), 0.0)
        return jnp.broadcast_to(jnp.sum(picked, axis=1, keepdims=True), shape)

    def send_sums(r, accs):
        row = lax.broadcasted_iota(jnp.int32, (16, LANES), 0)
        stacked = jnp.zeros((16, LANES), jnp.float32)
        for i, acc in enumerate(accs):
            stacked = jnp.where(row == i, jnp.sum(acc, axis=0, keepdims=True), stacked)
        stacked = jnp.broadcast_to(jnp.sum(stacked, axis=1, keepdims=True), (16, LANES))
        message = jnp.where(lane_iota((16, LANES)) == row, stacked, 0.0)
        message = jnp.sum(message, axis=0, keepdims=True)
        MSG[r, 0:1, :] = message
        AR[r, pl.ds(me, 1), :] = message
        for a, b in far_first:
            pltpu.make_async_remote_copy(
                MSG.at[r, pl.ds(0, 1)], AR.at[r, pl.ds(me, 1)], ar_s.at[r], ar_r.at[r],
                device_id=plane_peer(a, b), device_id_type=MESH,
            ).start()

    def recv_sums(r):
        wait_rows(ar_r.at[r], 15)
        return diagonal(jnp.sum(AR[r], axis=0, keepdims=True), 16)

    def prepare(field, slot):
        sums = Sums()
        for row, count in FULL:
            g, lg = spread(F.at[field], K, row, count)
            LG[slot, :, row : row + count, :] = lg
            g, lg = own_part(g, row, count), own_part(lg, row, count)
            sums.add(0, g, g)
            sums.add(1, g, lg)
            sums.add(2, lg, lg)
        for row, count in OWN:
            lg, llg = spread(LG.at[slot], K, row, count)
            sums.add(3, lg[:4], llg[:4])
        for i in range(4):
            KAP[slot, i] = sums.terms[i]

    def power(src, dst):
        for row, count in FULL:
            dst[:, row : row + count, :] = spread(src, K, row, count)[1]

    def line(acc):
        return jnp.sum(acc, axis=0, keepdims=True)

    def own_sum(a, b):
        return line(fold(a[:4, LOW:END, :] * b[:4, LOW:END, :]))

    g3_powers = [F.at[G3], LG.at[0]] + [GP.at[i] for i in range(5)]
    g2_powers = [F.at[G2], LG.at[2]] + [GP.at[i] for i in range(5, 9)]

    def powers_of_g3():
        for src, dst in zip(g3_powers[1:], g3_powers[2:]):
            power(src, dst)

    def powers_of_g2():
        prepare(G2, 2)
        for src, dst in zip(g2_powers[1:], g2_powers[2:]):
            power(src, dst)
        for i in range(4):
            KQ[i : i + 1, :] = line(KAP[0, i])
            KQ[11 + i : 12 + i, :] = line(KAP[2, i])
        KQ[4:5, :] = own_sum(g3_powers[2], g3_powers[2])
        KQ[5:6, :] = own_sum(g3_powers[2], g3_powers[3])
        for i in range(5):
            KQ[6 + i : 7 + i, :] = own_sum(g2_powers[0], g3_powers[i])

    def two_steps(r, v_ref, field, slot, between):
        phase(f"r{r}_moments")
        sums = Sums()
        for row, count in FULL:
            v, u = spread(v_ref, K, row, count)
            U[:, row : row + count, :] = u
            g = own_part(F[field, :, row : row + count, :], row, count)
            v, u = own_part(v, row, count), own_part(u, row, count)
            sums.add("m0", v, v)
            sums.add("m1", v, u)
            sums.add("m2", u, u)
            sums.add("n0", v, g)
            sums.add("n1", u, g)
        for row, count in FULL:
            u, w = spread(U, K, row, count)
            W[:, row : row + count, :] = w
            lg = own_part(LG[slot, :, row : row + count, :], row, count)
            u, w = own_part(u, row, count), own_part(w, row, count)
            sums.add("m3", u, w)
            sums.add("m4", w, w)
            sums.add("n2", u, lg)
            sums.add("n3", w, lg)
        for row, count in OWN:
            w, lw = spread(W, K, row, count)
            lg = LG[slot, :4, row : row + count, :]
            sums.add("m5", w[:4], lw[:4])
            sums.add("n4", lw[:4], lg)
        names = ["m0", "m1", "m2", "m3", "m4", "m5", "n0", "n1", "n2", "n3", "n4"]
        accs = [sums.terms[n] for n in names] + [KAP[slot, i] for i in range(4)]
        send_sums(r, accs)
        phase(f"r{r}_between")
        between()
        phase(f"r{r}_wait")
        total = recv_sums(r)
        phase(f"r{r}_scalars")
        at = [total[i : i + 1, :] for i in range(15)]
        m, n, k = at[:6], at[6:11], at[11:]
        a, b = fine_coefs(m)
        later = [
            jnp.maximum(
                a * a * m[i] + 2.0 * a * b * m[i + 1] + b * b * m[i + 2]
                + 2.0 * (a * n[i] + b * n[i + 1]) + k[i],
                0.0,
            )
            for i in range(4)
        ]
        a2, b2 = fine_coefs(later)
        return m, (a, b), (a2 * a, a2 * b + b2 * a, b2 * b, a2, b2)

    def scaled(s, x):
        return jnp.broadcast_to(s.reshape(1, 1, LANES), x.shape) * x

    phase("a7_prepare")
    prepare(G3, 0)

    def rest_of_halo():
        wait_rows(hr.at[1], 2 * 96)
        prepare(G1, 1)
        powers_of_g3()
        rows = pl.ds(pl.multiple_of(8 + 64 * core, 8), 80)
        for i in range(4):
            KH[i, :, 8:88, :] = K[i, :, rows, :]

    m_start, _, c = two_steps(0, F.at[CG], G3, 0, rest_of_halo)
    for row, count in FULL:
        part = slice(row, row + count)
        X[:, part, :] = (
            scaled(c[0], F[CG, :, part, :]) + scaled(c[1], U[:, part, :]) + scaled(c[2], W[:, part, :])
            + scaled(c[3], F[G3, :, part, :]) + scaled(c[4], LG[0, :, part, :]) + F[G2, :, part, :]
        )
    last = jnp.where(tm == 7, 1.0, 0.0).astype(jnp.float32)
    psi = m_start[0] / (m_start[0] + 4.0 * m_start[1] + EPS)
    drop = psi * (last - 1.0)

    _, _, c = two_steps(1, X, G1, 1, powers_of_g2)
    for h in range(2):
        for row, count in HALF:
            part = slice(64 * h + row, 64 * h + row + count)
            TH[h, tm, :, row : row + count, :] = (
                scaled(c[0], X[:, part, :]) + scaled(c[1], U[:, part, :])
                + scaled(c[2], W[:, part, :]) + scaled(c[3], F[G1, :, part, :])
                + scaled(c[4], LG[1, :, part, :]) + F[G0, :, part, :]
                + scaled(drop, F[CG, :, part, :])
            )

    phase("b0_gather")
    lane2 = lane_iota((8, LANES))
    for h in range(2):
        packed = jnp.zeros((8, LANES), jnp.float32)
        for t in range(10):
            row = 8 + 8 * t
            here = (lane2 >= 8 * t) & (lane2 < 8 * t + 8)
            edge = pltpu.roll(TH[h, tm, 4, row : row + 8, :], 8 * t + 4, 1)
            packed = jnp.where(here, edge, packed)
        PT[tm, h] = packed

    def half_copies(k, h, sem, target):
        main = TH.at[h, k, pl.ds(0, 4), pl.ds(12, 72), :]
        return [
            pltpu.make_async_remote_copy(
                ref, ref, sem, tr.at[k, h], device_id={"tm": target}, device_id_type=MESH
            )
            for ref in (main, PT.at[k, h])
        ]

    def start(copies):
        for copy in copies:
            copy.start()

    def sent(sem):
        wait_rows(sem, 4 * 72 + 8)

    def landed(k, h):
        wait_rows(tr.at[k, h], 4 * 72 + 8)

    def own_sends(act):
        for h in range(2):
            @pl.when(core == 1)
            def _():
                act(h, ts.at[0, h], sib)

            @pl.when(chip == 3)
            def _():
                act(h, ts.at[1, h], h)

            @pl.when(chip >= 1)
            def _():
                act(h, ts.at[2, h], jnp.maximum(2 * chip - 2 + h, 0))

            if h == 1:
                @pl.when(chip == 2)
                def _():
                    act(h, ts.at[1, h], 7)

    own_sends(lambda h, sem, target: start(half_copies(tm, h, sem, target)))

    def slab_at(e):
        dx = jnp.where((e == 1) | (e == 3), 1, jnp.where((e == 2) | (e == 5), 3, 2))
        odd = jnp.where((e == 1) | (e == 2) | (e == 4), 1, 0)
        k = jnp.where(e == 0, 2 * chip + 1, 2 * (chip + dx) + odd)
        valid = (e == 0) | (chip + dx <= 3)
        return jnp.minimum(k, 7), dx, odd, valid

    def unpack(k, h):
        packed = PT[k, h]
        for t in range(10):
            back = pltpu.roll(packed, (LANES - 8 * t - 4) % LANES, 1)
            back = jnp.where((lane2 < 4) | (lane2 >= 124), back, 0.0)
            TH[h, k, 4, 8 + 8 * t : 16 + 8 * t, :] = back

    def gram_sums(e, k):
        refs = [TH.at[core, k], UG.at[k], TG2.at[k], TG3.at[k]]
        for src, dst in zip(refs, refs[1:]):
            for row, count in HALF:
                dst[:, row : row + count, :] = spread(src, KH, row, count)[1]
        for row, count in HALF_OWN:
            last_power = spread(refs[3], KH, row, count)[1]
            TG4[k, :, row - HALF_LOW : row - HALF_LOW + count, :] = last_power[:4]

        def pair(q, _):
            j, _, _, held = slab_at(q)

            @pl.when(held)
            def _():
                sums = Sums()
                low, high = jnp.minimum(j, k), jnp.maximum(j, k)
                for t in range(4):
                    a, b = (
                        [TH[core, s, t, HALF_LOW:HALF_END, :]]
                        + [ref[s, t, HALF_LOW:HALF_END, :] for ref in (UG, TG2, TG3)]
                        for s in (low, high)
                    )
                    b.append(TG4[high, t])
                    for i in range(8):
                        sums.add(i, a[i // 2], b[(i + 1) // 2])
                for i in range(8):
                    value = line(sums.terms[i])
                    ROW[i, k, pl.ds(j, 1), :] = value
                    ROW[i, j, pl.ds(k, 1), :] = value

            return 0

        lax.fori_loop(0, e + 1, pair, 0)

    def cross_sums(k, h):
        sums = Sums()
        rows = pl.ds(pl.multiple_of(HALF_LOW + 64 * h, 8), HALF_END - HALF_LOW)
        for t in range(4):
            value = TH[h, k, t, HALF_LOW:HALF_END, :]
            for i, ref in enumerate(g3_powers + g2_powers):
                sums.add(i, value, ref[t, rows, :])
        for i in range(13):
            CR[k, i : i + 1, :] = CR[k, i : i + 1, :] + line(sums.terms[i])

    def first_hand(e):
        k, dx, odd, valid = slab_at(e)

        @pl.when(valid)
        def _():
            @pl.when((e > 0) | (core == 0))
            def _():
                with jax.named_scope("b1_slabwait"):
                    landed(k, core)

            @pl.when((dx == 1) & (core == 0) & ((chip == 1) | (chip == 2)) & (e > 0))
            def _():
                start(half_copies(k, 0, rs.at[odd], jnp.maximum(tm - 2, 0)))

            @pl.when((dx == 3) & (core == 1) & (chip == 0) & (e > 0))
            def _():
                start(half_copies(k, 1, rs.at[odd], 3))

            @pl.when(e > 0)
            def _():
                start(half_copies(k, core, fs.at[e], sib))

            @pl.when(k > tm)
            def _():
                unpack(k, core)

            gram_sums(e, k)

            @pl.when(k > tm)
            def _():
                cross_sums(k, core)

    def second_hand(e):
        k, _, _, valid = slab_at(e)

        @pl.when(valid & (k > tm))
        def _():
            with jax.named_scope("b1_sibwait"):
                landed(k, 1 - core)
            unpack(k, 1 - core)
            cross_sums(k, 1 - core)

    def arrive(i, _):
        @pl.when(i < 7)
        def _():
            first_hand(jnp.minimum(i, 6))

        @pl.when(i >= 3)
        def _():
            second_hand(jnp.maximum(i - 3, 0))

        return 0

    @pl.when(tm == 7)
    def _():
        refs = [F.at[CG], U, W, V, X]
        for src, dst in zip(refs, refs[1:]):
            power(src, dst)
        for i in range(8):
            KQ[16 + i : 17 + i, :] = own_sum(refs[i // 2], refs[(i + 1) // 2])
        for i, ref in enumerate(g3_powers + g2_powers):
            CR[0, i : i + 1, :] = own_sum(refs[0], ref)

    @pl.when(tm == 7)
    def _():
        for odd in (1, 0):
            landed(4 + odd, 1)
            start(half_copies(4 + odd, 1, rs.at[odd], 1))

    phase("b1_arrive")
    lax.fori_loop(0, 10, arrive, 0)

    phase("b2_gram")
    lane3 = lane_iota((8, 8, LANES))
    sub3 = lax.broadcasted_iota(jnp.int32, (8, 8, LANES), 1)
    gram = jnp.zeros((8, 8, LANES), jnp.float32)
    for i in range(8):
        gram = jnp.where(lane3 == 8 * i + sub3, jnp.sum(ROW[i], axis=2, keepdims=True), gram)
    gram = jnp.sum(gram, axis=1)
    lane4 = lane_iota((8, 16, LANES))
    sub4 = lax.broadcasted_iota(jnp.int32, (8, 16, LANES), 1)
    slab4 = lax.broadcasted_iota(jnp.int32, (8, 16, LANES), 0)
    cross = jnp.where(
        (lane4 == 13 * slab4 + sub4) & (sub4 < 13), jnp.sum(CR[...], axis=2, keepdims=True), 0.0
    )
    cross = jnp.sum(jnp.sum(cross, axis=0), axis=0, keepdims=True)
    lane5 = lane_iota((24, LANES))
    sub5 = lax.broadcasted_iota(jnp.int32, (24, LANES), 0)
    own = jnp.where(lane5 == 104 + sub5, jnp.sum(KQ[...], axis=1, keepdims=True), 0.0)
    own = cross + jnp.sum(own, axis=0, keepdims=True)
    sub2 = lax.broadcasted_iota(jnp.int32, (8, LANES), 0)
    folded = jnp.where(lane2 < 64, pltpu.roll(gram, 4, 0), pltpu.roll(gram, 64, 1))
    message = jnp.where(sub2 < 4, folded, jnp.where(sub2 == 4, own, 0.0))
    GM[...] = message
    GR[core * 16 + me] = message
    pl.semaphore_wait(plane_sem, 1)
    for a, b in far_first + [(0, 0)]:
        targets = [{"tm": sib, **plane_peer(a, b)}] + ([plane_peer(a, b)] if (a, b) != (0, 0) else [])
        for target in targets:
            pltpu.make_async_remote_copy(
                GM.at[pl.ds(0, 5)], GR.at[core * 16 + me, pl.ds(0, 5)], gs, gr,
                device_id=target, device_id_type=MESH,
            ).start()
    phase("b3_wait")
    wait_rows(gr, 31 * 5)
    total = jnp.sum(GR[...], axis=0)
    plane = jnp.sum(GR[pl.ds(core * 16, 16)], axis=0)
    phase("b4_chain")

    high_slabs = [diagonal(total[k : k + 1, :], LANES) for k in range(4)]
    own_sums = diagonal(plane[4:5, :], LANES)
    with_g = [[own_sums[13 * k + i : 13 * k + i + 1, :] for k in range(8)] for i in range(13)]
    first_row = [own_sums[104 + i : 105 + i, :] for i in range(24)]
    k33, k32, k22 = first_row[:6], first_row[6:11], first_row[11:15]

    def entry(i, k, j):
        at = 8 * i + j if k >= 4 else 64 + 8 * i + j
        return high_slabs[k % 4][at : at + 1, :]

    one = jnp.ones((1, LANES), jnp.float32)
    zero = jnp.zeros((1, LANES), jnp.float32)
    coefs = {7: one}
    quad = [entry(i, 7, 7) for i in range(8)]
    cross = [{j: entry(i, 7, j) for j in range(1, 7)} for i in range(8)]
    mixed = [x[7] for x in with_g]
    is_last = jnp.full((1, LANES), tm == 7)
    held_c = {k: zero for k in range(1, 8)}
    held_q = first_row[16:24]
    held_m = [x[0] for x in with_g]
    for t in range(7, 0, -1):
        if t < 7:
            psi_t = quad[0] / (quad[0] + 4.0 * quad[1] + EPS)
            quad = [
                psi_t * psi_t * quad[i] + 2.0 * psi_t * cross[i][t] + entry(i, t, t)
                for i in range(8)
            ]
            cross = [{j: psi_t * cross[i][j] + entry(i, t, j) for j in range(1, t)} for i in range(8)]
            mixed = [psi_t * x + y[t] for x, y in zip(mixed, with_g)]
            coefs = {k: psi_t * x for k, x in coefs.items()}
            coefs[t] = one
        now = jnp.full((1, LANES), tm + 1 == t)
        for k in coefs:
            held_c[k] = jnp.where(now, coefs[k], held_c[k])
        held_q = [jnp.where(now, quad[i], held_q[i]) for i in range(8)]
        held_m = [jnp.where(now, mixed[i], held_m[i]) for i in range(13)]
    psi = held_q[0] / (held_q[0] + 4.0 * held_q[1] + EPS)
    psi = jnp.where(is_last, 0.0, psi)
    for row, count in FULL:
        part = slice(row, row + count)
        value = F[CG, :, part, :] * last
        for k in range(1, 8):
            slab = TH[row // 80, k, :, row - 64 * (row // 80) : row - 64 * (row // 80) + count, :]
            value = value + scaled(held_c[k], jnp.where(tm < k, slab, 0.0))
        V[:, part, :] = value

    def put(level, row, value):
        for t in range(4):
            out[level, row - LOW : row - LOW + value.shape[1], cols(t)] = value[t]

    def next_moments(a, b, m, n, k, count):
        return [
            jnp.maximum(
                a * a * m[i] + 2.0 * a * b * m[i + 1] + b * b * m[i + 2]
                + 2.0 * (a * n[i] + b * n[i + 1]) + k[i],
                0.0,
            )
            for i in range(count)
        ]

    a1, b1 = fine_coefs(held_q)
    m1 = next_moments(a1, b1, held_q, held_m[:7], k33, 6)
    n1 = [a1 * held_m[7 + i] + b1 * held_m[8 + i] + k32[i] for i in range(5)]
    a2, b2 = fine_coefs(m1)
    m2 = next_moments(a2, b2, m1, n1, k22, 4)
    a3, b3 = fine_coefs(m2)
    phase("c0_correct")
    for row, count in FULL:
        part = slice(row, row + count)
        v, u = spread(V, K, row, count)
        value = scaled(a1, v) + scaled(b1, u) + F[G3, :, part, :]
        X[:, part, :] = value
        put(3, max(row, LOW), own_part(value, row, count))
    for row, count in FULL:
        part = slice(row, row + count)
        v, u = spread(X, K, row, count)
        value = scaled(a2, v) + scaled(b2, u) + F[G2, :, part, :]
        W[:, part, :] = value
        put(2, max(row, LOW), own_part(value, row, count))
    for row, count in OWN:
        part = slice(row, row + count)
        v, u = spread(W, K, row, count)
        put(1, row, scaled(a3, v[:4]) + scaled(b3, u[:4]) + F[G1, :4, part, :])
        first = row - 64 * (row // 80)
        put(0, row, scaled(psi, V[:4, part, :]) + TH[row // 80, tm, :4, first : first + count, :])

    phase("c9_end")
    wait_rows(hs, 4 * 8 + 2 * 48 + 4 * 96)
    for r in range(2):
        wait_rows(ar_s.at[r], 15)
    wait_rows(gs, 31 * 5)
    own_sends(lambda h, sem, target: sent(sem))
    for e in range(1, 7):
        @pl.when(slab_at(e)[3])
        def _():
            sent(fs.at[e])

    relays = ((core == 0) & ((chip == 1) | (chip == 2))) | ((core == 1) & ((chip == 0) | (chip == 3)))

    @pl.when(relays)
    def _():
        for odd in range(2):
            sent(rs.at[odd])

    phase(None)


def local(forcing, depth, mask, guess):
    f32 = jnp.float32
    field = (TILES, ROWS, LANES)
    half = (TILES, HALF_ROWS, LANES)
    dma = pltpu.SemaphoreType.DMA
    return pl.pallas_call(
        kernel,
        out_shape=jax.ShapeDtypeStruct(forcing.shape, f32),
        in_specs=[pl.BlockSpec(memory_space=pltpu.HBM)] * 4,
        out_specs=pl.BlockSpec(memory_space=pltpu.VMEM),
        scratch_shapes=[
            pltpu.VMEM((6, *field), f32),
            pltpu.VMEM((4, *field), f32),
            pltpu.VMEM(field, f32),
            pltpu.VMEM(field, f32),
            pltpu.VMEM(field, f32),
            pltpu.VMEM(field, f32),
            pltpu.VMEM((3, *field), f32),
            pltpu.VMEM((9, *field), f32),
            pltpu.VMEM((4, *half), f32),
            pltpu.VMEM((2, 8, *half), f32),
            pltpu.VMEM((8, *half), f32),
            pltpu.VMEM((8, *half), f32),
            pltpu.VMEM((8, *half), f32),
            pltpu.VMEM((8, 4, 64, LANES), f32),
            pltpu.VMEM((4, 128, LANES), f32),
            pltpu.VMEM((4, 128, LANES), jnp.int32),
            pltpu.VMEM((3, 4, 8, LANES), f32),
            pltpu.VMEM((8, 8, 8, LANES), f32),
            pltpu.VMEM((8, 16, LANES), f32),
            pltpu.VMEM((24, LANES), f32),
            pltpu.VMEM((2, 6, 8, LANES), f32),
            pltpu.VMEM((2, 6, 8, LANES), f32),
            pltpu.VMEM((4, 8, LANES), f32),
            pltpu.VMEM((4, 8, LANES), f32),
            pltpu.VMEM((8, 2, 8, LANES), f32),
            pltpu.VMEM((2, 8, LANES), f32),
            pltpu.VMEM((2, 16, LANES), f32),
            pltpu.VMEM((8, LANES), f32),
            pltpu.VMEM((32, 8, LANES), f32),
            pltpu.VMEM((512, LANES), f32),
            dma((3,)),
            dma,
            dma((2,)),
            dma((2,)),
            dma((2,)),
            dma((3, 2)),
            dma((8, 2)),
            dma((7,)),
            dma((2,)),
            dma,
            dma,
            pltpu.SemaphoreType.REGULAR,
        ],
        compiler_params=pltpu.CompilerParams(
            collective_id=0, has_side_effects=True, vmem_limit_bytes=VMEM_LIMIT
        ),
        name="cycle",
    )(*(pltpu.with_memory_space_constraint(x, pltpu.HBM) for x in (forcing, depth, mask, guess)))


def solution(mesh):
    return jax.shard_map(
        local,
        mesh=mesh,
        in_specs=(P("tm", "lat", "lon"), P("lat", "lon"), P("lat", "lon"), P("tm", "lat", "lon")),
        out_specs=P("tm", "lat", "lon"),
        check_vma=False,
    )
```

```python
import functools

import jax
import jax.numpy as jnp
from jax import lax
from jax.experimental import pallas as pl
from jax.experimental.pallas import tpu as pltpu
from jax.sharding import PartitionSpec as P

FS = 4
EPS = 1e-6
VMEM_LIMIT = 40 * 1024 * 1024
MESH = pl.DeviceIdType.MESH

TILES, ROWS, LANES = 5, 160, 128
TOP, LOW, END = 8, 16, 144
FULL = tuple((row, 24) for row in range(8, 152, 24))
OWN = tuple((row, 32) for row in range(16, 144, 32))
HALF_ROWS = 96
HALF = ((8, 24), (32, 24), (56, 32))
HALF_OWN = ((16, 32), (48, 32))
HALF_LOW, HALF_END = 16, 80
DM, CG, G3, G2, G1, G0 = range(6)


def lane_iota(shape):
    return lax.broadcasted_iota(jnp.int32, shape, len(shape) - 1)


def sides(ref, row, count):
    v = ref[:, row : row + count, :]
    down = ref[:, row + 1 : row + 1 + count, :]
    up = ref[:, row - 1 : row - 1 + count, :]
    lane = lane_iota(v.shape)
    ahead = pltpu.roll(v, LANES - 1, 2)
    right = jnp.where(lane == LANES - 1, jnp.concatenate([ahead[1:], ahead[:1]], 0), ahead)
    behind = pltpu.roll(v, 1, 2)
    left = jnp.where(lane == 0, jnp.concatenate([behind[-1:], behind[:-1]], 0), behind)
    return v, right, left, down, up


def spread(ref, coef, row, count):
    v, right, left, down, up = sides(ref, row, count)
    part = slice(row, row + count)
    out = coef[0, :, part, :] * (v - right) + coef[1, :, part, :] * (v - left)
    out = out + coef[2, :, part, :] * (v - down) + coef[3, :, part, :] * (v - up)
    return v, out


def own_part(x, row, count):
    first, last = max(row, LOW) - row, min(row + count, END) - row
    return x[:4, first:last, :]


def fold(x):
    return jnp.sum(x.reshape(-1, 8, LANES), axis=0)


class Phase:
    def __init__(self):
        self.open = None

    def __call__(self, name):
        if self.open is not None:
            self.open.__exit__(None, None, None)
        self.open = jax.named_scope(name) if name else None
        if self.open is not None:
            self.open.__enter__()


class Sums:
    def __init__(self):
        self.terms = {}

    def add(self, key, a, b):
        value = fold(a * b)
        self.terms[key] = value if key not in self.terms else self.terms[key] + value


def fine_coefs(m):
    den = m[0] + m[1] + EPS
    alpha = m[0] / den
    gamma = (m[1] + EPS) / den
    s1 = jnp.maximum(
        gamma * gamma * m[0] - 2.0 * gamma * alpha * m[1] + alpha * alpha * m[2], 0.0
    )
    beta = s1 / (m[0] + EPS)
    f = gamma + beta
    pp = s1 + beta * (2.0 * EPS * alpha + beta * m[0])
    plp = jnp.maximum(f * f * m[1] - 2.0 * f * alpha * m[2] + alpha * alpha * m[3], 0.0)
    later = jnp.minimum(s1 / (pp + plp + EPS), 1.0)
    return alpha + later * f, -alpha * later


def kernel(
    forcing, depth, mask, guess, out,
    F, K, V, X, U, W, LG, GP, KH, TH, UG, TG2, TG3, TG4, DEP, MSK, KAP, ROW, CR, KQ,
    PKS, PKR, CKS, CKR, PT, MSG, AR,
    GM, GR, BOX, in_sem, hs, hr, ar_s, ar_r, ts, tr, fs, rs, gs, gr, plane_sem,
):
    phase = Phase()
    phase("a0_load")
    tm = lax.axis_index("tm")
    lat = lax.axis_index("lat")
    lon = lax.axis_index("lon")
    me = lat * 4 + lon
    chip, core = tm // 2, tm % 2
    sib = 2 * chip + 1 - core

    def cols(c):
        return pl.ds(LANES * c, LANES)

    barrier = pltpu.get_barrier_semaphore()
    north, south = lax.rem(lat + 3, 4), lax.rem(lat + 1, 4)
    west, east = lax.rem(lon + 3, 4), lax.rem(lon + 1, 4)

    def greet(target):
        pl.semaphore_signal(barrier, inc=1, device_id=target, device_id_type=MESH)

    for a in (north, south):
        for b in (west, east):
            greet({"lat": a, "lon": b})
    for step in (4, 3, 5, 2, 6, 1, 7):
        greet({"tm": lax.rem(tm + step, 8)})
    for a in (north, south):
        greet({"lat": a})
    for b in (west, east):
        greet({"lon": b})

    own_rows = pl.ds(LOW, END - LOW)

    for c in range(4):
        pltpu.make_async_copy(depth.at[:, cols(c)], DEP.at[c], in_sem.at[0]).start()
        pltpu.make_async_copy(mask.at[:, cols(c)], MSK.at[c], in_sem.at[1]).start()
        pltpu.make_async_copy(
            guess.at[0, :, cols(c)], F.at[CG, c, own_rows, :], in_sem.at[2]
        ).start()
    for field, level, i in ((G3, 3, 2), (G2, 2, 3), (G1, 1, 3), (G0, 0, 3)):
        for c in range(4):
            pltpu.make_async_copy(
                forcing.at[level, :, cols(c)], F.at[field, c, own_rows, :], in_sem.at[i]
            ).start()

    phase("a1_clear")
    def clear(ref):
        zero = jnp.zeros((TILES, 8, LANES), jnp.float32)
        ref[:, 0:8, :] = zero
        ref[:, 152:160, :] = zero

    def clear_fields(i, _):
        clear(F.at[i])
        return 0

    lax.fori_loop(0, 6, clear_fields, 0)
    for ref in (V, X, U):
        clear(ref)

    def clear_slab(i, _):
        ROW[:, i] = jnp.zeros((8, 8, LANES), jnp.float32)
        CR[i] = jnp.zeros((16, LANES), jnp.float32)
        return 0

    lax.fori_loop(0, 8, clear_slab, 0)
    KQ[...] = jnp.zeros((24, LANES), jnp.float32)
    for i in range(9):
        clear(GP.at[i])
    for i in range(3):
        clear(LG.at[i])

    phase("a2_loadwait")
    fields = F.at[pl.ds(1, 2), pl.ds(0, 4), own_rows, :]
    for i, ref in enumerate((DEP, MSK, fields)):
        pltpu.make_async_copy(ref, ref, in_sem.at[i]).wait()
    for c in range(4):
        F[DM, c, LOW:END, :] = jnp.where(MSK[c] > 0, DEP[c], 0.0)

    phase("a3_pack")
    lane3f = lane_iota((3, 8, LANES))
    lane1 = lane_iota((8, LANES))
    corners = ((136, 3, 8), (136, 0, 0), (16, 3, 8), (16, 0, 0))

    def pack(group):
        three = slice(3 * group, 3 * group + 3)
        right_edge = jnp.zeros((3, 8, LANES), jnp.float32)
        left_edge = jnp.zeros((3, 8, LANES), jnp.float32)
        for t in range(16):
            here = (lane3f >= 8 * t) & (lane3f < 8 * t + 8)
            rows = slice(LOW + 8 * t, LOW + 8 * t + 8)
            right = pltpu.roll(F[three, 3, rows, :], (8 * t + 8) % LANES, 2)
            right_edge = jnp.where(here, right, right_edge)
            left_edge = jnp.where(here, pltpu.roll(F[three, 0, rows, :], 8 * t, 2), left_edge)
        PKS[group, 0] = right_edge
        PKS[group, 1] = left_edge
        for i, (row, tile, shift) in enumerate(corners):
            packed = jnp.zeros((8, LANES), jnp.float32)
            for f in range(3):
                here = (lane1 >= 8 * f) & (lane1 < 8 * f + 8)
                edge = F[3 * group + f, tile, row : row + 8, :]
                packed = jnp.where(here, pltpu.roll(edge, (8 * f + shift) % LANES, 1), packed)
            CKS[group, i] = packed

    def unpack_halo(group):
        three = slice(3 * group, 3 * group + 3)
        from_left, from_right = PKR[group, 0], PKR[group, 1]
        for t in range(16):
            rows = slice(LOW + 8 * t, LOW + 8 * t + 8)
            a = pltpu.roll(from_left, (120 - 8 * t) % LANES, 2)
            b = pltpu.roll(from_right, (LANES - 8 * t) % LANES, 2)
            F[three, 4, rows, :] = jnp.where(lane3f >= 120, a, jnp.where(lane3f < 8, b, 0.0))
        for row, left, right in ((8, 0, 1), (144, 2, 3)):
            a0, b0 = CKR[group, left], CKR[group, right]
            for f in range(3):
                a = pltpu.roll(a0, (120 - 8 * f) % LANES, 1)
                b = pltpu.roll(b0, (LANES - 8 * f) % LANES, 1)
                edge = jnp.where(lane1 >= 120, a, jnp.where(lane1 < 8, b, 0.0))
                F[3 * group + f, 4, row : row + 8, :] = edge

    pack(0)

    phase("a4_barrier")
    pl.semaphore_wait(barrier, 15)


    def push(src, dst, i, target):
        pltpu.make_async_remote_copy(
            src, dst, hs, hr.at[i], device_id=target, device_id_type=MESH
        ).start()

    def wait_rows(sem, count):
        box = BOX.at[pl.ds(0, count)]
        pltpu.make_async_copy(box, box, sem).wait()

    targets = ((south, east), (south, west), (north, east), (north, west))

    def push_halo(group):
        for i, (a, b) in enumerate(targets):
            push(CKS.at[group, i], CKR.at[group, i], group, {"lat": a, "lon": b})
        fields = pl.ds(3 * group, 3)
        push(
            F.at[fields, pl.ds(0, 4), pl.ds(136, 8), :],
            F.at[fields, pl.ds(0, 4), pl.ds(8, 8), :],
            group, {"lat": south},
        )
        push(
            F.at[fields, pl.ds(0, 4), pl.ds(16, 8), :],
            F.at[fields, pl.ds(0, 4), pl.ds(144, 8), :],
            group, {"lat": north},
        )
        push(PKS.at[group, 0], PKR.at[group, 0], group, {"lon": east})
        push(PKS.at[group, 1], PKR.at[group, 1], group, {"lon": west})

    halo_rows = 4 * 8 + 2 * 96 + 2 * 24
    push_halo(0)
    fields = F.at[pl.ds(3, 3), pl.ds(0, 4), own_rows, :]
    pltpu.make_async_copy(fields, fields, in_sem.at[3]).wait()
    pack(1)
    push_halo(1)
    phase("a5_halowait")
    wait_rows(hr.at[0], halo_rows)

    pl.semaphore_signal(plane_sem, inc=1, device_id={"tm": sib}, device_id_type=MESH)
    phase("a6_unpack")
    unpack_halo(0)

    inside_top = jnp.where(lat > 0, 1.0, 0.0).astype(jnp.float32)
    inside_end = jnp.where(lat < 3, 1.0, 0.0).astype(jnp.float32)
    F[DM, :, 8:16, :] = F[DM, :, 8:16, :] * inside_top
    F[DM, :, 144:152, :] = F[DM, :, 144:152, :] * inside_end

    for row, count in FULL:
        d, *around = sides(F.at[DM], row, count)
        for i, other in enumerate(around):
            K[i, :, row : row + count, :] = jnp.where(
                (d > 0.0) & (other > 0.0), 1.5 * (d + other), 0.0
            )

    far_first = sorted(
        ((a, b) for a in range(4) for b in range(4) if (a, b) != (0, 0)),
        key=lambda ab: -(min(ab[0], 4 - ab[0]) + min(ab[1], 4 - ab[1])),
    )

    def plane_peer(a, b):
        return {"lat": lax.rem(lat + a, 4), "lon": lax.rem(lon + b, 4)}

    def diagonal(x, count):
        shape = (count, LANES)
        here = lane_iota(shape) == lax.broadcasted_iota(jnp.int32, shape, 0)
        picked = jnp.where(here, jnp.broadcast_to(x, shape), 0.0)
        return jnp.broadcast_to(jnp.sum(picked, axis=1, keepdims=True), shape)

    def send_sums(r, accs):
        row = lax.broadcasted_iota(jnp.int32, (16, LANES), 0)
        stacked = jnp.zeros((16, LANES), jnp.float32)
        for i, acc in enumerate(accs):
            stacked = jnp.where(row == i, jnp.sum(acc, axis=0, keepdims=True), stacked)
        stacked = jnp.broadcast_to(jnp.sum(stacked, axis=1, keepdims=True), (16, LANES))
        message = jnp.where(lane_iota((16, LANES)) == row, stacked, 0.0)
        message = jnp.sum(message, axis=0, keepdims=True)
        MSG[r, 0:1, :] = message
        AR[r, pl.ds(me, 1), :] = message
        for a, b in far_first:
            pltpu.make_async_remote_copy(
                MSG.at[r, pl.ds(0, 1)], AR.at[r, pl.ds(me, 1)], ar_s.at[r], ar_r.at[r],
                device_id=plane_peer(a, b), device_id_type=MESH,
            ).start()

    def recv_sums(r):
        wait_rows(ar_r.at[r], 15)
        return diagonal(jnp.sum(AR[r], axis=0, keepdims=True), 16)

    def prepare(field, slot):
        sums = Sums()
        for row, count in FULL:
            g, lg = spread(F.at[field], K, row, count)
            LG[slot, :, row : row + count, :] = lg
            g, lg = own_part(g, row, count), own_part(lg, row, count)
            sums.add(0, g, g)
            sums.add(1, g, lg)
            sums.add(2, lg, lg)
        for row, count in OWN:
            lg, llg = spread(LG.at[slot], K, row, count)
            sums.add(3, lg[:4], llg[:4])
        for i in range(4):
            KAP[slot, i] = sums.terms[i]

    def power(src, dst):
        for row, count in FULL:
            dst[:, row : row + count, :] = spread(src, K, row, count)[1]

    def line(acc):
        return jnp.sum(acc, axis=0, keepdims=True)

    def own_sum(a, b):
        return line(fold(a[:4, LOW:END, :] * b[:4, LOW:END, :]))

    g3_powers = [F.at[G3], LG.at[0]] + [GP.at[i] for i in range(5)]
    g2_powers = [F.at[G2], LG.at[2]] + [GP.at[i] for i in range(5, 9)]

    def powers_of_g3():
        for src, dst in zip(g3_powers[1:], g3_powers[2:]):
            power(src, dst)

    def powers_of_g2():
        prepare(G2, 2)
        for src, dst in zip(g2_powers[1:], g2_powers[2:]):
            power(src, dst)
        for i in range(4):
            KQ[i : i + 1, :] = line(KAP[0, i])
            KQ[11 + i : 12 + i, :] = line(KAP[2, i])
        KQ[4:5, :] = own_sum(g3_powers[2], g3_powers[2])
        KQ[5:6, :] = own_sum(g3_powers[2], g3_powers[3])
        for i in range(5):
            KQ[6 + i : 7 + i, :] = own_sum(g2_powers[0], g3_powers[i])

    def two_steps(r, v_ref, field, slot, between):
        phase(f"r{r}_moments")
        sums = Sums()
        for row, count in FULL:
            v, u = spread(v_ref, K, row, count)
            U[:, row : row + count, :] = u
            g = own_part(F[field, :, row : row + count, :], row, count)
            v, u = own_part(v, row, count), own_part(u, row, count)
            sums.add("m0", v, v)
            sums.add("m1", v, u)
            sums.add("m2", u, u)
            sums.add("n0", v, g)
            sums.add("n1", u, g)
        for row, count in FULL:
            u, w = spread(U, K, row, count)
            W[:, row : row + count, :] = w
            lg = own_part(LG[slot, :, row : row + count, :], row, count)
            u, w = own_part(u, row, count), own_part(w, row, count)
            sums.add("m3", u, w)
            sums.add("m4", w, w)
            sums.add("n2", u, lg)
            sums.add("n3", w, lg)
        for row, count in OWN:
            w, lw = spread(W, K, row, count)
            lg = LG[slot, :4, row : row + count, :]
            sums.add("m5", w[:4], lw[:4])
            sums.add("n4", lw[:4], lg)
        names = ["m0", "m1", "m2", "m3", "m4", "m5", "n0", "n1", "n2", "n3", "n4"]
        accs = [sums.terms[n] for n in names] + [KAP[slot, i] for i in range(4)]
        send_sums(r, accs)
        phase(f"r{r}_between")
        between()
        phase(f"r{r}_wait")
        total = recv_sums(r)
        phase(f"r{r}_scalars")
        at = [total[i : i + 1, :] for i in range(15)]
        m, n, k = at[:6], at[6:11], at[11:]
        a, b = fine_coefs(m)
        later = [
            jnp.maximum(
                a * a * m[i] + 2.0 * a * b * m[i + 1] + b * b * m[i + 2]
                + 2.0 * (a * n[i] + b * n[i + 1]) + k[i],
                0.0,
            )
            for i in range(4)
        ]
        a2, b2 = fine_coefs(later)
        return m, (a, b), (a2 * a, a2 * b + b2 * a, b2 * b, a2, b2)

    def scaled(s, x):
        return jnp.broadcast_to(s.reshape(1, 1, LANES), x.shape) * x

    phase("a7_prepare")
    prepare(G3, 0)

    def rest_of_halo():
        wait_rows(hr.at[1], halo_rows)
        unpack_halo(1)
        prepare(G1, 1)
        powers_of_g3()
        rows = pl.ds(pl.multiple_of(8 + 64 * core, 8), 80)
        for i in range(4):
            KH[i, :, 8:88, :] = K[i, :, rows, :]

    m_start, _, c = two_steps(0, F.at[CG], G3, 0, rest_of_halo)
    for row, count in FULL:
        part = slice(row, row + count)
        X[:, part, :] = (
            scaled(c[0], F[CG, :, part, :]) + scaled(c[1], U[:, part, :]) + scaled(c[2], W[:, part, :])
            + scaled(c[3], F[G3, :, part, :]) + scaled(c[4], LG[0, :, part, :]) + F[G2, :, part, :]
        )
    last = jnp.where(tm == 7, 1.0, 0.0).astype(jnp.float32)
    psi = m_start[0] / (m_start[0] + 4.0 * m_start[1] + EPS)
    drop = psi * (last - 1.0)

    _, _, c = two_steps(1, X, G1, 1, powers_of_g2)
    for h in range(2):
        for row, count in HALF:
            part = slice(64 * h + row, 64 * h + row + count)
            TH[h, tm, :, row : row + count, :] = (
                scaled(c[0], X[:, part, :]) + scaled(c[1], U[:, part, :])
                + scaled(c[2], W[:, part, :]) + scaled(c[3], F[G1, :, part, :])
                + scaled(c[4], LG[1, :, part, :]) + F[G0, :, part, :]
                + scaled(drop, F[CG, :, part, :])
            )

    phase("b0_gather")
    lane2 = lane_iota((8, LANES))
    for h in range(2):
        packed = jnp.zeros((8, LANES), jnp.float32)
        for t in range(10):
            row = 8 + 8 * t
            here = (lane2 >= 8 * t) & (lane2 < 8 * t + 8)
            edge = pltpu.roll(TH[h, tm, 4, row : row + 8, :], 8 * t + 4, 1)
            packed = jnp.where(here, edge, packed)
        PT[tm, h] = packed

    def half_copies(k, h, sem, target):
        main = TH.at[h, k, pl.ds(0, 4), pl.ds(12, 72), :]
        return [
            pltpu.make_async_remote_copy(
                ref, ref, sem, tr.at[k, h], device_id={"tm": target}, device_id_type=MESH
            )
            for ref in (main, PT.at[k, h])
        ]

    def start(copies):
        for copy in copies:
            copy.start()

    def sent(sem):
        wait_rows(sem, 4 * 72 + 8)

    def landed(k, h):
        wait_rows(tr.at[k, h], 4 * 72 + 8)

    def own_sends(act):
        for h in range(2):
            @pl.when(core == 1)
            def _():
                act(h, ts.at[0, h], sib)

            @pl.when(chip == 3)
            def _():
                act(h, ts.at[1, h], h)

            @pl.when(chip >= 1)
            def _():
                act(h, ts.at[2, h], jnp.maximum(2 * chip - 2 + h, 0))

            if h == 1:
                @pl.when(chip == 2)
                def _():
                    act(h, ts.at[1, h], 7)

    own_sends(lambda h, sem, target: start(half_copies(tm, h, sem, target)))

    def slab_at(e):
        dx = jnp.where((e == 1) | (e == 3), 1, jnp.where((e == 2) | (e == 5), 3, 2))
        odd = jnp.where((e == 1) | (e == 2) | (e == 4), 1, 0)
        k = jnp.where(e == 0, 2 * chip + 1, 2 * (chip + dx) + odd)
        valid = (e == 0) | (chip + dx <= 3)
        return jnp.minimum(k, 7), dx, odd, valid

    def unpack(k, h):
        packed = PT[k, h]
        for t in range(10):
            back = pltpu.roll(packed, (LANES - 8 * t - 4) % LANES, 1)
            back = jnp.where((lane2 < 4) | (lane2 >= 124), back, 0.0)
            TH[h, k, 4, 8 + 8 * t : 16 + 8 * t, :] = back

    def cross_sums(k, h):
        sums = Sums()
        rows = pl.ds(pl.multiple_of(HALF_LOW + 64 * h, 8), HALF_END - HALF_LOW)
        for t in range(4):
            value = TH[h, k, t, HALF_LOW:HALF_END, :]
            for i, ref in enumerate(g3_powers + g2_powers):
                sums.add(i, value, ref[t, rows, :])
        for i in range(13):
            CR[k, i : i + 1, :] = CR[k, i : i + 1, :] + line(sums.terms[i])

    def gram_sums(e, k):
        refs = [TH.at[core, k], UG.at[k], TG2.at[k], TG3.at[k]]
        for src, dst in zip(refs, refs[1:]):
            for row, count in HALF:
                dst[:, row : row + count, :] = spread(src, KH, row, count)[1]
        for row, count in HALF_OWN:
            last_power = spread(refs[3], KH, row, count)[1]
            TG4[k, :, row - HALF_LOW : row - HALF_LOW + count, :] = last_power[:4]
        cross_sums(k, core)

        def pair(q, _):
            j, _, _, held = slab_at(q)

            @pl.when(held)
            def _():
                sums = Sums()
                low, high = jnp.minimum(j, k), jnp.maximum(j, k)
                for t in range(4):
                    a, b = (
                        [TH[core, s, t, HALF_LOW:HALF_END, :]]
                        + [ref[s, t, HALF_LOW:HALF_END, :] for ref in (UG, TG2, TG3)]
                        for s in (low, high)
                    )
                    b.append(TG4[high, t])
                    for i in range(8):
                        sums.add(i, a[i // 2], b[(i + 1) // 2])
                for i in range(8):
                    value = line(sums.terms[i])
                    ROW[i, k, pl.ds(j, 1), :] = value
                    ROW[i, j, pl.ds(k, 1), :] = value

            return 0

        lax.fori_loop(0, e + 1, pair, 0)

    def first_hand(e):
        k, dx, odd, valid = slab_at(e)

        @pl.when(valid)
        def _():
            @pl.when((e > 0) | (core == 0))
            def _():
                with jax.named_scope("b1_slabwait"):
                    landed(k, core)

            @pl.when((dx == 1) & (core == 0) & ((chip == 1) | (chip == 2)) & (e > 0))
            def _():
                start(half_copies(k, 0, rs.at[odd], jnp.maximum(tm - 2, 0)))

            @pl.when((dx == 3) & (core == 1) & (chip == 0) & (e > 0))
            def _():
                start(half_copies(k, 1, rs.at[odd], 3))

            @pl.when(e > 0)
            def _():
                start(half_copies(k, core, fs.at[e], sib))

            unpack(k, core)
            gram_sums(e, k)

    def second_hand(e):
        k, _, _, valid = slab_at(e)

        @pl.when(valid & (k > tm))
        def _():
            with jax.named_scope("b1_sibwait"):
                landed(k, 1 - core)
            unpack(k, 1 - core)
            cross_sums(k, 1 - core)

    def arrive(i, _):
        @pl.when(i < 7)
        def _():
            first_hand(jnp.minimum(i, 6))

        @pl.when(i >= 2)
        def _():
            second_hand(jnp.maximum(i - 2, 0))

        return 0

    @pl.when(tm == 7)
    def _():
        refs = [F.at[CG], U, W, V, X]
        for src, dst in zip(refs, refs[1:]):
            power(src, dst)
        for i in range(8):
            KQ[16 + i : 17 + i, :] = own_sum(refs[i // 2], refs[(i + 1) // 2])
        for i, ref in enumerate(g3_powers + g2_powers):
            CR[0, i : i + 1, :] = own_sum(refs[0], ref)

    @pl.when(tm == 7)
    def _():
        for odd in (1, 0):
            landed(4 + odd, 1)
            start(half_copies(4 + odd, 1, rs.at[odd], 1))

    phase("b1_arrive")
    lax.fori_loop(0, 9, arrive, 0)

    phase("b2_gram")
    lane3 = lane_iota((8, 8, LANES))
    sub3 = lax.broadcasted_iota(jnp.int32, (8, 8, LANES), 1)
    gram = jnp.zeros((8, 8, LANES), jnp.float32)
    for i in range(8):
        gram = jnp.where(lane3 == 8 * i + sub3, jnp.sum(ROW[i], axis=2, keepdims=True), gram)
    gram = jnp.sum(gram, axis=1)
    lane4 = lane_iota((8, 16, LANES))
    sub4 = lax.broadcasted_iota(jnp.int32, (8, 16, LANES), 1)
    slab4 = lax.broadcasted_iota(jnp.int32, (8, 16, LANES), 0)
    cross = jnp.where(
        (lane4 == 13 * slab4 + sub4) & (sub4 < 13), jnp.sum(CR[...], axis=2, keepdims=True), 0.0
    )
    cross = jnp.sum(jnp.sum(cross, axis=0), axis=0, keepdims=True)
    lane5 = lane_iota((24, LANES))
    sub5 = lax.broadcasted_iota(jnp.int32, (24, LANES), 0)
    own = jnp.where(lane5 == 104 + sub5, jnp.sum(KQ[...], axis=1, keepdims=True), 0.0)
    own = cross + jnp.sum(own, axis=0, keepdims=True)
    sub2 = lax.broadcasted_iota(jnp.int32, (8, LANES), 0)
    folded = jnp.where(lane2 < 64, pltpu.roll(gram, 4, 0), pltpu.roll(gram, 64, 1))
    message = jnp.where(sub2 < 4, folded, jnp.where(sub2 == 4, own, 0.0))
    GM[...] = message
    GR[core * 16 + me] = message
    pl.semaphore_wait(plane_sem, 1)
    for a, b in far_first + [(0, 0)]:
        targets = [{"tm": sib, **plane_peer(a, b)}] + ([plane_peer(a, b)] if (a, b) != (0, 0) else [])
        for target in targets:
            pltpu.make_async_remote_copy(
                GM.at[pl.ds(0, 5)], GR.at[core * 16 + me, pl.ds(0, 5)], gs, gr,
                device_id=target, device_id_type=MESH,
            ).start()
    phase("b3_wait")
    wait_rows(gr, 31 * 5)
    total = jnp.sum(GR[...], axis=0)
    plane = jnp.sum(GR[pl.ds(core * 16, 16)], axis=0)
    phase("b4_chain")

    high_slabs = [diagonal(total[k : k + 1, :], LANES) for k in range(4)]
    own_sums = diagonal(plane[4:5, :], LANES)
    with_g = [[own_sums[13 * k + i : 13 * k + i + 1, :] for k in range(8)] for i in range(13)]
    first_row = [own_sums[104 + i : 105 + i, :] for i in range(24)]
    k33, k32, k22 = first_row[:6], first_row[6:11], first_row[11:15]

    def entry(i, k, j):
        at = 8 * i + j if k >= 4 else 64 + 8 * i + j
        return high_slabs[k % 4][at : at + 1, :]

    one = jnp.ones((1, LANES), jnp.float32)
    zero = jnp.zeros((1, LANES), jnp.float32)
    coefs = {7: one}
    quad = [entry(i, 7, 7) for i in range(8)]
    cross = [{j: entry(i, 7, j) for j in range(1, 7)} for i in range(8)]
    mixed = [x[7] for x in with_g]
    is_last = jnp.full((1, LANES), tm == 7)
    held_c = {k: zero for k in range(1, 8)}
    held_q = first_row[16:24]
    held_m = [x[0] for x in with_g]
    for t in range(7, 0, -1):
        if t < 7:
            psi_t = quad[0] / (quad[0] + 4.0 * quad[1] + EPS)
            quad = [
                psi_t * psi_t * quad[i] + 2.0 * psi_t * cross[i][t] + entry(i, t, t)
                for i in range(8)
            ]
            cross = [{j: psi_t * cross[i][j] + entry(i, t, j) for j in range(1, t)} for i in range(8)]
            mixed = [psi_t * x + y[t] for x, y in zip(mixed, with_g)]
            coefs = {k: psi_t * x for k, x in coefs.items()}
            coefs[t] = one
        now = jnp.full((1, LANES), tm + 1 == t)
        for k in coefs:
            held_c[k] = jnp.where(now, coefs[k], held_c[k])
        held_q = [jnp.where(now, quad[i], held_q[i]) for i in range(8)]
        held_m = [jnp.where(now, mixed[i], held_m[i]) for i in range(13)]
    psi = held_q[0] / (held_q[0] + 4.0 * held_q[1] + EPS)
    psi = jnp.where(is_last, 0.0, psi)
    for row, count in FULL:
        part = slice(row, row + count)
        value = F[CG, :, part, :] * last
        for k in range(1, 8):
            slab = TH[row // 80, k, :, row - 64 * (row // 80) : row - 64 * (row // 80) + count, :]
            value = value + scaled(held_c[k], jnp.where(tm < k, slab, 0.0))
        V[:, part, :] = value

    def put(level, row, value):
        for t in range(4):
            out[level, row - LOW : row - LOW + value.shape[1], cols(t)] = value[t]

    def next_moments(a, b, m, n, k, count):
        return [
            jnp.maximum(
                a * a * m[i] + 2.0 * a * b * m[i + 1] + b * b * m[i + 2]
                + 2.0 * (a * n[i] + b * n[i + 1]) + k[i],
                0.0,
            )
            for i in range(count)
        ]

    a1, b1 = fine_coefs(held_q)
    m1 = next_moments(a1, b1, held_q, held_m[:7], k33, 6)
    n1 = [a1 * held_m[7 + i] + b1 * held_m[8 + i] + k32[i] for i in range(5)]
    a2, b2 = fine_coefs(m1)
    m2 = next_moments(a2, b2, m1, n1, k22, 4)
    a3, b3 = fine_coefs(m2)
    phase("c0_correct")
    for row, count in FULL:
        part = slice(row, row + count)
        v, u = spread(V, K, row, count)
        value = scaled(a1, v) + scaled(b1, u) + F[G3, :, part, :]
        X[:, part, :] = value
        put(3, max(row, LOW), own_part(value, row, count))
    for row, count in FULL:
        part = slice(row, row + count)
        v, u = spread(X, K, row, count)
        value = scaled(a2, v) + scaled(b2, u) + F[G2, :, part, :]
        W[:, part, :] = value
        put(2, max(row, LOW), own_part(value, row, count))
    for row, count in OWN:
        part = slice(row, row + count)
        v, u = spread(W, K, row, count)
        put(1, row, scaled(a3, v[:4]) + scaled(b3, u[:4]) + F[G1, :4, part, :])
        first = row - 64 * (row // 80)
        put(0, row, scaled(psi, V[:4, part, :]) + TH[row // 80, tm, :4, first : first + count, :])

    phase("c9_end")
    wait_rows(hs, 2 * halo_rows)
    for r in range(2):
        wait_rows(ar_s.at[r], 15)
    wait_rows(gs, 31 * 5)
    own_sends(lambda h, sem, target: sent(sem))
    for e in range(1, 7):
        @pl.when(slab_at(e)[3])
        def _():
            sent(fs.at[e])

    relays = ((core == 0) & ((chip == 1) | (chip == 2))) | ((core == 1) & ((chip == 0) | (chip == 3)))

    @pl.when(relays)
    def _():
        for odd in range(2):
            sent(rs.at[odd])

    phase(None)


def local(forcing, depth, mask, guess):
    f32 = jnp.float32
    field = (TILES, ROWS, LANES)
    half = (TILES, HALF_ROWS, LANES)
    dma = pltpu.SemaphoreType.DMA
    return pl.pallas_call(
        kernel,
        out_shape=jax.ShapeDtypeStruct(forcing.shape, f32),
        in_specs=[pl.BlockSpec(memory_space=pltpu.HBM)] * 4,
        out_specs=pl.BlockSpec(memory_space=pltpu.VMEM),
        scratch_shapes=[
            pltpu.VMEM((6, *field), f32),
            pltpu.VMEM((4, *field), f32),
            pltpu.VMEM(field, f32),
            pltpu.VMEM(field, f32),
            pltpu.VMEM(field, f32),
            pltpu.VMEM(field, f32),
            pltpu.VMEM((3, *field), f32),
            pltpu.VMEM((9, *field), f32),
            pltpu.VMEM((4, *half), f32),
            pltpu.VMEM((2, 8, *half), f32),
            pltpu.VMEM((8, *half), f32),
            pltpu.VMEM((8, *half), f32),
            pltpu.VMEM((8, *half), f32),
            pltpu.VMEM((8, 4, 64, LANES), f32),
            pltpu.VMEM((4, 128, LANES), f32),
            pltpu.VMEM((4, 128, LANES), jnp.int32),
            pltpu.VMEM((3, 4, 8, LANES), f32),
            pltpu.VMEM((8, 8, 8, LANES), f32),
            pltpu.VMEM((8, 16, LANES), f32),
            pltpu.VMEM((24, LANES), f32),
            pltpu.VMEM((2, 2, 3, 8, LANES), f32),
            pltpu.VMEM((2, 2, 3, 8, LANES), f32),
            pltpu.VMEM((2, 4, 8, LANES), f32),
            pltpu.VMEM((2, 4, 8, LANES), f32),
            pltpu.VMEM((8, 2, 8, LANES), f32),
            pltpu.VMEM((2, 8, LANES), f32),
            pltpu.VMEM((2, 16, LANES), f32),
            pltpu.VMEM((8, LANES), f32),
            pltpu.VMEM((32, 8, LANES), f32),
            pltpu.VMEM((544, LANES), f32),
            dma((4,)),
            dma,
            dma((2,)),
            dma((2,)),
            dma((2,)),
            dma((3, 2)),
            dma((8, 2)),
            dma((7,)),
            dma((2,)),
            dma,
            dma,
            pltpu.SemaphoreType.REGULAR,
        ],
        compiler_params=pltpu.CompilerParams(
            collective_id=0, has_side_effects=True, vmem_limit_bytes=VMEM_LIMIT
        ),
        name="cycle",
    )(*(pltpu.with_memory_space_constraint(x, pltpu.HBM) for x in (forcing, depth, mask, guess)))


def solution(mesh):
    return jax.shard_map(
        local,
        mesh=mesh,
        in_specs=(P("tm", "lat", "lon"), P("lat", "lon"), P("lat", "lon"), P("tm", "lat", "lon")),
        out_specs=P("tm", "lat", "lon"),
        check_vma=False,
    )
```

```python
import functools

import jax
import jax.numpy as jnp
from jax import lax
from jax.experimental import pallas as pl
from jax.experimental.pallas import tpu as pltpu
from jax.sharding import PartitionSpec as P

FS = 4
EPS = 1e-6
VMEM_LIMIT = 40 * 1024 * 1024
MESH = pl.DeviceIdType.MESH

TILES, ROWS, LANES = 5, 160, 128
TOP, LOW, END = 8, 16, 144
FULL = tuple((row, 24) for row in range(8, 152, 24))
OWN = tuple((row, 32) for row in range(16, 144, 32))
HALF_ROWS = 96
HALF = ((8, 24), (32, 24), (56, 32))
HALF_OWN = ((16, 32), (48, 32))
HALF_LOW, HALF_END = 16, 80
DM, CG, G3, G2, G1, G0 = range(6)


def lane_iota(shape):
    return lax.broadcasted_iota(jnp.int32, shape, len(shape) - 1)


def sides(ref, row, count):
    v = ref[:, row : row + count, :]
    down = ref[:, row + 1 : row + 1 + count, :]
    up = ref[:, row - 1 : row - 1 + count, :]
    lane = lane_iota(v.shape)
    ahead = pltpu.roll(v, LANES - 1, 2)
    right = jnp.where(lane == LANES - 1, jnp.concatenate([ahead[1:], ahead[:1]], 0), ahead)
    behind = pltpu.roll(v, 1, 2)
    left = jnp.where(lane == 0, jnp.concatenate([behind[-1:], behind[:-1]], 0), behind)
    return v, right, left, down, up


def spread(ref, coef, row, count):
    v, right, left, down, up = sides(ref, row, count)
    part = slice(row, row + count)
    out = coef[0, :, part, :] * (v - right) + coef[1, :, part, :] * (v - left)
    out = out + coef[2, :, part, :] * (v - down) + coef[3, :, part, :] * (v - up)
    return v, out


def own_part(x, row, count):
    first, last = max(row, LOW) - row, min(row + count, END) - row
    return x[:4, first:last, :]


def fold(x):
    return jnp.sum(x.reshape(-1, 8, LANES), axis=0)


class Phase:
    def __init__(self):
        self.open = None

    def __call__(self, name):
        if self.open is not None:
            self.open.__exit__(None, None, None)
        self.open = jax.named_scope(name) if name else None
        if self.open is not None:
            self.open.__enter__()


class Sums:
    def __init__(self):
        self.terms = {}

    def add(self, key, a, b):
        value = fold(a * b)
        self.terms[key] = value if key not in self.terms else self.terms[key] + value


def fine_coefs(m):
    den = m[0] + m[1] + EPS
    alpha = m[0] / den
    gamma = (m[1] + EPS) / den
    s1 = jnp.maximum(
        gamma * gamma * m[0] - 2.0 * gamma * alpha * m[1] + alpha * alpha * m[2], 0.0
    )
    beta = s1 / (m[0] + EPS)
    f = gamma + beta
    pp = s1 + beta * (2.0 * EPS * alpha + beta * m[0])
    plp = jnp.maximum(f * f * m[1] - 2.0 * f * alpha * m[2] + alpha * alpha * m[3], 0.0)
    later = jnp.minimum(s1 / (pp + plp + EPS), 1.0)
    return alpha + later * f, -alpha * later


def kernel(
    forcing, depth, mask, guess, out,
    F, K, V, X, U, W, LG, GP, KH, TH, UG, TG2, TG3, TG4, DEP, MSK, KAP, ROW, CR, KQ,
    PKS, PKR, CKS, CKR, PT, MSG, AR,
    GM, GR, BOX, in_sem, hs, hr, ar_s, ar_r, ts, tr, fs, rs, gs, gr, plane_sem,
):
    phase = Phase()
    phase("a0_load")
    tm = lax.axis_index("tm")
    lat = lax.axis_index("lat")
    lon = lax.axis_index("lon")
    me = lat * 4 + lon
    chip, core = tm // 2, tm % 2
    sib = 2 * chip + 1 - core

    def cols(c):
        return pl.ds(LANES * c, LANES)

    barrier = pltpu.get_barrier_semaphore()
    north, south = lax.rem(lat + 3, 4), lax.rem(lat + 1, 4)
    west, east = lax.rem(lon + 3, 4), lax.rem(lon + 1, 4)

    def greet(target):
        pl.semaphore_signal(barrier, inc=1, device_id=target, device_id_type=MESH)

    for a in (north, south):
        for b in (west, east):
            greet({"lat": a, "lon": b})
    for step in (4, 3, 5, 2, 6, 1, 7):
        greet({"tm": lax.rem(tm + step, 8)})
    for a in (north, south):
        greet({"lat": a})
    for b in (west, east):
        greet({"lon": b})

    own_rows = pl.ds(LOW, END - LOW)

    for c in range(4):
        pltpu.make_async_copy(depth.at[:, cols(c)], DEP.at[c], in_sem.at[0]).start()
        pltpu.make_async_copy(mask.at[:, cols(c)], MSK.at[c], in_sem.at[1]).start()
        pltpu.make_async_copy(
            guess.at[0, :, cols(c)], F.at[CG, c, own_rows, :], in_sem.at[2]
        ).start()
    for field, level, i in ((G3, 3, 2), (G2, 2, 3), (G1, 1, 3), (G0, 0, 3)):
        for c in range(4):
            pltpu.make_async_copy(
                forcing.at[level, :, cols(c)], F.at[field, c, own_rows, :], in_sem.at[i]
            ).start()

    phase("a1_clear")
    def clear(ref):
        zero = jnp.zeros((TILES, 8, LANES), jnp.float32)
        ref[:, 0:8, :] = zero
        ref[:, 152:160, :] = zero

    def clear_fields(i, _):
        clear(F.at[i])
        return 0

    lax.fori_loop(0, 6, clear_fields, 0)
    for ref in (V, X, U):
        clear(ref)

    def clear_slab(i, _):
        ROW[:, i] = jnp.zeros((8, 8, LANES), jnp.float32)
        CR[i] = jnp.zeros((16, LANES), jnp.float32)
        return 0

    lax.fori_loop(0, 8, clear_slab, 0)
    KQ[...] = jnp.zeros((24, LANES), jnp.float32)
    for i in range(9):
        clear(GP.at[i])
    for i in range(3):
        clear(LG.at[i])

    phase("a2_loadwait")
    fields = F.at[pl.ds(1, 2), pl.ds(0, 4), own_rows, :]
    for i, ref in enumerate((DEP, MSK, fields)):
        pltpu.make_async_copy(ref, ref, in_sem.at[i]).wait()
    for c in range(4):
        F[DM, c, LOW:END, :] = jnp.where(MSK[c] > 0, DEP[c], 0.0)

    phase("a3_pack")
    lane3f = lane_iota((3, 8, LANES))
    lane1 = lane_iota((8, LANES))
    corners = ((136, 3, 8), (136, 0, 0), (16, 3, 8), (16, 0, 0))

    def pack(group):
        three = slice(3 * group, 3 * group + 3)
        right_edge = jnp.zeros((3, 8, LANES), jnp.float32)
        left_edge = jnp.zeros((3, 8, LANES), jnp.float32)
        for t in range(16):
            here = (lane3f >= 8 * t) & (lane3f < 8 * t + 8)
            rows = slice(LOW + 8 * t, LOW + 8 * t + 8)
            right = pltpu.roll(F[three, 3, rows, :], (8 * t + 8) % LANES, 2)
            right_edge = jnp.where(here, right, right_edge)
            left_edge = jnp.where(here, pltpu.roll(F[three, 0, rows, :], 8 * t, 2), left_edge)
        PKS[group, 0] = right_edge
        PKS[group, 1] = left_edge
        for i, (row, tile, shift) in enumerate(corners):
            packed = jnp.zeros((8, LANES), jnp.float32)
            for f in range(3):
                here = (lane1 >= 8 * f) & (lane1 < 8 * f + 8)
                edge = F[3 * group + f, tile, row : row + 8, :]
                packed = jnp.where(here, pltpu.roll(edge, (8 * f + shift) % LANES, 1), packed)
            CKS[group, i] = packed

    def unpack_halo(group):
        three = slice(3 * group, 3 * group + 3)
        from_left, from_right = PKR[group, 0], PKR[group, 1]
        for t in range(16):
            rows = slice(LOW + 8 * t, LOW + 8 * t + 8)
            a = pltpu.roll(from_left, (120 - 8 * t) % LANES, 2)
            b = pltpu.roll(from_right, (LANES - 8 * t) % LANES, 2)
            F[three, 4, rows, :] = jnp.where(lane3f >= 120, a, jnp.where(lane3f < 8, b, 0.0))
        for row, left, right in ((8, 0, 1), (144, 2, 3)):
            a0, b0 = CKR[group, left], CKR[group, right]
            for f in range(3):
                a = pltpu.roll(a0, (120 - 8 * f) % LANES, 1)
                b = pltpu.roll(b0, (LANES - 8 * f) % LANES, 1)
                edge = jnp.where(lane1 >= 120, a, jnp.where(lane1 < 8, b, 0.0))
                F[3 * group + f, 4, row : row + 8, :] = edge

    pack(0)

    phase("a4_barrier")
    pl.semaphore_wait(barrier, 15)


    def push(src, dst, i, target):
        pltpu.make_async_remote_copy(
            src, dst, hs, hr.at[i], device_id=target, device_id_type=MESH
        ).start()

    def wait_rows(sem, count):
        box = BOX.at[pl.ds(0, count)]
        pltpu.make_async_copy(box, box, sem).wait()

    targets = ((south, east), (south, west), (north, east), (north, west))

    def push_halo(group):
        for i, (a, b) in enumerate(targets):
            push(CKS.at[group, i], CKR.at[group, i], group, {"lat": a, "lon": b})
        fields = pl.ds(3 * group, 3)
        push(
            F.at[fields, pl.ds(0, 4), pl.ds(136, 8), :],
            F.at[fields, pl.ds(0, 4), pl.ds(8, 8), :],
            group, {"lat": south},
        )
        push(
            F.at[fields, pl.ds(0, 4), pl.ds(16, 8), :],
            F.at[fields, pl.ds(0, 4), pl.ds(144, 8), :],
            group, {"lat": north},
        )
        push(PKS.at[group, 0], PKR.at[group, 0], group, {"lon": east})
        push(PKS.at[group, 1], PKR.at[group, 1], group, {"lon": west})

    halo_rows = 4 * 8 + 2 * 96 + 2 * 24
    push_halo(0)
    fields = F.at[pl.ds(3, 3), pl.ds(0, 4), own_rows, :]
    pltpu.make_async_copy(fields, fields, in_sem.at[3]).wait()
    pack(1)
    push_halo(1)
    phase("a5_halowait")
    wait_rows(hr.at[0], halo_rows)

    pl.semaphore_signal(plane_sem, inc=1, device_id={"tm": sib}, device_id_type=MESH)
    phase("a6_unpack")
    unpack_halo(0)

    inside_top = jnp.where(lat > 0, 1.0, 0.0).astype(jnp.float32)
    inside_end = jnp.where(lat < 3, 1.0, 0.0).astype(jnp.float32)
    F[DM, :, 8:16, :] = F[DM, :, 8:16, :] * inside_top
    F[DM, :, 144:152, :] = F[DM, :, 144:152, :] * inside_end

    for row, count in FULL:
        d, *around = sides(F.at[DM], row, count)
        for i, other in enumerate(around):
            K[i, :, row : row + count, :] = jnp.where(
                (d > 0.0) & (other > 0.0), 1.5 * (d + other), 0.0
            )

    far_first = sorted(
        ((a, b) for a in range(4) for b in range(4) if (a, b) != (0, 0)),
        key=lambda ab: -(min(ab[0], 4 - ab[0]) + min(ab[1], 4 - ab[1])),
    )

    def plane_peer(a, b):
        return {"lat": lax.rem(lat + a, 4), "lon": lax.rem(lon + b, 4)}

    def diagonal(x, count):
        shape = (count, LANES)
        here = lane_iota(shape) == lax.broadcasted_iota(jnp.int32, shape, 0)
        picked = jnp.where(here, jnp.broadcast_to(x, shape), 0.0)
        return jnp.broadcast_to(jnp.sum(picked, axis=1, keepdims=True), shape)

    def send_sums(r, accs):
        row = lax.broadcasted_iota(jnp.int32, (16, LANES), 0)
        stacked = jnp.zeros((16, LANES), jnp.float32)
        for i, acc in enumerate(accs):
            stacked = jnp.where(row == i, jnp.sum(acc, axis=0, keepdims=True), stacked)
        stacked = jnp.broadcast_to(jnp.sum(stacked, axis=1, keepdims=True), (16, LANES))
        message = jnp.where(lane_iota((16, LANES)) == row, stacked, 0.0)
        message = jnp.sum(message, axis=0, keepdims=True)
        MSG[r, 0:1, :] = message
        AR[r, pl.ds(me, 1), :] = message
        for a, b in far_first:
            pltpu.make_async_remote_copy(
                MSG.at[r, pl.ds(0, 1)], AR.at[r, pl.ds(me, 1)], ar_s.at[r], ar_r.at[r],
                device_id=plane_peer(a, b), device_id_type=MESH,
            ).start()

    def recv_sums(r):
        wait_rows(ar_r.at[r], 15)
        return diagonal(jnp.sum(AR[r], axis=0, keepdims=True), 16)

    def prepare(field, slot):
        sums = Sums()
        for row, count in FULL:
            g, lg = spread(F.at[field], K, row, count)
            LG[slot, :, row : row + count, :] = lg
            g, lg = own_part(g, row, count), own_part(lg, row, count)
            sums.add(0, g, g)
            sums.add(1, g, lg)
            sums.add(2, lg, lg)
        for row, count in OWN:
            lg, llg = spread(LG.at[slot], K, row, count)
            sums.add(3, lg[:4], llg[:4])
        for i in range(4):
            KAP[slot, i] = sums.terms[i]

    def power(src, dst):
        for row, count in FULL:
            dst[:, row : row + count, :] = spread(src, K, row, count)[1]

    def line(acc):
        return jnp.sum(acc, axis=0, keepdims=True)

    def own_sum(a, b):
        return line(fold(a[:4, LOW:END, :] * b[:4, LOW:END, :]))

    g3_powers = [F.at[G3], LG.at[0]] + [GP.at[i] for i in range(5)]
    g2_powers = [F.at[G2], LG.at[2]] + [GP.at[i] for i in range(5, 9)]

    def powers_of_g3():
        for src, dst in zip(g3_powers[1:], g3_powers[2:]):
            power(src, dst)

    def powers_of_g2():
        prepare(G2, 2)
        for src, dst in zip(g2_powers[1:], g2_powers[2:]):
            power(src, dst)
        for i in range(4):
            KQ[i : i + 1, :] = line(KAP[0, i])
            KQ[11 + i : 12 + i, :] = line(KAP[2, i])
        KQ[4:5, :] = own_sum(g3_powers[2], g3_powers[2])
        KQ[5:6, :] = own_sum(g3_powers[2], g3_powers[3])
        for i in range(5):
            KQ[6 + i : 7 + i, :] = own_sum(g2_powers[0], g3_powers[i])

    def two_steps(r, v_ref, field, slot, between):
        phase(f"r{r}_moments")
        sums = Sums()
        for row, count in FULL:
            v, u = spread(v_ref, K, row, count)
            U[:, row : row + count, :] = u
            g = own_part(F[field, :, row : row + count, :], row, count)
            v, u = own_part(v, row, count), own_part(u, row, count)
            sums.add("m0", v, v)
            sums.add("m1", v, u)
            sums.add("m2", u, u)
            sums.add("n0", v, g)
            sums.add("n1", u, g)
        for row, count in FULL:
            u, w = spread(U, K, row, count)
            W[:, row : row + count, :] = w
            lg = own_part(LG[slot, :, row : row + count, :], row, count)
            u, w = own_part(u, row, count), own_part(w, row, count)
            sums.add("m3", u, w)
            sums.add("m4", w, w)
            sums.add("n2", u, lg)
            sums.add("n3", w, lg)
        for row, count in OWN:
            w, lw = spread(W, K, row, count)
            lg = LG[slot, :4, row : row + count, :]
            sums.add("m5", w[:4], lw[:4])
            sums.add("n4", lw[:4], lg)
        names = ["m0", "m1", "m2", "m3", "m4", "m5", "n0", "n1", "n2", "n3", "n4"]
        accs = [sums.terms[n] for n in names] + [KAP[slot, i] for i in range(4)]
        send_sums(r, accs)
        phase(f"r{r}_between")
        between()
        phase(f"r{r}_wait")
        total = recv_sums(r)
        phase(f"r{r}_scalars")
        at = [total[i : i + 1, :] for i in range(15)]
        m, n, k = at[:6], at[6:11], at[11:]
        a, b = fine_coefs(m)
        later = [
            jnp.maximum(
                a * a * m[i] + 2.0 * a * b * m[i + 1] + b * b * m[i + 2]
                + 2.0 * (a * n[i] + b * n[i + 1]) + k[i],
                0.0,
            )
            for i in range(4)
        ]
        a2, b2 = fine_coefs(later)
        return m, (a, b), (a2 * a, a2 * b + b2 * a, b2 * b, a2, b2)

    def scaled(s, x):
        return jnp.broadcast_to(s.reshape(1, 1, LANES), x.shape) * x

    phase("a7_prepare")
    prepare(G3, 0)

    def rest_of_halo():
        wait_rows(hr.at[1], halo_rows)
        unpack_halo(1)
        prepare(G1, 1)
        powers_of_g3()
        rows = pl.ds(pl.multiple_of(8 + 64 * core, 8), 80)
        for i in range(4):
            KH[i, :, 8:88, :] = K[i, :, rows, :]

    m_start, _, c = two_steps(0, F.at[CG], G3, 0, rest_of_halo)
    for row, count in FULL:
        part = slice(row, row + count)
        X[:, part, :] = (
            scaled(c[0], F[CG, :, part, :]) + scaled(c[1], U[:, part, :]) + scaled(c[2], W[:, part, :])
            + scaled(c[3], F[G3, :, part, :]) + scaled(c[4], LG[0, :, part, :]) + F[G2, :, part, :]
        )
    last = jnp.where(tm == 7, 1.0, 0.0).astype(jnp.float32)
    psi = m_start[0] / (m_start[0] + 4.0 * m_start[1] + EPS)
    drop = psi * (last - 1.0)

    _, _, c = two_steps(1, X, G1, 1, powers_of_g2)
    for h in range(2):
        for row, count in HALF:
            part = slice(64 * h + row, 64 * h + row + count)
            TH[h, tm, :, row : row + count, :] = (
                scaled(c[0], X[:, part, :]) + scaled(c[1], U[:, part, :])
                + scaled(c[2], W[:, part, :]) + scaled(c[3], F[G1, :, part, :])
                + scaled(c[4], LG[1, :, part, :]) + F[G0, :, part, :]
                + scaled(drop, F[CG, :, part, :])
            )

    phase("b0_gather")
    lane2 = lane_iota((8, LANES))
    for h in range(2):
        packed = jnp.zeros((8, LANES), jnp.float32)
        for t in range(10):
            row = 8 + 8 * t
            here = (lane2 >= 8 * t) & (lane2 < 8 * t + 8)
            edge = pltpu.roll(TH[h, tm, 4, row : row + 8, :], 8 * t + 4, 1)
            packed = jnp.where(here, edge, packed)
        PT[tm, h] = packed

    def half_copies(k, h, sem, target):
        main = TH.at[h, k, pl.ds(0, 4), pl.ds(12, 72), :]
        return [
            pltpu.make_async_remote_copy(
                ref, ref, sem, tr.at[k, h], device_id={"tm": target}, device_id_type=MESH
            )
            for ref in (main, PT.at[k, h])
        ]

    def start(copies):
        for copy in copies:
            copy.start()

    def sent(sem):
        wait_rows(sem, 4 * 72 + 8)

    def landed(k, h):
        wait_rows(tr.at[k, h], 4 * 72 + 8)

    def own_sends(act):
        for h in range(2):
            @pl.when(core == 1)
            def _():
                act(h, ts.at[0, h], sib)

            @pl.when(chip == 3)
            def _():
                act(h, ts.at[1, h], h)

            @pl.when(chip >= 1)
            def _():
                act(h, ts.at[2, h], jnp.maximum(2 * chip - 2 + h, 0))

            if h == 1:
                @pl.when(chip == 2)
                def _():
                    act(h, ts.at[1, h], 7)

    own_sends(lambda h, sem, target: start(half_copies(tm, h, sem, target)))

    def slab_at(e):
        dx = jnp.where((e == 1) | (e == 3), 1, jnp.where((e == 2) | (e == 5), 3, 2))
        odd = jnp.where((e == 1) | (e == 2) | (e == 4), 1, 0)
        k = jnp.where(e == 0, 2 * chip + 1, 2 * (chip + dx) + odd)
        valid = (e == 0) | (chip + dx <= 3)
        return jnp.minimum(k, 7), dx, odd, valid

    def unpack(k, h):
        packed = PT[k, h]
        for t in range(10):
            back = pltpu.roll(packed, (LANES - 8 * t - 4) % LANES, 1)
            back = jnp.where((lane2 < 4) | (lane2 >= 124), back, 0.0)
            TH[h, k, 4, 8 + 8 * t : 16 + 8 * t, :] = back

    def cross_sums(k, h):
        sums = Sums()
        rows = pl.ds(pl.multiple_of(HALF_LOW + 64 * h, 8), HALF_END - HALF_LOW)
        for t in range(4):
            value = TH[h, k, t, HALF_LOW:HALF_END, :]
            for i, ref in enumerate(g3_powers + g2_powers):
                sums.add(i, value, ref[t, rows, :])
        for i in range(13):
            CR[k, i : i + 1, :] = CR[k, i : i + 1, :] + line(sums.terms[i])

    def gram_sums(e, k):
        refs = [TH.at[core, k], UG.at[k], TG2.at[k], TG3.at[k]]
        for src, dst in zip(refs, refs[1:]):
            for row, count in HALF:
                dst[:, row : row + count, :] = spread(src, KH, row, count)[1]
        for row, count in HALF_OWN:
            last_power = spread(refs[3], KH, row, count)[1]
            TG4[k, :, row - HALF_LOW : row - HALF_LOW + count, :] = last_power[:4]
        cross_sums(k, core)

        def pair(q, _):
            j, _, _, held = slab_at(q)

            @pl.when(held)
            def _():
                sums = Sums()
                low, high = jnp.minimum(j, k), jnp.maximum(j, k)
                for t, (row, count) in ((t, rows) for t in range(4) for rows in HALF_OWN):
                    part = slice(row, row + count)
                    a, b = (
                        [TH[core, s, t, part, :]] + [ref[s, t, part, :] for ref in (UG, TG2, TG3)]
                        for s in (low, high)
                    )
                    b.append(TG4[high, t, row - HALF_LOW : row - HALF_LOW + count, :])
                    for i in range(8):
                        sums.add(i, a[i // 2], b[(i + 1) // 2])
                for i in range(8):
                    ROW[i, high, pl.ds(low, 1), :] = line(sums.terms[i])

            return 0

        lax.fori_loop(0, e + 1, pair, 0)

    def first_hand(e):
        k, dx, odd, valid = slab_at(e)

        @pl.when(valid)
        def _():
            @pl.when((e > 0) | (core == 0))
            def _():
                with jax.named_scope("b1_slabwait"):
                    landed(k, core)

            @pl.when((dx == 1) & (core == 0) & ((chip == 1) | (chip == 2)) & (e > 0))
            def _():
                start(half_copies(k, 0, rs.at[odd], jnp.maximum(tm - 2, 0)))

            @pl.when((dx == 3) & (core == 1) & (chip == 0) & (e > 0))
            def _():
                start(half_copies(k, 1, rs.at[odd], 3))

            @pl.when(e > 0)
            def _():
                start(half_copies(k, core, fs.at[e], sib))

            unpack(k, core)
            gram_sums(e, k)

    def second_hand(e):
        k, _, _, valid = slab_at(e)

        @pl.when(valid & (k > tm))
        def _():
            with jax.named_scope("b1_sibwait"):
                landed(k, 1 - core)
            unpack(k, 1 - core)
            cross_sums(k, 1 - core)

    def arrive(i, _):
        @pl.when(i < 7)
        def _():
            first_hand(jnp.minimum(i, 6))

        @pl.when(i >= 1)
        def _():
            second_hand(jnp.maximum(i - 1, 0))

        return 0

    @pl.when(tm == 7)
    def _():
        refs = [F.at[CG], U, W, V, X]
        for src, dst in zip(refs, refs[1:]):
            power(src, dst)
        for i in range(8):
            KQ[16 + i : 17 + i, :] = own_sum(refs[i // 2], refs[(i + 1) // 2])
        for i, ref in enumerate(g3_powers + g2_powers):
            CR[0, i : i + 1, :] = own_sum(refs[0], ref)

    @pl.when(tm == 7)
    def _():
        for odd in (1, 0):
            landed(4 + odd, 1)
            start(half_copies(4 + odd, 1, rs.at[odd], 1))

    phase("b1_arrive")
    lax.fori_loop(0, 8, arrive, 0)

    phase("b2_gram")
    lane3 = lane_iota((8, 8, LANES))
    sub3 = lax.broadcasted_iota(jnp.int32, (8, 8, LANES), 1)
    gram = jnp.zeros((8, 8, LANES), jnp.float32)
    for i in range(8):
        gram = jnp.where(lane3 == 8 * i + sub3, jnp.sum(ROW[i], axis=2, keepdims=True), gram)
    gram = jnp.sum(gram, axis=1)
    lane4 = lane_iota((8, 16, LANES))
    sub4 = lax.broadcasted_iota(jnp.int32, (8, 16, LANES), 1)
    slab4 = lax.broadcasted_iota(jnp.int32, (8, 16, LANES), 0)
    cross = jnp.where(
        (lane4 == 13 * slab4 + sub4) & (sub4 < 13), jnp.sum(CR[...], axis=2, keepdims=True), 0.0
    )
    cross = jnp.sum(jnp.sum(cross, axis=0), axis=0, keepdims=True)
    lane5 = lane_iota((24, LANES))
    sub5 = lax.broadcasted_iota(jnp.int32, (24, LANES), 0)
    own = jnp.where(lane5 == 104 + sub5, jnp.sum(KQ[...], axis=1, keepdims=True), 0.0)
    own = cross + jnp.sum(own, axis=0, keepdims=True)
    sub2 = lax.broadcasted_iota(jnp.int32, (8, LANES), 0)
    folded = jnp.where(lane2 < 64, pltpu.roll(gram, 4, 0), pltpu.roll(gram, 64, 1))
    message = jnp.where(sub2 < 4, folded, jnp.where(sub2 == 4, own, 0.0))
    GM[...] = message
    GR[core * 16 + me] = message
    pl.semaphore_wait(plane_sem, 1)
    for a, b in far_first + [(0, 0)]:
        targets = [{"tm": sib, **plane_peer(a, b)}] + ([plane_peer(a, b)] if (a, b) != (0, 0) else [])
        for target in targets:
            pltpu.make_async_remote_copy(
                GM.at[pl.ds(0, 5)], GR.at[core * 16 + me, pl.ds(0, 5)], gs, gr,
                device_id=target, device_id_type=MESH,
            ).start()
    phase("b3_wait")
    wait_rows(gr, 31 * 5)
    total = jnp.sum(GR[...], axis=0)
    plane = jnp.sum(GR[pl.ds(core * 16, 16)], axis=0)
    phase("b4_chain")

    high_slabs = [diagonal(total[k : k + 1, :], LANES) for k in range(4)]
    own_sums = diagonal(plane[4:5, :], LANES)
    with_g = [[own_sums[13 * k + i : 13 * k + i + 1, :] for k in range(8)] for i in range(13)]
    first_row = [own_sums[104 + i : 105 + i, :] for i in range(24)]
    k33, k32, k22 = first_row[:6], first_row[6:11], first_row[11:15]

    def entry(i, k, j):
        at = 8 * i + j if k >= 4 else 64 + 8 * i + j
        return high_slabs[k % 4][at : at + 1, :]

    one = jnp.ones((1, LANES), jnp.float32)
    zero = jnp.zeros((1, LANES), jnp.float32)
    coefs = {7: one}
    quad = [entry(i, 7, 7) for i in range(8)]
    cross = [{j: entry(i, 7, j) for j in range(1, 7)} for i in range(8)]
    mixed = [x[7] for x in with_g]
    is_last = jnp.full((1, LANES), tm == 7)
    held_c = {k: zero for k in range(1, 8)}
    held_q = first_row[16:24]
    held_m = [x[0] for x in with_g]
    for t in range(7, 0, -1):
        if t < 7:
            psi_t = quad[0] / (quad[0] + 4.0 * quad[1] + EPS)
            quad = [
                psi_t * psi_t * quad[i] + 2.0 * psi_t * cross[i][t] + entry(i, t, t)
                for i in range(8)
            ]
            cross = [{j: psi_t * cross[i][j] + entry(i, t, j) for j in range(1, t)} for i in range(8)]
            mixed = [psi_t * x + y[t] for x, y in zip(mixed, with_g)]
            coefs = {k: psi_t * x for k, x in coefs.items()}
            coefs[t] = one
        now = jnp.full((1, LANES), tm + 1 == t)
        for k in coefs:
            held_c[k] = jnp.where(now, coefs[k], held_c[k])
        held_q = [jnp.where(now, quad[i], held_q[i]) for i in range(8)]
        held_m = [jnp.where(now, mixed[i], held_m[i]) for i in range(13)]
    psi = held_q[0] / (held_q[0] + 4.0 * held_q[1] + EPS)
    psi = jnp.where(is_last, 0.0, psi)
    for row, count in FULL:
        part = slice(row, row + count)
        value = F[CG, :, part, :] * last
        for k in range(1, 8):
            slab = TH[row // 80, k, :, row - 64 * (row // 80) : row - 64 * (row // 80) + count, :]
            value = value + scaled(held_c[k], jnp.where(tm < k, slab, 0.0))
        V[:, part, :] = value

    def put(level, row, value):
        for t in range(4):
            out[level, row - LOW : row - LOW + value.shape[1], cols(t)] = value[t]

    def next_moments(a, b, m, n, k, count):
        return [
            jnp.maximum(
                a * a * m[i] + 2.0 * a * b * m[i + 1] + b * b * m[i + 2]
                + 2.0 * (a * n[i] + b * n[i + 1]) + k[i],
                0.0,
            )
            for i in range(count)
        ]

    a1, b1 = fine_coefs(held_q)
    m1 = next_moments(a1, b1, held_q, held_m[:7], k33, 6)
    n1 = [a1 * held_m[7 + i] + b1 * held_m[8 + i] + k32[i] for i in range(5)]
    a2, b2 = fine_coefs(m1)
    m2 = next_moments(a2, b2, m1, n1, k22, 4)
    a3, b3 = fine_coefs(m2)
    phase("c0_correct")
    for row, count in FULL:
        part = slice(row, row + count)
        v, u = spread(V, K, row, count)
        value = scaled(a1, v) + scaled(b1, u) + F[G3, :, part, :]
        X[:, part, :] = value
        put(3, max(row, LOW), own_part(value, row, count))
    for row, count in FULL:
        part = slice(row, row + count)
        v, u = spread(X, K, row, count)
        value = scaled(a2, v) + scaled(b2, u) + F[G2, :, part, :]
        W[:, part, :] = value
        put(2, max(row, LOW), own_part(value, row, count))
    for row, count in OWN:
        part = slice(row, row + count)
        v, u = spread(W, K, row, count)
        put(1, row, scaled(a3, v[:4]) + scaled(b3, u[:4]) + F[G1, :4, part, :])
        first = row - 64 * (row // 80)
        put(0, row, scaled(psi, V[:4, part, :]) + TH[row // 80, tm, :4, first : first + count, :])

    phase("c9_end")
    wait_rows(hs, 2 * halo_rows)
    for r in range(2):
        wait_rows(ar_s.at[r], 15)
    wait_rows(gs, 31 * 5)
    own_sends(lambda h, sem, target: sent(sem))
    for e in range(1, 7):
        @pl.when(slab_at(e)[3])
        def _():
            sent(fs.at[e])

    relays = ((core == 0) & ((chip == 1) | (chip == 2))) | ((core == 1) & ((chip == 0) | (chip == 3)))

    @pl.when(relays)
    def _():
        for odd in range(2):
            sent(rs.at[odd])

    phase(None)


def local(forcing, depth, mask, guess):
    f32 = jnp.float32
    field = (TILES, ROWS, LANES)
    half = (TILES, HALF_ROWS, LANES)
    dma = pltpu.SemaphoreType.DMA
    return pl.pallas_call(
        kernel,
        out_shape=jax.ShapeDtypeStruct(forcing.shape, f32),
        in_specs=[pl.BlockSpec(memory_space=pltpu.HBM)] * 4,
        out_specs=pl.BlockSpec(memory_space=pltpu.VMEM),
        scratch_shapes=[
            pltpu.VMEM((6, *field), f32),
            pltpu.VMEM((4, *field), f32),
            pltpu.VMEM(field, f32),
            pltpu.VMEM(field, f32),
            pltpu.VMEM(field, f32),
            pltpu.VMEM(field, f32),
            pltpu.VMEM((3, *field), f32),
            pltpu.VMEM((9, *field), f32),
            pltpu.VMEM((4, *half), f32),
            pltpu.VMEM((2, 8, *half), f32),
            pltpu.VMEM((8, *half), f32),
            pltpu.VMEM((8, *half), f32),
            pltpu.VMEM((8, *half), f32),
            pltpu.VMEM((8, 4, 64, LANES), f32),
            pltpu.VMEM((4, 128, LANES), f32),
            pltpu.VMEM((4, 128, LANES), jnp.int32),
            pltpu.VMEM((3, 4, 8, LANES), f32),
            pltpu.VMEM((8, 8, 8, LANES), f32),
            pltpu.VMEM((8, 16, LANES), f32),
            pltpu.VMEM((24, LANES), f32),
            pltpu.VMEM((2, 2, 3, 8, LANES), f32),
            pltpu.VMEM((2, 2, 3, 8, LANES), f32),
            pltpu.VMEM((2, 4, 8, LANES), f32),
            pltpu.VMEM((2, 4, 8, LANES), f32),
            pltpu.VMEM((8, 2, 8, LANES), f32),
            pltpu.VMEM((2, 8, LANES), f32),
            pltpu.VMEM((2, 16, LANES), f32),
            pltpu.VMEM((8, LANES), f32),
            pltpu.VMEM((32, 8, LANES), f32),
            pltpu.VMEM((544, LANES), f32),
            dma((4,)),
            dma,
            dma((2,)),
            dma((2,)),
            dma((2,)),
            dma((3, 2)),
            dma((8, 2)),
            dma((7,)),
            dma((2,)),
            dma,
            dma,
            pltpu.SemaphoreType.REGULAR,
        ],
        compiler_params=pltpu.CompilerParams(
            collective_id=0, has_side_effects=True, vmem_limit_bytes=VMEM_LIMIT
        ),
        name="cycle",
    )(*(pltpu.with_memory_space_constraint(x, pltpu.HBM) for x in (forcing, depth, mask, guess)))


def solution(mesh):
    return jax.shard_map(
        local,
        mesh=mesh,
        in_specs=(P("tm", "lat", "lon"), P("lat", "lon"), P("lat", "lon"), P("tm", "lat", "lon")),
        out_specs=P("tm", "lat", "lon"),
        check_vma=False,
    )
```

```python
import functools

import jax
import jax.numpy as jnp
from jax import lax
from jax.experimental import pallas as pl
from jax.experimental.pallas import tpu as pltpu
from jax.sharding import PartitionSpec as P

FS = 4
EPS = 1e-6
VMEM_LIMIT = 40 * 1024 * 1024
MESH = pl.DeviceIdType.MESH

TILES, ROWS, LANES = 5, 160, 128
TOP, LOW, END = 8, 16, 144
FULL = tuple((row, 24) for row in range(8, 152, 24))
OWN = tuple((row, 32) for row in range(16, 144, 32))
HALF_ROWS = 96
HALF = ((8, 24), (32, 24), (56, 32))
HALF_OWN = ((16, 32), (48, 32))
HALF_LOW, HALF_END = 16, 80
DM, CG, G3, G2, G1, G0 = range(6)


def lane_iota(shape):
    return lax.broadcasted_iota(jnp.int32, shape, len(shape) - 1)


def sides(ref, row, count):
    v = ref[:, row : row + count, :]
    down = ref[:, row + 1 : row + 1 + count, :]
    up = ref[:, row - 1 : row - 1 + count, :]
    lane = lane_iota(v.shape)
    ahead = pltpu.roll(v, LANES - 1, 2)
    right = jnp.where(lane == LANES - 1, jnp.concatenate([ahead[1:], ahead[:1]], 0), ahead)
    behind = pltpu.roll(v, 1, 2)
    left = jnp.where(lane == 0, jnp.concatenate([behind[-1:], behind[:-1]], 0), behind)
    return v, right, left, down, up


def spread(ref, coef, row, count):
    v, right, left, down, up = sides(ref, row, count)
    part = slice(row, row + count)
    out = coef[0, :, part, :] * (v - right) + coef[1, :, part, :] * (v - left)
    out = out + coef[2, :, part, :] * (v - down) + coef[3, :, part, :] * (v - up)
    return v, out


def own_part(x, row, count):
    first, last = max(row, LOW) - row, min(row + count, END) - row
    return x[:4, first:last, :]


def fold(x):
    return jnp.sum(x.reshape(-1, 8, LANES), axis=0)


class Phase:
    def __init__(self):
        self.open = None

    def __call__(self, name):
        if self.open is not None:
            self.open.__exit__(None, None, None)
        self.open = jax.named_scope(name) if name else None
        if self.open is not None:
            self.open.__enter__()


class Sums:
    def __init__(self):
        self.terms = {}

    def add(self, key, a, b):
        value = fold(a * b)
        self.terms[key] = value if key not in self.terms else self.terms[key] + value


def fine_coefs(m):
    den = m[0] + m[1] + EPS
    alpha = m[0] / den
    gamma = (m[1] + EPS) / den
    s1 = jnp.maximum(
        gamma * gamma * m[0] - 2.0 * gamma * alpha * m[1] + alpha * alpha * m[2], 0.0
    )
    beta = s1 / (m[0] + EPS)
    f = gamma + beta
    pp = s1 + beta * (2.0 * EPS * alpha + beta * m[0])
    plp = jnp.maximum(f * f * m[1] - 2.0 * f * alpha * m[2] + alpha * alpha * m[3], 0.0)
    later = jnp.minimum(s1 / (pp + plp + EPS), 1.0)
    return alpha + later * f, -alpha * later


def kernel(
    forcing, depth, mask, guess, out,
    F, K, V, X, U, W, LG, GP, KH, TH, UG, TG2, TG3, TG4, DEP, MSK, KAP, ROW, CR, KQ,
    PKS, PKR, CKS, CKR, PT, MSG, AR,
    GM, GR, BOX, in_sem, done, hr, ar_r, tr, gr, plane_sem,
):
    phase = Phase()
    phase("a0_load")
    tm = lax.axis_index("tm")
    lat = lax.axis_index("lat")
    lon = lax.axis_index("lon")
    me = lat * 4 + lon
    chip, core = tm // 2, tm % 2
    sib = 2 * chip + 1 - core

    def cols(c):
        return pl.ds(LANES * c, LANES)

    barrier = pltpu.get_barrier_semaphore()
    north, south = lax.rem(lat + 3, 4), lax.rem(lat + 1, 4)
    west, east = lax.rem(lon + 3, 4), lax.rem(lon + 1, 4)

    def greet(target):
        pl.semaphore_signal(barrier, inc=1, device_id=target, device_id_type=MESH)

    for a in (north, south):
        for b in (west, east):
            greet({"lat": a, "lon": b})
    for step in (4, 3, 5, 2, 6, 1, 7):
        greet({"tm": lax.rem(tm + step, 8)})
    for a in (north, south):
        greet({"lat": a})
    for b in (west, east):
        greet({"lon": b})

    own_rows = pl.ds(LOW, END - LOW)

    for c in range(4):
        pltpu.make_async_copy(depth.at[:, cols(c)], DEP.at[c], in_sem.at[0]).start()
        pltpu.make_async_copy(mask.at[:, cols(c)], MSK.at[c], in_sem.at[1]).start()
        pltpu.make_async_copy(
            guess.at[0, :, cols(c)], F.at[CG, c, own_rows, :], in_sem.at[2]
        ).start()
    for field, level, i in ((G3, 3, 2), (G2, 2, 3), (G1, 1, 3), (G0, 0, 3)):
        for c in range(4):
            pltpu.make_async_copy(
                forcing.at[level, :, cols(c)], F.at[field, c, own_rows, :], in_sem.at[i]
            ).start()

    phase("a1_clear")
    def clear(ref):
        zero = jnp.zeros((TILES, 8, LANES), jnp.float32)
        ref[:, 0:8, :] = zero
        ref[:, 152:160, :] = zero

    def clear_fields(i, _):
        clear(F.at[i])
        return 0

    lax.fori_loop(0, 6, clear_fields, 0)
    for ref in (V, X, U):
        clear(ref)

    def clear_slab(i, _):
        ROW[:, i] = jnp.zeros((8, 8, LANES), jnp.float32)
        CR[i] = jnp.zeros((16, LANES), jnp.float32)
        return 0

    lax.fori_loop(0, 8, clear_slab, 0)
    KQ[...] = jnp.zeros((24, LANES), jnp.float32)
    for i in range(9):
        clear(GP.at[i])
    for i in range(3):
        clear(LG.at[i])

    phase("a2_loadwait")
    fields = F.at[pl.ds(1, 2), pl.ds(0, 4), own_rows, :]
    for i, ref in enumerate((DEP, MSK, fields)):
        pltpu.make_async_copy(ref, ref, in_sem.at[i]).wait()
    for c in range(4):
        F[DM, c, LOW:END, :] = jnp.where(MSK[c] > 0, DEP[c], 0.0)

    phase("a3_pack")
    lane3f = lane_iota((3, 8, LANES))
    lane1 = lane_iota((8, LANES))
    corners = ((136, 3, 8), (136, 0, 0), (16, 3, 8), (16, 0, 0))

    def pack(group):
        three = slice(3 * group, 3 * group + 3)
        right_edge = jnp.zeros((3, 8, LANES), jnp.float32)
        left_edge = jnp.zeros((3, 8, LANES), jnp.float32)
        for t in range(16):
            here = (lane3f >= 8 * t) & (lane3f < 8 * t + 8)
            rows = slice(LOW + 8 * t, LOW + 8 * t + 8)
            right = pltpu.roll(F[three, 3, rows, :], (8 * t + 8) % LANES, 2)
            right_edge = jnp.where(here, right, right_edge)
            left_edge = jnp.where(here, pltpu.roll(F[three, 0, rows, :], 8 * t, 2), left_edge)
        PKS[group, 0] = right_edge
        PKS[group, 1] = left_edge
        for i, (row, tile, shift) in enumerate(corners):
            packed = jnp.zeros((8, LANES), jnp.float32)
            for f in range(3):
                here = (lane1 >= 8 * f) & (lane1 < 8 * f + 8)
                edge = F[3 * group + f, tile, row : row + 8, :]
                packed = jnp.where(here, pltpu.roll(edge, (8 * f + shift) % LANES, 1), packed)
            CKS[group, i] = packed

    def unpack_halo(group):
        three = slice(3 * group, 3 * group + 3)
        from_left, from_right = PKR[group, 0], PKR[group, 1]
        for t in range(16):
            rows = slice(LOW + 8 * t, LOW + 8 * t + 8)
            a = pltpu.roll(from_left, (120 - 8 * t) % LANES, 2)
            b = pltpu.roll(from_right, (LANES - 8 * t) % LANES, 2)
            F[three, 4, rows, :] = jnp.where(lane3f >= 120, a, jnp.where(lane3f < 8, b, 0.0))
        for row, left, right in ((8, 0, 1), (144, 2, 3)):
            a0, b0 = CKR[group, left], CKR[group, right]
            for f in range(3):
                a = pltpu.roll(a0, (120 - 8 * f) % LANES, 1)
                b = pltpu.roll(b0, (LANES - 8 * f) % LANES, 1)
                edge = jnp.where(lane1 >= 120, a, jnp.where(lane1 < 8, b, 0.0))
                F[3 * group + f, 4, row : row + 8, :] = edge

    pack(0)

    phase("a4_barrier")
    pl.semaphore_wait(barrier, 15)


    def push(src, dst, i, target):
        pltpu.make_async_remote_copy(
            src, dst, done, hr.at[i], device_id=target, device_id_type=MESH
        ).start()

    def wait_rows(sem, count):
        box = BOX.at[pl.ds(0, count)]
        pltpu.make_async_copy(box, box, sem).wait()

    targets = ((south, east), (south, west), (north, east), (north, west))

    def push_halo(group):
        for i, (a, b) in enumerate(targets):
            push(CKS.at[group, i], CKR.at[group, i], group, {"lat": a, "lon": b})
        fields = pl.ds(3 * group, 3)
        push(
            F.at[fields, pl.ds(0, 4), pl.ds(136, 8), :],
            F.at[fields, pl.ds(0, 4), pl.ds(8, 8), :],
            group, {"lat": south},
        )
        push(
            F.at[fields, pl.ds(0, 4), pl.ds(16, 8), :],
            F.at[fields, pl.ds(0, 4), pl.ds(144, 8), :],
            group, {"lat": north},
        )
        push(PKS.at[group, 0], PKR.at[group, 0], group, {"lon": east})
        push(PKS.at[group, 1], PKR.at[group, 1], group, {"lon": west})

    halo_rows = 4 * 8 + 2 * 96 + 2 * 24
    push_halo(0)
    fields = F.at[pl.ds(3, 3), pl.ds(0, 4), own_rows, :]
    pltpu.make_async_copy(fields, fields, in_sem.at[3]).wait()
    pack(1)
    push_halo(1)
    phase("a5_halowait")
    wait_rows(hr.at[0], halo_rows)

    pl.semaphore_signal(plane_sem, inc=1, device_id={"tm": sib}, device_id_type=MESH)
    phase("a6_unpack")
    unpack_halo(0)

    inside_top = jnp.where(lat > 0, 1.0, 0.0).astype(jnp.float32)
    inside_end = jnp.where(lat < 3, 1.0, 0.0).astype(jnp.float32)
    F[DM, :, 8:16, :] = F[DM, :, 8:16, :] * inside_top
    F[DM, :, 144:152, :] = F[DM, :, 144:152, :] * inside_end

    for row, count in FULL:
        d, *around = sides(F.at[DM], row, count)
        for i, other in enumerate(around):
            K[i, :, row : row + count, :] = jnp.where(
                (d > 0.0) & (other > 0.0), 1.5 * (d + other), 0.0
            )

    far_first = sorted(
        ((a, b) for a in range(4) for b in range(4) if (a, b) != (0, 0)),
        key=lambda ab: -(min(ab[0], 4 - ab[0]) + min(ab[1], 4 - ab[1])),
    )

    def plane_peer(a, b):
        return {"lat": lax.rem(lat + a, 4), "lon": lax.rem(lon + b, 4)}

    def diagonal(x, count):
        shape = (count, LANES)
        here = lane_iota(shape) == lax.broadcasted_iota(jnp.int32, shape, 0)
        picked = jnp.where(here, jnp.broadcast_to(x, shape), 0.0)
        return jnp.broadcast_to(jnp.sum(picked, axis=1, keepdims=True), shape)

    def send_sums(r, accs):
        row = lax.broadcasted_iota(jnp.int32, (16, LANES), 0)
        stacked = jnp.zeros((16, LANES), jnp.float32)
        for i, acc in enumerate(accs):
            stacked = jnp.where(row == i, jnp.sum(acc, axis=0, keepdims=True), stacked)
        stacked = jnp.broadcast_to(jnp.sum(stacked, axis=1, keepdims=True), (16, LANES))
        message = jnp.where(lane_iota((16, LANES)) == row, stacked, 0.0)
        message = jnp.sum(message, axis=0, keepdims=True)
        MSG[r, 0:1, :] = message
        AR[r, pl.ds(me, 1), :] = message
        for a, b in far_first:
            pltpu.make_async_remote_copy(
                MSG.at[r, pl.ds(0, 1)], AR.at[r, pl.ds(me, 1)], done, ar_r.at[r],
                device_id=plane_peer(a, b), device_id_type=MESH,
            ).start()

    def recv_sums(r):
        wait_rows(ar_r.at[r], 15)
        return diagonal(jnp.sum(AR[r], axis=0, keepdims=True), 16)

    def prepare(field, slot):
        sums = Sums()
        for row, count in FULL:
            g, lg = spread(F.at[field], K, row, count)
            LG[slot, :, row : row + count, :] = lg
            g, lg = own_part(g, row, count), own_part(lg, row, count)
            sums.add(0, g, g)
            sums.add(1, g, lg)
            sums.add(2, lg, lg)
        for row, count in OWN:
            lg, llg = spread(LG.at[slot], K, row, count)
            sums.add(3, lg[:4], llg[:4])
        for i in range(4):
            KAP[slot, i] = sums.terms[i]

    def power(src, dst):
        for row, count in FULL:
            dst[:, row : row + count, :] = spread(src, K, row, count)[1]

    def line(acc):
        return jnp.sum(acc, axis=0, keepdims=True)

    def own_sum(a, b):
        return line(fold(a[:4, LOW:END, :] * b[:4, LOW:END, :]))

    g3_powers = [F.at[G3], LG.at[0]] + [GP.at[i] for i in range(5)]
    g2_powers = [F.at[G2], LG.at[2]] + [GP.at[i] for i in range(5, 9)]

    def powers_of_g3():
        for src, dst in zip(g3_powers[1:], g3_powers[2:]):
            power(src, dst)

    def powers_of_g2():
        prepare(G2, 2)
        for src, dst in zip(g2_powers[1:], g2_powers[2:]):
            power(src, dst)
        for i in range(4):
            KQ[i : i + 1, :] = line(KAP[0, i])
            KQ[11 + i : 12 + i, :] = line(KAP[2, i])
        KQ[4:5, :] = own_sum(g3_powers[2], g3_powers[2])
        KQ[5:6, :] = own_sum(g3_powers[2], g3_powers[3])
        for i in range(5):
            KQ[6 + i : 7 + i, :] = own_sum(g2_powers[0], g3_powers[i])

    def two_steps(r, v_ref, field, slot, between):
        phase(f"r{r}_moments")
        sums = Sums()
        for row, count in FULL:
            v, u = spread(v_ref, K, row, count)
            U[:, row : row + count, :] = u
            g = own_part(F[field, :, row : row + count, :], row, count)
            v, u = own_part(v, row, count), own_part(u, row, count)
            sums.add("m0", v, v)
            sums.add("m1", v, u)
            sums.add("m2", u, u)
            sums.add("n0", v, g)
            sums.add("n1", u, g)
        for row, count in FULL:
            u, w = spread(U, K, row, count)
            W[:, row : row + count, :] = w
            lg = own_part(LG[slot, :, row : row + count, :], row, count)
            u, w = own_part(u, row, count), own_part(w, row, count)
            sums.add("m3", u, w)
            sums.add("m4", w, w)
            sums.add("n2", u, lg)
            sums.add("n3", w, lg)
        for row, count in OWN:
            w, lw = spread(W, K, row, count)
            lg = LG[slot, :4, row : row + count, :]
            sums.add("m5", w[:4], lw[:4])
            sums.add("n4", lw[:4], lg)
        names = ["m0", "m1", "m2", "m3", "m4", "m5", "n0", "n1", "n2", "n3", "n4"]
        accs = [sums.terms[n] for n in names] + [KAP[slot, i] for i in range(4)]
        send_sums(r, accs)
        phase(f"r{r}_between")
        between()
        phase(f"r{r}_wait")
        total = recv_sums(r)
        phase(f"r{r}_scalars")
        at = [total[i : i + 1, :] for i in range(15)]
        m, n, k = at[:6], at[6:11], at[11:]
        a, b = fine_coefs(m)
        later = [
            jnp.maximum(
                a * a * m[i] + 2.0 * a * b * m[i + 1] + b * b * m[i + 2]
                + 2.0 * (a * n[i] + b * n[i + 1]) + k[i],
                0.0,
            )
            for i in range(4)
        ]
        a2, b2 = fine_coefs(later)
        return m, (a, b), (a2 * a, a2 * b + b2 * a, b2 * b, a2, b2)

    def scaled(s, x):
        return jnp.broadcast_to(s.reshape(1, 1, LANES), x.shape) * x

    phase("a7_prepare")
    prepare(G3, 0)

    def rest_of_halo():
        wait_rows(hr.at[1], halo_rows)
        unpack_halo(1)
        prepare(G1, 1)
        powers_of_g3()
        rows = pl.ds(pl.multiple_of(8 + 64 * core, 8), 80)
        for i in range(4):
            KH[i, :, 8:88, :] = K[i, :, rows, :]

    m_start, _, c = two_steps(0, F.at[CG], G3, 0, rest_of_halo)
    for row, count in FULL:
        part = slice(row, row + count)
        X[:, part, :] = (
            scaled(c[0], F[CG, :, part, :]) + scaled(c[1], U[:, part, :]) + scaled(c[2], W[:, part, :])
            + scaled(c[3], F[G3, :, part, :]) + scaled(c[4], LG[0, :, part, :]) + F[G2, :, part, :]
        )
    last = jnp.where(tm == 7, 1.0, 0.0).astype(jnp.float32)
    psi = m_start[0] / (m_start[0] + 4.0 * m_start[1] + EPS)
    drop = psi * (last - 1.0)

    _, _, c = two_steps(1, X, G1, 1, powers_of_g2)
    for h in range(2):
        for row, count in HALF:
            part = slice(64 * h + row, 64 * h + row + count)
            TH[h, tm, :, row : row + count, :] = (
                scaled(c[0], X[:, part, :]) + scaled(c[1], U[:, part, :])
                + scaled(c[2], W[:, part, :]) + scaled(c[3], F[G1, :, part, :])
                + scaled(c[4], LG[1, :, part, :]) + F[G0, :, part, :]
                + scaled(drop, F[CG, :, part, :])
            )

    phase("b0_gather")
    lane2 = lane_iota((8, LANES))
    for h in range(2):
        packed = jnp.zeros((8, LANES), jnp.float32)
        for t in range(10):
            row = 8 + 8 * t
            here = (lane2 >= 8 * t) & (lane2 < 8 * t + 8)
            edge = pltpu.roll(TH[h, tm, 4, row : row + 8, :], 8 * t + 4, 1)
            packed = jnp.where(here, edge, packed)
        PT[tm, h] = packed

    def half_copies(k, h, sem, target):
        main = TH.at[h, k, pl.ds(0, 4), pl.ds(12, 72), :]
        return [
            pltpu.make_async_remote_copy(
                ref, ref, sem, tr.at[k, h], device_id={"tm": target}, device_id_type=MESH
            )
            for ref in (main, PT.at[k, h])
        ]

    def start(copies):
        for copy in copies:
            copy.start()

    def landed(k, h):
        wait_rows(tr.at[k, h], 4 * 72 + 8)

    def own_sends(act):
        for h in range(2):
            @pl.when(core == 1)
            def _():
                act(h, done, sib)

            @pl.when(chip == 3)
            def _():
                act(h, done, h)

            @pl.when(chip >= 1)
            def _():
                act(h, done, jnp.maximum(2 * chip - 2 + h, 0))

            if h == 1:
                @pl.when(chip == 2)
                def _():
                    act(h, done, 7)

    own_sends(lambda h, sem, target: start(half_copies(tm, h, sem, target)))

    def slab_at(e):
        dx = jnp.where((e == 1) | (e == 3), 1, jnp.where((e == 2) | (e == 5), 3, 2))
        odd = jnp.where((e == 1) | (e == 2) | (e == 4), 1, 0)
        k = jnp.where(e == 0, 2 * chip + 1, 2 * (chip + dx) + odd)
        valid = (e == 0) | (chip + dx <= 3)
        return jnp.minimum(k, 7), dx, odd, valid

    def unpack(k, h):
        packed = PT[k, h]
        for t in range(10):
            back = pltpu.roll(packed, (LANES - 8 * t - 4) % LANES, 1)
            back = jnp.where((lane2 < 4) | (lane2 >= 124), back, 0.0)
            TH[h, k, 4, 8 + 8 * t : 16 + 8 * t, :] = back

    def cross_sums(k, h):
        sums = Sums()
        rows = pl.ds(pl.multiple_of(HALF_LOW + 64 * h, 8), HALF_END - HALF_LOW)
        for t in range(4):
            value = TH[h, k, t, HALF_LOW:HALF_END, :]
            for i, ref in enumerate(g3_powers + g2_powers):
                sums.add(i, value, ref[t, rows, :])
        for i in range(13):
            CR[k, i : i + 1, :] = CR[k, i : i + 1, :] + line(sums.terms[i])

    def gram_sums(e, k):
        refs = [TH.at[core, k], UG.at[k], TG2.at[k], TG3.at[k]]
        for src, dst in zip(refs, refs[1:]):
            for row, count in HALF:
                dst[:, row : row + count, :] = spread(src, KH, row, count)[1]
        for row, count in HALF_OWN:
            last_power = spread(refs[3], KH, row, count)[1]
            TG4[k, :, row - HALF_LOW : row - HALF_LOW + count, :] = last_power[:4]
        cross_sums(k, core)

        def pair(q, _):
            j, _, _, held = slab_at(q)

            @pl.when(held)
            def _():
                sums = Sums()
                low, high = jnp.minimum(j, k), jnp.maximum(j, k)
                for t, (row, count) in ((t, rows) for t in range(4) for rows in HALF_OWN):
                    part = slice(row, row + count)
                    a, b = (
                        [TH[core, s, t, part, :]] + [ref[s, t, part, :] for ref in (UG, TG2, TG3)]
                        for s in (low, high)
                    )
                    b.append(TG4[high, t, row - HALF_LOW : row - HALF_LOW + count, :])
                    for i in range(8):
                        sums.add(i, a[i // 2], b[(i + 1) // 2])
                for i in range(8):
                    ROW[i, high, pl.ds(low, 1), :] = line(sums.terms[i])

            return 0

        lax.fori_loop(0, e + 1, pair, 0)

    def first_hand(e):
        k, dx, odd, valid = slab_at(e)

        @pl.when(valid)
        def _():
            @pl.when((e > 0) | (core == 0))
            def _():
                with jax.named_scope("b1_slabwait"):
                    landed(k, core)

            @pl.when((dx == 1) & (core == 0) & ((chip == 1) | (chip == 2)) & (e > 0))
            def _():
                start(half_copies(k, 0, done, jnp.maximum(tm - 2, 0)))

            @pl.when((dx == 3) & (core == 1) & (chip == 0) & (e > 0))
            def _():
                start(half_copies(k, 1, done, 3))

            @pl.when(e > 0)
            def _():
                start(half_copies(k, core, done, sib))

            unpack(k, core)
            gram_sums(e, k)

    def second_hand(e):
        k, _, _, valid = slab_at(e)

        @pl.when(valid & (k > tm))
        def _():
            with jax.named_scope("b1_sibwait"):
                landed(k, 1 - core)
            unpack(k, 1 - core)
            cross_sums(k, 1 - core)

    def arrive(i, _):
        @pl.when(i < 7)
        def _():
            first_hand(jnp.minimum(i, 6))

        @pl.when(i >= 1)
        def _():
            second_hand(jnp.maximum(i - 1, 0))

        return 0

    @pl.when(tm == 7)
    def _():
        refs = [F.at[CG], U, W, V, X]
        for src, dst in zip(refs, refs[1:]):
            power(src, dst)
        for i in range(8):
            KQ[16 + i : 17 + i, :] = own_sum(refs[i // 2], refs[(i + 1) // 2])
        for i, ref in enumerate(g3_powers + g2_powers):
            CR[0, i : i + 1, :] = own_sum(refs[0], ref)

    @pl.when(tm == 7)
    def _():
        for odd in (1, 0):
            landed(4 + odd, 1)
            start(half_copies(4 + odd, 1, done, 1))

    phase("b1_arrive")
    lax.fori_loop(0, 8, arrive, 0)

    phase("b2_gram")
    lane3 = lane_iota((8, 8, LANES))
    sub3 = lax.broadcasted_iota(jnp.int32, (8, 8, LANES), 1)
    gram = jnp.zeros((8, 8, LANES), jnp.float32)
    for i in range(8):
        gram = jnp.where(lane3 == 8 * i + sub3, jnp.sum(ROW[i], axis=2, keepdims=True), gram)
    gram = jnp.sum(gram, axis=1)
    lane4 = lane_iota((8, 16, LANES))
    sub4 = lax.broadcasted_iota(jnp.int32, (8, 16, LANES), 1)
    slab4 = lax.broadcasted_iota(jnp.int32, (8, 16, LANES), 0)
    cross = jnp.where(
        (lane4 == 13 * slab4 + sub4) & (sub4 < 13), jnp.sum(CR[...], axis=2, keepdims=True), 0.0
    )
    cross = jnp.sum(jnp.sum(cross, axis=0), axis=0, keepdims=True)
    lane5 = lane_iota((24, LANES))
    sub5 = lax.broadcasted_iota(jnp.int32, (24, LANES), 0)
    own = jnp.where(lane5 == 104 + sub5, jnp.sum(KQ[...], axis=1, keepdims=True), 0.0)
    own = cross + jnp.sum(own, axis=0, keepdims=True)
    sub2 = lax.broadcasted_iota(jnp.int32, (8, LANES), 0)
    folded = jnp.where(lane2 < 64, pltpu.roll(gram, 4, 0), pltpu.roll(gram, 64, 1))
    message = jnp.where(sub2 < 4, folded, jnp.where(sub2 == 4, own, 0.0))
    GM[...] = message
    GR[core * 16 + me] = message
    pl.semaphore_wait(plane_sem, 1)
    for a, b in far_first + [(0, 0)]:
        targets = [{"tm": sib, **plane_peer(a, b)}] + ([plane_peer(a, b)] if (a, b) != (0, 0) else [])
        for target in targets:
            pltpu.make_async_remote_copy(
                GM.at[pl.ds(0, 5)], GR.at[core * 16 + me, pl.ds(0, 5)], done, gr,
                device_id=target, device_id_type=MESH,
            ).start()
    phase("b3_wait")
    wait_rows(gr, 31 * 5)
    total = jnp.sum(GR[...], axis=0)
    plane = jnp.sum(GR[pl.ds(core * 16, 16)], axis=0)
    phase("b4_chain")

    high_slabs = [diagonal(total[k : k + 1, :], LANES) for k in range(4)]
    own_sums = diagonal(plane[4:5, :], LANES)
    with_g = [[own_sums[13 * k + i : 13 * k + i + 1, :] for k in range(8)] for i in range(13)]
    first_row = [own_sums[104 + i : 105 + i, :] for i in range(24)]
    k33, k32, k22 = first_row[:6], first_row[6:11], first_row[11:15]

    def entry(i, k, j):
        at = 8 * i + j if k >= 4 else 64 + 8 * i + j
        return high_slabs[k % 4][at : at + 1, :]

    one = jnp.ones((1, LANES), jnp.float32)
    zero = jnp.zeros((1, LANES), jnp.float32)
    coefs = {7: one}
    quad = [entry(i, 7, 7) for i in range(8)]
    cross = [{j: entry(i, 7, j) for j in range(1, 7)} for i in range(8)]
    mixed = [x[7] for x in with_g]
    is_last = jnp.full((1, LANES), tm == 7)
    held_c = {k: zero for k in range(1, 8)}
    held_q = first_row[16:24]
    held_m = [x[0] for x in with_g]
    for t in range(7, 0, -1):
        if t < 7:
            psi_t = quad[0] / (quad[0] + 4.0 * quad[1] + EPS)
            quad = [
                psi_t * psi_t * quad[i] + 2.0 * psi_t * cross[i][t] + entry(i, t, t)
                for i in range(8)
            ]
            cross = [{j: psi_t * cross[i][j] + entry(i, t, j) for j in range(1, t)} for i in range(8)]
            mixed = [psi_t * x + y[t] for x, y in zip(mixed, with_g)]
            coefs = {k: psi_t * x for k, x in coefs.items()}
            coefs[t] = one
        now = jnp.full((1, LANES), tm + 1 == t)
        for k in coefs:
            held_c[k] = jnp.where(now, coefs[k], held_c[k])
        held_q = [jnp.where(now, quad[i], held_q[i]) for i in range(8)]
        held_m = [jnp.where(now, mixed[i], held_m[i]) for i in range(13)]
    psi = held_q[0] / (held_q[0] + 4.0 * held_q[1] + EPS)
    psi = jnp.where(is_last, 0.0, psi)
    for row, count in FULL:
        part = slice(row, row + count)
        value = F[CG, :, part, :] * last
        for k in range(1, 8):
            slab = TH[row // 80, k, :, row - 64 * (row // 80) : row - 64 * (row // 80) + count, :]
            value = value + scaled(held_c[k], jnp.where(tm < k, slab, 0.0))
        V[:, part, :] = value

    def put(level, row, value):
        for t in range(4):
            out[level, row - LOW : row - LOW + value.shape[1], cols(t)] = value[t]

    def next_moments(a, b, m, n, k, count):
        return [
            jnp.maximum(
                a * a * m[i] + 2.0 * a * b * m[i + 1] + b * b * m[i + 2]
                + 2.0 * (a * n[i] + b * n[i + 1]) + k[i],
                0.0,
            )
            for i in range(count)
        ]

    a1, b1 = fine_coefs(held_q)
    m1 = next_moments(a1, b1, held_q, held_m[:7], k33, 6)
    n1 = [a1 * held_m[7 + i] + b1 * held_m[8 + i] + k32[i] for i in range(5)]
    a2, b2 = fine_coefs(m1)
    m2 = next_moments(a2, b2, m1, n1, k22, 4)
    a3, b3 = fine_coefs(m2)
    phase("c0_correct")
    for row, count in FULL:
        part = slice(row, row + count)
        v, u = spread(V, K, row, count)
        value = scaled(a1, v) + scaled(b1, u) + F[G3, :, part, :]
        X[:, part, :] = value
        put(3, max(row, LOW), own_part(value, row, count))
    for row, count in FULL:
        part = slice(row, row + count)
        v, u = spread(X, K, row, count)
        value = scaled(a2, v) + scaled(b2, u) + F[G2, :, part, :]
        W[:, part, :] = value
        put(2, max(row, LOW), own_part(value, row, count))
    for row, count in OWN:
        part = slice(row, row + count)
        v, u = spread(W, K, row, count)
        put(1, row, scaled(a3, v[:4]) + scaled(b3, u[:4]) + F[G1, :4, part, :])
        first = row - 64 * (row // 80)
        put(0, row, scaled(psi, V[:4, part, :]) + TH[row // 80, tm, :4, first : first + count, :])

    phase("c9_end")
    fixed = 2 * halo_rows + 2 * 15 + 31 * 5
    for place, halves in enumerate((6, 10, 8, 8, 7, 7, 4, 8)):
        @pl.when(tm == place)
        def _():
            wait_rows(done, fixed + halves * (4 * 72 + 8))

    phase(None)


def local(forcing, depth, mask, guess):
    f32 = jnp.float32
    field = (TILES, ROWS, LANES)
    half = (TILES, HALF_ROWS, LANES)
    dma = pltpu.SemaphoreType.DMA
    return pl.pallas_call(
        kernel,
        out_shape=jax.ShapeDtypeStruct(forcing.shape, f32),
        in_specs=[pl.BlockSpec(memory_space=pltpu.HBM)] * 4,
        out_specs=pl.BlockSpec(memory_space=pltpu.VMEM),
        scratch_shapes=[
            pltpu.VMEM((6, *field), f32),
            pltpu.VMEM((4, *field), f32),
            pltpu.VMEM(field, f32),
            pltpu.VMEM(field, f32),
            pltpu.VMEM(field, f32),
            pltpu.VMEM(field, f32),
            pltpu.VMEM((3, *field), f32),
            pltpu.VMEM((9, *field), f32),
            pltpu.VMEM((4, *half), f32),
            pltpu.VMEM((2, 8, *half), f32),
            pltpu.VMEM((8, *half), f32),
            pltpu.VMEM((8, *half), f32),
            pltpu.VMEM((8, *half), f32),
            pltpu.VMEM((8, 4, 64, LANES), f32),
            pltpu.VMEM((4, 128, LANES), f32),
            pltpu.VMEM((4, 128, LANES), jnp.int32),
            pltpu.VMEM((3, 4, 8, LANES), f32),
            pltpu.VMEM((8, 8, 8, LANES), f32),
            pltpu.VMEM((8, 16, LANES), f32),
            pltpu.VMEM((24, LANES), f32),
            pltpu.VMEM((2, 2, 3, 8, LANES), f32),
            pltpu.VMEM((2, 2, 3, 8, LANES), f32),
            pltpu.VMEM((2, 4, 8, LANES), f32),
            pltpu.VMEM((2, 4, 8, LANES), f32),
            pltpu.VMEM((8, 2, 8, LANES), f32),
            pltpu.VMEM((2, 8, LANES), f32),
            pltpu.VMEM((2, 16, LANES), f32),
            pltpu.VMEM((8, LANES), f32),
            pltpu.VMEM((32, 8, LANES), f32),
            pltpu.VMEM((3696, LANES), f32),
            dma((4,)),
            dma,
            dma((2,)),
            dma((2,)),
            dma((8, 2)),
            dma,
            pltpu.SemaphoreType.REGULAR,
        ],
        compiler_params=pltpu.CompilerParams(
            collective_id=0, has_side_effects=True, vmem_limit_bytes=VMEM_LIMIT
        ),
        name="cycle",
    )(*(pltpu.with_memory_space_constraint(x, pltpu.HBM) for x in (forcing, depth, mask, guess)))


def solution(mesh):
    return jax.shard_map(
        local,
        mesh=mesh,
        in_specs=(P("tm", "lat", "lon"), P("lat", "lon"), P("lat", "lon"), P("tm", "lat", "lon")),
        out_specs=P("tm", "lat", "lon"),
        check_vma=False,
    )
```
